32 devices in a mesh: dp: 8 (over z, y), tensor: 4 (over x, core).
Axes of the slice: x: 2, y: 2, z: 4, core: 2. Of those that a mesh axis runs over, the one named last changes fastest.
Arguments:
- inputs: bfloat16 [8, 1024, 2048], P('dp', 'tensor'), may hold values from -6 to 6
- cotangent: bfloat16 [8, 1024, 2048], P('dp', 'tensor'), may hold values from -6 to 6
- lengths: int32 [8], P('dp'), may hold values from 256 to 1024, as said below
- norm1_gain: float32 [2048], replicated, may hold values from 0.5 to 1.5
- w_query: bfloat16 [2048, 2048], P('dp', 'tensor'), may hold values from -0.125 to 0.125
- w_key: bfloat16 [2048, 2048], P('dp', 'tensor'), may hold values from -0.125 to 0.125
- w_value: bfloat16 [2048, 4096], P('dp', 'tensor'), may hold values from -0.125 to 0.125
- w_outgate: bfloat16 [2048, 4096], P('dp', 'tensor'), may hold values from -0.125 to 0.125
- w_beta: bfloat16 [2048, 16], P('dp', 'tensor'), may hold values from -0.125 to 0.125
- w_alpha: bfloat16 [2048, 16], P('dp', 'tensor'), may hold values from -0.125 to 0.125
- conv_query: bfloat16 [128, 16, 4], P('dp', 'tensor'), may hold values from -3 to 3
- conv_key: bfloat16 [128, 16, 4], P('dp', 'tensor'), may hold values from -3 to 3
- conv_value: bfloat16 [256, 16, 4], P('dp', 'tensor'), may hold values from -3 to 3
- a_log: float32 [16], replicated, may hold values from -6.5 to -3
- dt_bias: float32 [16], replicated, may hold values from -1.5 to 0.5
- head_gain: float32 [256], replicated, may hold values from 0.5 to 1.5
- w_out: bfloat16 [2048, 4096], P('dp', 'tensor'), may hold values from -0.125 to 0.125
- norm2_gain: float32 [2048], replicated, may hold values from 0.5 to 1.5
- w_gate: bfloat16 [2048, 5632], P('dp', 'tensor'), may hold values from -0.125 to 0.125
- w_up: bfloat16 [2048, 5632], P('dp', 'tensor'), may hold values from -0.125 to 0.125
- w_down: bfloat16 [2048, 5632], P('dp', 'tensor'), may hold values from -0.109375 to 0.109375
Outputs:
- outputs: bfloat16 [8, 1024, 2048], P('dp', 'tensor')
- grad_inputs: float32 [8, 1024, 2048], P('dp', 'tensor')
- grad_norm1: float32 [2048], replicated
- grad_query: float32 [2048, 2048], P('dp', 'tensor')
- grad_key: float32 [2048, 2048], P('dp', 'tensor')
- grad_value: float32 [2048, 4096], P('dp', 'tensor')
- grad_outgate: float32 [2048, 4096], P('dp', 'tensor')
- grad_beta: float32 [2048, 16], P('dp', 'tensor')
- grad_alpha: float32 [2048, 16], P('dp', 'tensor')
- grad_convq: float32 [128, 16, 4], P('dp', 'tensor')
- grad_convk: float32 [128, 16, 4], P('dp', 'tensor')
- grad_convv: float32 [256, 16, 4], P('dp', 'tensor')
- grad_alog: float32 [16], replicated
- grad_dtbias: float32 [16], replicated
- grad_headgain: float32 [256], replicated
- grad_out: float32 [2048, 4096], P('dp', 'tensor')
- grad_norm2: float32 [2048], replicated
- grad_gate: float32 [2048, 5632], P('dp', 'tensor')
- grad_up: float32 [2048, 5632], P('dp', 'tensor')
- grad_down: float32 [2048, 5632], P('dp', 'tensor')
The draws below stay inside these ranges and needn't reach their ends.
Inputs may be any that keep to these rules, and one draw needn't show every extreme that they name: `lengths`: each sequence's valid tokens start at its slot's first position; in every draw some sequence fills its whole slot of 1024 positions.
All inputs are finite; a program needn't handle non-finite values.
Results may differ from the reference program's by a relative error of at most 0.025.
Values may be sent and summed in bfloat16 or wider, within the bound.
A program may use at most 320 MiB of HBM per device.

```python
import jax
import jax.numpy as jnp
from jax import lax

D = 2048
H = 16
DK = 128
DV = 256
FF = 5632
CONV = 4
BLOCK = 64
LEN = 1024
SEQS = 8
HK = 2048
HV = 4096


def draw_lengths(key, part):
    base_lengths = jax.random.randint(jax.random.fold_in(key, 11), (SEQS,), LEN // 4, LEN + 1)
    fullest = jax.random.randint(jax.random.fold_in(key, 12), (), 0, SEQS)
    return jnp.where(jnp.arange(SEQS) == fullest, LEN, base_lengths).astype(jnp.int32)


def shard_levels(own_key, extent, cuts, smallest, high):
    factor_of = 1.0
    for dim, parts in cuts:
        draws = jax.random.uniform(jax.random.fold_in(jax.random.fold_in(own_key, 6), dim), (parts,), jnp.float32, smallest / len(cuts), high / len(cuts))
        factor_of = factor_of * jnp.repeat(jnp.exp(draws), extent[dim] // parts).reshape((-1,) + (1,) * (len(extent) - 1 - dim))
    return factor_of


def normal_values(stream_key, extent, deviation, bound, split=(), kind=jnp.bfloat16):
    entries = deviation * jax.random.normal(stream_key, extent, jnp.float32)
    if split:
        entries = entries * shard_levels(stream_key, extent, split, -0.22, 0.18)
    return jnp.clip(entries, -bound, bound).astype(kind)


def setup_inputs(seed: int = 0) -> dict:
    key_list = jax.random.split(jax.random.key(seed), 22)
    return {
        "inputs": normal_values(key_list[0], (SEQS, LEN, D), 1.0, 6.0, ((0, 8), (1, 4))),
        "cotangent": normal_values(key_list[1], (SEQS, LEN, D), 1.0, 6.0, ((0, 8), (1, 4))),
        "lengths": draw_lengths(jax.random.fold_in(key_list[21], 71), 0),
        "norm1_gain": jnp.clip(1.0 + 0.1 * jax.random.normal(key_list[3], (D,), jnp.float32), 0.5, 1.5),
        "w_query": normal_values(key_list[4], (D, HK), D ** -0.5, 0.125, ((0, 8), (1, 4))),
        "w_key": normal_values(key_list[5], (D, HK), D ** -0.5, 0.125, ((0, 8), (1, 4))),
        "w_value": normal_values(key_list[6], (D, HV), D ** -0.5, 0.125, ((0, 8), (1, 4))),
        "w_outgate": normal_values(key_list[7], (D, HV), D ** -0.5, 0.125, ((0, 8), (1, 4))),
        "w_beta": normal_values(key_list[8], (D, H), D ** -0.5, 0.125, ((0, 8), (1, 4))),
        "w_alpha": normal_values(key_list[9], (D, H), D ** -0.5, 0.125, ((0, 8), (1, 4))),
        "conv_query": normal_values(key_list[10], (DK, H, CONV), CONV ** -0.5, 3.0, ((0, 8), (1, 4))),
        "conv_key": normal_values(key_list[11], (DK, H, CONV), CONV ** -0.5, 3.0, ((0, 8), (1, 4))),
        "conv_value": normal_values(key_list[12], (DV, H, CONV), CONV ** -0.5, 3.0, ((0, 8), (1, 4))),
        "a_log": jnp.clip(jax.random.uniform(key_list[13], (H,), jnp.float32, -6.5, -3.0), -6.5, -3.0),
        "dt_bias": jnp.clip(jax.random.uniform(key_list[14], (H,), jnp.float32, -1.5, 0.5), -1.5, 0.5),
        "head_gain": jnp.clip(1.0 + 0.1 * jax.random.normal(key_list[15], (DV,), jnp.float32), 0.5, 1.5),
        "w_out": normal_values(key_list[16], (D, HV), (HV // 2) ** -0.5, 0.125, ((0, 8), (1, 4))),
        "norm2_gain": jnp.clip(1.0 + 0.1 * jax.random.normal(key_list[17], (D,), jnp.float32), 0.5, 1.5),
        "w_gate": normal_values(key_list[18], (D, FF), D ** -0.5, 0.125, ((0, 8), (1, 4))),
        "w_up": normal_values(key_list[19], (D, FF), D ** -0.5, 0.125, ((0, 8), (1, 4))),
        "w_down": normal_values(key_list[20], (D, FF), (FF // 2) ** -0.5, 0.109375, ((0, 8), (1, 4))),
    }


@jax.custom_vjp
def low(v):
    return lax.optimization_barrier(v.astype(jnp.bfloat16)).astype(jnp.float32)

@jax.custom_vjp
def low_back(v):
    return v

def low_keep(v):
    return (low(v), None)

def low_pass(kept, grad):
    return (grad,)

def back_keep(v):
    return (v, None)

def back_low(kept, grad):
    return (low(grad),)
low.defvjp(low_keep, low_pass)
low_back.defvjp(back_keep, back_low)
exact_mode = lax.Precision.HIGHEST

def matmul(left_mat, right_mat):
    return jnp.dot(left_mat.astype(jnp.float32), right_mat.astype(jnp.float32), precision=exact_mode, preferred_element_type=jnp.float32)

def rms_apply(values, gain_vec):
    return values * lax.rsqrt(lax.optimization_barrier(jnp.mean(values * values, axis=-1, keepdims=True)) + 1e-05) * gain_vec

def unit_rows(values):
    return values * lax.rsqrt(lax.optimization_barrier(jnp.sum(values * values, axis=-1, keepdims=True)) + 1e-06)

def short_conv(values, weight):
    tap_count = weight.shape[2]
    row_count = values.shape[0]
    tap_table = jnp.transpose(weight, (1, 0, 2)).reshape(-1, tap_count)
    padded = jnp.pad(values, ((tap_count - 1, 0), (0, 0)))
    summed = padded[0:row_count] * tap_table[:, 0]
    for tap_index in range(1, tap_count):
        summed = summed + padded[tap_index:tap_index + row_count] * tap_table[:, tap_index]
    return jax.nn.silu(summed)

def block_step(carry_state, pieces):
    query_rows, key_rows, value_rows, beta_rows, decay_rows = pieces
    running = jnp.cumsum(decay_rows, axis=0)
    query_h = jnp.transpose(query_rows, (1, 0, 2))
    key_h = jnp.transpose(key_rows, (1, 0, 2))
    value_h = jnp.transpose(value_rows, (1, 0, 2))
    beta_h = jnp.transpose(beta_rows)
    cum_h = jnp.transpose(running)
    size_c = query_rows.shape[0]
    pos_row = lax.broadcasted_iota(jnp.int32, (size_c, size_c), 0)
    pos_col = lax.broadcasted_iota(jnp.int32, (size_c, size_c), 1)
    lower_inc = pos_row >= pos_col
    lower_strict = pos_row > pos_col
    differ = cum_h[:, :, None] - cum_h[:, None, :]
    within = jnp.where(lower_inc, jnp.exp(jnp.where(lower_inc, differ, 0.0)), 0.0)
    key_key = jnp.einsum('htd,hjd->htj', key_h, key_h, precision=exact_mode)
    coupling = jnp.where(lower_strict, beta_h[:, :, None] * within * key_key, 0.0)
    start_decay = jnp.exp(cum_h)
    key_state = jnp.einsum('htd,hde->hte', key_h, carry_state, precision=exact_mode)
    right_side = beta_h[:, :, None] * value_h - (beta_h * start_decay)[:, :, None] * key_state
    identity_mat = jnp.eye(size_c, dtype=jnp.float32)
    new_values = jax.scipy.linalg.solve_triangular(identity_mat + coupling, right_side, lower=True, unit_diagonal=True)
    query_key = jnp.einsum('htd,hjd->htj', query_h, key_h, precision=exact_mode)
    query_state = jnp.einsum('htd,hde->hte', query_h, carry_state, precision=exact_mode)
    output = start_decay[:, :, None] * query_state + jnp.einsum('htj,hje->hte', query_key * within, new_values, precision=exact_mode)
    end_decay = cum_h[:, -1]
    tail_decay = jnp.exp(end_decay[:, None] - cum_h)
    carry_state = jnp.exp(end_decay)[:, None, None] * carry_state + jnp.einsum('hjd,hje->hde', key_h * tail_decay[:, :, None], new_values, precision=exact_mode)
    return (carry_state, jnp.transpose(output, (1, 0, 2)))

def delta_rule(query_rows, key_rows, value_rows, beta_rows, decay_rows):
    row_count, heads_n, key_size = query_rows.shape
    value_size = value_rows.shape[2]
    blocks = row_count // BLOCK

    def to_blocks(array_in):
        return array_in.reshape((blocks, BLOCK) + array_in.shape[1:])
    carry_state = jnp.zeros((heads_n, key_size, value_size), jnp.float32)
    unused, outputs = lax.scan(jax.checkpoint(block_step), carry_state, (to_blocks(query_rows), to_blocks(key_rows), to_blocks(value_rows), to_blocks(beta_rows), to_blocks(decay_rows)))
    return outputs.reshape(row_count, heads_n, value_size)

def mixer_core(q_raw, k_raw, v_raw, og_raw, b_raw, a_raw, conv_q, conv_k, conv_v, a_log, dt_bias, head_gain):
    row_count = q_raw.shape[0]
    heads_n = a_log.shape[0]
    key_size = conv_q.shape[0]
    value_size = conv_v.shape[0]
    query_rows = unit_rows(short_conv(q_raw, conv_q).reshape(row_count, heads_n, key_size)) * key_size ** (-0.5)
    key_rows = unit_rows(short_conv(k_raw, conv_k).reshape(row_count, heads_n, key_size))
    value_rows = short_conv(v_raw, conv_v).reshape(row_count, heads_n, value_size)
    beta_rows = jax.nn.sigmoid(b_raw)
    decay_rows = -jnp.exp(a_log) * jax.nn.softplus(a_raw + dt_bias)
    delta_out = delta_rule(query_rows, key_rows, value_rows, beta_rows, decay_rows)
    normed = rms_apply(delta_out, head_gain) * jax.nn.silu(og_raw.reshape(row_count, heads_n, value_size))
    return normed.reshape(row_count, heads_n * value_size)

def block_forward(params, inputs, length):
    norm1_gain, w_query, w_key, w_value, w_outgate, w_beta, w_alpha, conv_query, conv_key, conv_value, a_log, dt_bias, head_gain, w_out, norm2_gain, w_gate, w_up, w_down = params
    row_count = inputs.shape[0]
    valid_rows = (jnp.arange(row_count, dtype=jnp.int32) < length).astype(jnp.float32)[:, None]
    normed_one = low(rms_apply(inputs, norm1_gain))
    q_raw = low_back(matmul(normed_one, w_query))
    k_raw = low_back(matmul(normed_one, w_key))
    v_raw = low_back(matmul(normed_one, w_value))
    og_raw = low_back(matmul(normed_one, w_outgate))
    b_raw = low_back(matmul(normed_one, w_beta))
    a_raw = low_back(matmul(normed_one, w_alpha))
    head_out = low(mixer_core(q_raw, k_raw, v_raw, og_raw, b_raw, a_raw, conv_query, conv_key, conv_value, a_log, dt_bias, head_gain))
    after_mix = inputs + low_back(matmul(head_out, w_out.T))
    normed_two = low(rms_apply(after_mix, norm2_gain))
    gate_pre = low_back(matmul(normed_two, w_gate))
    up_pre = low_back(matmul(normed_two, w_up))
    hidden = low(jax.nn.silu(gate_pre) * up_pre)
    after_ffn = after_mix + low_back(matmul(hidden, w_down.T))
    return after_ffn * valid_rows

def reference(inputs, cotangent, lengths, norm1_gain, w_query, w_key, w_value, w_outgate, w_beta, w_alpha, conv_query, conv_key, conv_value, a_log, dt_bias, head_gain, w_out, norm2_gain, w_gate, w_up, w_down):
    params = tuple((weight.astype(jnp.float32) for weight in (norm1_gain, w_query, w_key, w_value, w_outgate, w_beta, w_alpha, conv_query, conv_key, conv_value, a_log, dt_bias, head_gain, w_out, norm2_gain, w_gate, w_up, w_down)))

    def per_sequence(totals, entry_items):
        seq_inputs, seq_cot, seq_length = entry_items

        def forward_of(param_set, layer_in):
            return block_forward(param_set, layer_in, seq_length)
        result, vjp_back = jax.vjp(forward_of, params, seq_inputs.astype(jnp.float32))
        grad_params, grad_layer_in = vjp_back(seq_cot.astype(jnp.float32))
        totals = tuple((total_now + grad_now for total_now, grad_now in zip(totals, grad_params)))
        return (totals, (result.astype(jnp.bfloat16), grad_layer_in))
    zero_sums = tuple((jnp.zeros_like(weight) for weight in params))
    totals, (outputs, grad_inputs) = lax.scan(per_sequence, zero_sums, (inputs, cotangent, lengths))
    return (outputs, grad_inputs) + totals
```

```python
import functools

import jax
import jax.numpy as jnp
from jax import lax
from jax.experimental import pallas as pl
from jax.experimental.pallas import tpu as pltpu
from jax.sharding import PartitionSpec as P

CH = 128
HALO = 8
LANES = 128
F32 = jnp.float32
BF = jnp.bfloat16


def mm(a, b, dims=((1,), (0,))):
    return lax.dot_general(a, b, (dims, ((), ())), preferred_element_type=F32)


NT = ((1,), (1,))
TN = ((0,), (0,))


def split(x):
    hi = x.astype(BF)
    return hi, (x - hi.astype(F32)).astype(BF)


def mm3(a, b):
    return mm(a[0], b[0]) + (mm(a[0], b[1]) + mm(a[1], b[0]))


def exact_mm(a, b):
    return lax.dot_general(
        a, b, (((1,), (0,)), ((), ())), precision=lax.Precision.HIGHEST, preferred_element_type=F32
    )


def unit_lower_inverse(mats):
    n = mats[0].shape[0]
    row = lax.broadcasted_iota(jnp.int32, (n, n), 0)
    col = lax.broadcasted_iota(jnp.int32, (n, n), 1)

    def off_block(size):
        same = (row // (2 * size)) == (col // (2 * size))
        return same & ((row // size) % 2 == 1) & ((col // size) % 2 == 0)

    eye = jnp.where(row == col, 1.0, 0.0)
    inv = [eye - jnp.where(off_block(1), a, 0.0) for a in mats]
    size = 2
    while size < n:
        mask = off_block(size)
        halves = [split(x) for x in inv]
        low = [split(jnp.where(mask, a, 0.0)) for a in mats]
        mid = [split(mm3(b, x)) for b, x in zip(low, halves)]
        inv = [x - mm3(xs, y) for x, xs, y in zip(inv, halves, mid)]
        size *= 2
    return inv


def softplus(x):
    return jnp.maximum(x, 0.0) + jnp.log1p(jnp.exp(-jnp.abs(x)))


def sigmoid(x):
    return 1.0 / (1.0 + jnp.exp(-x))


def conv_of(buf, taps, rows):
    out = buf[HALO - 3 : HALO - 3 + rows, :] * taps[0:1, :]
    for i in range(1, 4):
        out = out + buf[HALO - 3 + i : HALO - 3 + i + rows, :] * taps[i : i + 1, :]
    return out


def decay_tables(ab, par, rows):
    beta = sigmoid(ab)
    decay = -jnp.exp(par[0:1, :]) * softplus(ab + par[1:2, :])
    row = lax.broadcasted_iota(jnp.int32, (rows, rows), 0)
    col = lax.broadcasted_iota(jnp.int32, (rows, rows), 1)
    run = exact_mm(jnp.where(row >= col, 1.0, 0.0), decay)
    return beta, decay, run, jnp.transpose(run), row, col


def fwd_body(
    heads, dk, dv, q_ref, k_ref, v_ref, og_ref, ab_ref, tq_ref, tk_ref, tv_ref, par_ref, gain_ref,
    head_ref, o_ref, u_ref, t_ref, s_ref, qb, kb, vb, state,
):
    rows = CH

    @pl.when(pl.program_id(0) == 0)
    def _():
        for buf in (qb, kb, vb):
            buf[0:HALO, :] = jnp.zeros((HALO, buf.shape[1]), F32)
        state[...] = jnp.zeros_like(state)

    hs = range(heads)
    raw = []
    for buf, ref, taps in ((qb, q_ref, tq_ref), (kb, k_ref, tk_ref), (vb, v_ref, tv_ref)):
        buf[HALO : HALO + rows, :] = ref[...]
        raw.append(conv_of(buf, taps, rows))
        buf[0:HALO, :] = buf[rows : rows + HALO, :]
    zq, zk, zv = raw
    beta, _, run, run_t, row, col = decay_tables(ab_ref[...], par_ref, rows)
    low_inc = row >= col
    low_strict = row > col
    scale = dk ** (-0.5)

    def unit(z):
        y = z * sigmoid(z)
        return y * lax.rsqrt(jnp.sum(y * y, axis=-1, keepdims=True) + 1e-6)

    q = [unit(zq[:, h * dk : (h + 1) * dk]) * scale for h in hs]
    k = [unit(zk[:, h * dk : (h + 1) * dk]) for h in hs]
    qk_b = [(a.astype(BF), b.astype(BF)) for a, b in zip(q, k)]
    bt = [beta[:, h : h + 1] for h in hs]
    g_col = [run[:, heads + h : heads + h + 1] for h in hs]
    g_row = [run_t[heads + h : heads + h + 1, :] for h in hs]
    dec = [jnp.where(low_inc, jnp.exp(jnp.where(low_inc, g_col[h] - g_row[h], 0.0)), 0.0) for h in hs]
    kk = [mm(qk_b[h][1], qk_b[h][1], NT) for h in hs]
    inv = unit_lower_inverse([jnp.where(low_strict, bt[h] * dec[h] * kk[h], 0.0) for h in hs])
    inv_b = [x.astype(BF) for x in inv]
    p_b = [(mm(qk_b[h][0], qk_b[h][1], NT) * dec[h]).astype(BF) for h in hs]
    start = [jnp.exp(g) for g in g_col]
    end = [run[rows - 1 : rows, heads + h : heads + h + 1] for h in hs]
    s0 = [state[h] for h in hs]
    s0_b = [x.astype(BF) for x in s0]
    for h in hs:
        t_ref[:, h * rows : (h + 1) * rows] = inv_b[h]
        s_ref[:, h * dv : (h + 1) * dv] = s0_b[h]
    rhs = []
    for h in hs:
        z = zv[:, h * dv : (h + 1) * dv]
        val = z * sigmoid(z)
        rhs.append((bt[h] * val - (bt[h] * start[h]) * mm(qk_b[h][1], s0_b[h])).astype(BF))
    u_b = [mm(inv_b[h], rhs[h]).astype(BF) for h in hs]
    for h in hs:
        u_ref[:, h * dv : (h + 1) * dv] = u_b[h]
        tail = (k[h] * jnp.exp(end[h] - g_col[h])).astype(BF)
        state[h] = jnp.exp(end[h]) * s0[h] + mm(tail, u_b[h], TN)
    for h in hs:
        o = start[h] * mm(qk_b[h][0], s0_b[h]) + mm(p_b[h], u_b[h])
        o_ref[:, h * dv : (h + 1) * dv] = o
        og = og_ref[:, h * dv : (h + 1) * dv]
        r = lax.rsqrt(jnp.mean(o * o, axis=-1, keepdims=True) + 1e-5)
        head_ref[:, h * dv : (h + 1) * dv] = (o * r * gain_ref[...] * (og * sigmoid(og))).astype(BF)


def bwd_body(
    heads, dk, dv, q_ref, k_ref, v_ref, og_ref, ab_ref, qh_ref, kh_ref, vh_ref,
    tq_ref, tk_ref, tv_ref, par_ref, gain_ref, g_ref, o_ref, u_ref, t_ref, s_ref,
    dqk_ref, dv_ref, dog_ref, dab_ref, dtq_ref, dtk_ref, dtv_ref, dpar_ref, dgain_ref,
    qb, kb, vb, qn, kn, vn, dstate,
):
    rows = CH
    step = pl.program_id(0)
    first = step == 0
    is_top = step == pl.num_programs(0) - 1

    @pl.when(first)
    def _():
        for buf in (qn, kn, vn):
            buf[rows : rows + HALO, :] = jnp.zeros((HALO, buf.shape[1]), F32)
        for ref in (dtq_ref, dtk_ref, dtv_ref, dpar_ref, dgain_ref, dstate):
            ref[...] = jnp.zeros_like(ref)

    hs = range(heads)
    raw = []
    for buf, ref, halo, taps in (
        (qb, q_ref, qh_ref, tq_ref), (kb, k_ref, kh_ref, tk_ref), (vb, v_ref, vh_ref, tv_ref)
    ):
        buf[0:HALO, :] = jnp.where(is_top, 0.0, halo[...])
        buf[HALO : HALO + rows, :] = ref[...]
        raw.append(conv_of(buf, taps, rows))
    zq, zk, zv = raw
    ab = ab_ref[...]
    beta, decay, run, run_t, row, col = decay_tables(ab, par_ref, rows)
    low_inc = row >= col
    low_strict = row > col
    scale = dk ** (-0.5)

    def unit(z):
        sg = sigmoid(z)
        y = z * sg
        n = lax.rsqrt(jnp.sum(y * y, axis=-1, keepdims=True) + 1e-6)
        return y * n, n, sg * (1.0 + z * (1.0 - sg))

    qu = [unit(zq[:, h * dk : (h + 1) * dk]) for h in hs]
    ku = [unit(zk[:, h * dk : (h + 1) * dk]) for h in hs]
    q = [x[0] * scale for x in qu]
    k = [x[0] for x in ku]
    q_b = [x.astype(BF) for x in q]
    k_b = [x.astype(BF) for x in k]
    bt = [beta[:, h : h + 1] for h in hs]
    g_col = [run[:, heads + h : heads + h + 1] for h in hs]
    g_row = [run_t[heads + h : heads + h + 1, :] for h in hs]
    dec = [jnp.where(low_inc, jnp.exp(jnp.where(low_inc, g_col[h] - g_row[h], 0.0)), 0.0) for h in hs]
    start = [jnp.exp(g) for g in g_col]
    end = [run[rows - 1 : rows, heads + h : heads + h + 1] for h in hs]
    tail = [jnp.exp(end[h] - g_col[h]) for h in hs]
    dkk = [mm(k_b[h], k_b[h], NT) * dec[h] for h in hs]
    prob = [mm(q_b[h], k_b[h], NT) * dec[h] for h in hs]
    u_b = [u_ref[:, h * dv : (h + 1) * dv] for h in hs]
    s0_b = [s_ref[:, h * dv : (h + 1) * dv] for h in hs]
    ds1 = [dstate[h] for h in hs]
    ds1_b = [x.astype(BF) for x in ds1]

    gain = gain_ref[...]
    do_b = []
    dgain = jnp.zeros_like(gain)
    for h in hs:
        sl = slice(h * dv, (h + 1) * dv)
        o = o_ref[:, sl]
        og = og_ref[:, sl]
        g = g_ref[:, sl]
        r = lax.rsqrt(jnp.mean(o * o, axis=-1, keepdims=True) + 1e-5)
        sg = sigmoid(og)
        gor = g * (o * r)
        dgain = dgain + jnp.sum(gor * (og * sg), axis=0, keepdims=True)
        dog_ref[:, sl] = (gor * gain * (sg * (1.0 + og * (1.0 - sg)))).astype(BF)
        m = g * gain * (og * sg)
        d_o = r * m - o * (r * r * r * jnp.mean(m * o, axis=-1, keepdims=True))
        do_b.append(d_o.astype(BF))
    dgain_ref[...] += dgain

    d_u = [
        mm(prob[h].astype(BF), do_b[h], TN) + mm((k[h] * tail[h]).astype(BF), ds1_b[h]) for h in hs
    ]
    d_r = [mm(t_ref[:, h * rows : (h + 1) * rows], d_u[h].astype(BF), TN) for h in hs]
    dr_b = [x.astype(BF) for x in d_r]
    for h in hs:
        left = jnp.concatenate(
            [(q[h] * start[h]).astype(BF), (k[h] * (-(bt[h] * start[h]))).astype(BF)], axis=0
        )
        right = jnp.concatenate([do_b[h], dr_b[h]], axis=0)
        dstate[h] = jnp.exp(end[h]) * ds1[h] + mm(left, right, TN)

    lane = lax.broadcasted_iota(jnp.int32, (rows, LANES), 1)
    sub = lax.broadcasted_iota(jnp.int32, (LANES, rows), 0)
    dab_cols = jnp.zeros((rows, LANES), F32)
    dg_cols = jnp.zeros((rows, LANES), F32)
    dg_rows = jnp.zeros((LANES, rows), F32)
    dend = jnp.zeros((1, LANES), F32)
    lane_one = lax.broadcasted_iota(jnp.int32, (1, LANES), 1)
    for h in hs:
        sl = slice(h * dv, (h + 1) * dv)
        ks = slice(h * dk, (h + 1) * dk)
        d_p = jnp.where(low_inc, mm(do_b[h], u_b[h], NT), 0.0)
        d_a = jnp.where(low_strict, -mm(dr_b[h], u_b[h], NT), 0.0)
        pp = d_p * prob[h]
        dqk_b = (d_p * dec[h]).astype(BF)
        ad = d_a * dkk[h]
        d_kk = d_a * (bt[h] * dec[h])
        d_kk = (d_kk + jnp.transpose(d_kk)).astype(BF)
        y = mm(do_b[h], s0_b[h], NT)
        x = mm(dr_b[h], s0_b[h], NT)
        z = mm(u_b[h], ds1_b[h], NT)
        dq = mm(dqk_b, k_b[h]) + start[h] * y
        bstart = bt[h] * start[h]
        kx = jnp.sum(k[h] * x, axis=-1, keepdims=True)
        kz = tail[h] * jnp.sum(k[h] * z, axis=-1, keepdims=True)
        dkey = mm(d_kk, k_b[h]) + mm(dqk_b, q_b[h], TN) - bstart * x + tail[h] * z
        zval = zv[:, sl]
        sgv = sigmoid(zval)
        val = zval * sgv
        ad_row = jnp.sum(ad, axis=-1, keepdims=True)
        d_beta = jnp.sum(d_r[h] * val, axis=-1, keepdims=True) - start[h] * kx + ad_row
        d_g = (
            jnp.sum(pp, axis=-1, keepdims=True)
            + bt[h] * ad_row
            + start[h] * jnp.sum(q[h] * y, axis=-1, keepdims=True)
            - bstart * kx
            - kz
        )
        d_g_row = -jnp.sum(pp + bt[h] * ad, axis=0, keepdims=True)
        d_end = jnp.sum(kz, axis=0, keepdims=True) + jnp.exp(end[h]) * jnp.sum(
            jnp.sum(s0_b[h].astype(F32) * ds1[h], axis=-1, keepdims=True), axis=0, keepdims=True
        )
        dab_cols = dab_cols + jnp.where(lane == h, d_beta, 0.0)
        dg_cols = dg_cols + jnp.where(lane == heads + h, d_g, 0.0)
        dg_rows = dg_rows + jnp.where(sub == heads + h, d_g_row, 0.0)
        dend = dend + jnp.where(lane_one == heads + h, d_end, 0.0)
        vn[0:rows, sl] = (bt[h] * d_r[h]) * (sgv * (1.0 + zval * (1.0 - sgv)))
        for buf, du, (un, n, slope) in ((qn, dq * scale, qu[h]), (kn, dkey, ku[h])):
            dy = n * (du - un * jnp.sum(un * du, axis=-1, keepdims=True))
            buf[0:rows, ks] = dy * slope

    d_run = dg_cols + jnp.transpose(dg_rows)
    d_decay = exact_mm(jnp.where(col >= row, 1.0, 0.0), d_run) + dend
    pick = (lane >= heads) & (lane < 2 * heads)
    d_decay = jnp.where(pick, d_decay, 0.0)
    d_alpha = d_decay * (-jnp.exp(par_ref[0:1, :])) * sigmoid(ab + par_ref[1:2, :])
    dpar_ref[0:1, :] += jnp.sum(d_decay * decay, axis=0, keepdims=True)
    dpar_ref[1:2, :] += jnp.sum(d_alpha, axis=0, keepdims=True)
    dab_ref[...] = (dab_cols * beta * (1.0 - beta) + d_alpha).astype(BF)

    wide = heads * dk
    for buf, cur, taps, out, at, dtap in (
        (qn, qb, tq_ref, dqk_ref, 0, dtq_ref),
        (kn, kb, tk_ref, dqk_ref, wide, dtk_ref),
        (vn, vb, tv_ref, dv_ref, 0, dtv_ref),
    ):
        here = cur[HALO : HALO + rows, :]
        total = None
        for i in range(4):
            moved = buf[3 - i : 3 - i + rows, :]
            term = moved * taps[i : i + 1, :]
            total = term if total is None else total + term
            dtap[i : i + 1, :] += jnp.sum(here * moved, axis=0, keepdims=True)
        out[:, at : at + total.shape[1]] = total.astype(BF)
        buf[rows : rows + HALO, :] = buf[0:HALO, :]


def mixer_specs(heads, dk, dv, at):
    wide_k, wide_v = heads * dk, heads * dv
    full = lambda shape: pl.BlockSpec(shape, lambda c: (0,) * len(shape))
    return {
        "q": pl.BlockSpec((CH, wide_k), lambda c: (at(c), 0)),
        "k": pl.BlockSpec((CH, wide_k), lambda c: (at(c), 1)),
        "qk": pl.BlockSpec((CH, 2 * wide_k), lambda c: (at(c), 0)),
        "v": pl.BlockSpec((CH, wide_v), lambda c: (at(c), 0)),
        "ab": pl.BlockSpec((CH, LANES), lambda c: (at(c), 0)),
        "t": pl.BlockSpec((CH, heads * CH), lambda c: (at(c), 0)),
        "s": pl.BlockSpec((None, dk, wide_v), lambda c: (at(c), 0, 0)),
        "tk": full((8, wide_k)),
        "tv": full((8, wide_v)),
        "par": full((8, LANES)),
        "gain": full((1, dv)),
    }


def mixer_forward(qk_raw, v_raw, og_raw, ab, tq, tk, tv, par, gain):
    length, wide_k = qk_raw.shape[0], qk_raw.shape[1] // 2
    wide_v = v_raw.shape[1]
    dv = gain.shape[1]
    heads = wide_v // dv
    dk = wide_k // heads
    steps = length // CH
    sp = mixer_specs(heads, dk, dv, lambda c: c)
    return pl.pallas_call(
        functools.partial(fwd_body, heads, dk, dv),
        grid=(steps,),
        in_specs=[sp[n] for n in ("q", "k", "v", "v", "ab", "tk", "tk", "tv", "par", "gain")],
        out_specs=[sp[n] for n in ("v", "v", "v", "t", "s")],
        out_shape=[
            jax.ShapeDtypeStruct((length, wide_v), BF),
            jax.ShapeDtypeStruct((length, wide_v), F32),
            jax.ShapeDtypeStruct((length, wide_v), BF),
            jax.ShapeDtypeStruct((length, heads * CH), BF),
            jax.ShapeDtypeStruct((steps, dk, wide_v), BF),
        ],
        scratch_shapes=[
            pltpu.VMEM((CH + HALO, wide_k), F32),
            pltpu.VMEM((CH + HALO, wide_k), F32),
            pltpu.VMEM((CH + HALO, wide_v), F32),
            pltpu.VMEM((heads, dk, dv), F32),
        ],
        compiler_params=pltpu.CompilerParams(
            dimension_semantics=("arbitrary",), vmem_limit_bytes=40 << 20
        ),
        cost_estimate=pl.CostEstimate(flops=20_000_000_000, bytes_accessed=40_000_000, transcendentals=6_000_000),
        name="mixer_forward",
    )(qk_raw, qk_raw, v_raw, og_raw, ab, tq, tk, tv, par, gain)


def mixer_backward(qk_raw, v_raw, og_raw, ab, tq, tk, tv, par, gain, grad, o, u, t, s):
    length, wide_k = qk_raw.shape[0], qk_raw.shape[1] // 2
    wide_v = v_raw.shape[1]
    dv = gain.shape[1]
    heads = wide_v // dv
    dk = wide_k // heads
    steps = length // CH
    at = lambda c: steps - 1 - c
    sp = mixer_specs(heads, dk, dv, at)
    before = lambda c: jnp.maximum(at(c) * (CH // HALO) - 1, 0)
    hq = pl.BlockSpec((HALO, wide_k), lambda c: (before(c), 0))
    hk = pl.BlockSpec((HALO, wide_k), lambda c: (before(c), 1))
    hv = pl.BlockSpec((HALO, wide_v), lambda c: (before(c), 0))
    names = ("q", "k", "v", "v", "ab")
    rest = ("tk", "tk", "tv", "par", "gain", "v", "v", "v", "t", "s")
    return pl.pallas_call(
        functools.partial(bwd_body, heads, dk, dv),
        grid=(steps,),
        in_specs=[sp[n] for n in names] + [hq, hk, hv] + [sp[n] for n in rest],
        out_specs=[sp[n] for n in ("qk", "v", "v", "ab", "tk", "tk", "tv", "par", "gain")],
        out_shape=[
            jax.ShapeDtypeStruct((length, 2 * wide_k), BF),
            jax.ShapeDtypeStruct((length, wide_v), BF),
            jax.ShapeDtypeStruct((length, wide_v), BF),
            jax.ShapeDtypeStruct((length, LANES), BF),
            jax.ShapeDtypeStruct((8, wide_k), F32),
            jax.ShapeDtypeStruct((8, wide_k), F32),
            jax.ShapeDtypeStruct((8, wide_v), F32),
            jax.ShapeDtypeStruct((8, LANES), F32),
            jax.ShapeDtypeStruct((1, dv), F32),
        ],
        scratch_shapes=[
            pltpu.VMEM((CH + HALO, wide_k), F32),
            pltpu.VMEM((CH + HALO, wide_k), F32),
            pltpu.VMEM((CH + HALO, wide_v), F32),
            pltpu.VMEM((CH + HALO, wide_k), F32),
            pltpu.VMEM((CH + HALO, wide_k), F32),
            pltpu.VMEM((CH + HALO, wide_v), F32),
            pltpu.VMEM((heads, dk, dv), F32),
        ],
        compiler_params=pltpu.CompilerParams(
            dimension_semantics=("arbitrary",), vmem_limit_bytes=48 << 20
        ),
        cost_estimate=pl.CostEstimate(flops=40_000_000_000, bytes_accessed=60_000_000, transcendentals=9_000_000),
        name="mixer_backward",
    )(
        qk_raw, qk_raw, v_raw, og_raw, ab, qk_raw, qk_raw, v_raw, tq, tk, tv, par, gain, grad, o, u, t, s
    )


def plain_dot(left_mat, right_mat):
    return jnp.dot(left_mat, right_mat, preferred_element_type=F32)


def dot_rows(left_mat, right_mat):
    return lax.dot_general(left_mat, right_mat, (((1,), (1,)), ((), ())), preferred_element_type=F32)


def dot_tokens(left_mat, right_mat):
    return lax.dot_general(left_mat, right_mat, (((0,), (0,)), ((), ())), preferred_element_type=F32)


def rms_apply(values, gain_vec):
    return values * lax.rsqrt(jnp.mean(values * values, axis=-1, keepdims=True) + 1e-05) * gain_vec


def swiglu(gate_pre, up_pre):
    return jax.nn.silu(gate_pre) * up_pre


class RingRows:
    def __init__(self, dp_size):
        self.outer = dp_size // 2
        self.index = lax.axis_index("dp")
        self.last = None

    def _roll(self, x, axis, blocks):
        size = x.shape[axis] // self.outer * blocks
        return jnp.concatenate(
            [lax.slice_in_dim(x, size, None, axis=axis), lax.slice_in_dim(x, 0, size, axis=axis)], axis
        )

    def reorder(self, x, axis):
        outer_at, pair_at = self.index // 2, self.index % 2
        size = x.shape[axis] // (2 * self.outer)
        cut = [lax.slice_in_dim(x, b * size, (b + 1) * size, axis=axis) for b in range(2 * self.outer)]
        even, odd = jnp.concatenate(cut[0::2], axis), jnp.concatenate(cut[1::2], axis)
        sides = [jnp.where(pair_at == 0, even, odd), jnp.where(pair_at == 0, odd, even)]
        bit = 1
        while bit < self.outer:
            sides = [jnp.where((outer_at // bit) % 2 == 1, self._roll(s, axis, bit), s) for s in sides]
            bit *= 2
        return jnp.concatenate(sides, axis)

    def restore(self, x, axis):
        outer_at, pair_at = self.index // 2, self.index % 2
        half = x.shape[axis] // 2
        sides = [lax.slice_in_dim(x, 0, half, axis=axis), lax.slice_in_dim(x, half, None, axis=axis)]
        bit = 1
        while bit < self.outer:
            sides = [
                jnp.where((outer_at // bit) % 2 == 1, self._roll(s, axis, self.outer - bit), s) for s in sides
            ]
            bit *= 2
        even = jnp.where(pair_at == 0, sides[0], sides[1])
        odd = jnp.where(pair_at == 0, sides[1], sides[0])
        size = half // self.outer
        cut = []
        for b in range(self.outer):
            cut += [lax.slice_in_dim(s, b * size, (b + 1) * size, axis=axis) for s in (even, odd)]
        return jnp.concatenate(cut, axis)

    def _swap(self, x):
        return lax.ppermute(x, "dp", [(i, i ^ 1) for i in range(2 * self.outer)])

    def _from(self, x, steps):
        n = 2 * self.outer
        return lax.ppermute(x, "dp", [((i + 2 * steps) % n, i) for i in range(n)])

    def gather(self, block):
        if self.last is not None:
            block, self.last = lax.optimization_barrier((block, self.last))
        own = [block] + [self._from(block, k) for k in range(1, self.outer)]
        self.last = own[-1]
        other = [self._swap(b) for b in own]
        return jnp.concatenate(own + other, axis=0)

    def scatter(self, left, right):
        half = left.shape[1] // 2
        sent = dot_tokens(left[:, half:], right).astype(BF)
        came = self._swap(sent)
        pair = (dot_tokens(left[:, :half], right) + came.astype(F32)).astype(BF)
        size = half // self.outer
        n = 2 * self.outer
        total = pair[:size].astype(F32)
        for k in range(1, self.outer):
            piece = pair[k * size : (k + 1) * size]
            total = total + lax.ppermute(
                piece, "dp", [(i, (i + 2 * k) % n) for i in range(n)]
            ).astype(F32)
        return total


class PlainRows:
    def reorder(self, x, axis):
        return x

    def restore(self, x, axis):
        return x

    def gather(self, block):
        return lax.all_gather(block, "dp", axis=0, tiled=True)

    def scatter(self, left, right):
        full = dot_tokens(left, right).astype(BF)
        return lax.psum_scatter(full, "dp", scatter_dimension=0, tiled=True).astype(F32)


def tensor_gather(x):
    return lax.all_gather(x, "tensor", axis=0, tiled=True)


def tensor_scatter(x):
    return lax.psum_scatter(x, "tensor", scatter_dimension=0, tiled=True)


def shards(
    dp_size, inputs, cotangent, lengths, norm1_gain, w_query, w_key, w_value, w_outgate, w_beta, w_alpha,
    conv_query, conv_key, conv_value, a_log, dt_bias, head_gain, w_out, norm2_gain, w_gate, w_up, w_down,
):
    rows = RingRows(dp_size) if dp_size == 8 else PlainRows()
    heads = w_beta.shape[1]
    wide_k, wide_v = w_query.shape[1], w_value.shape[1]
    dk, dv = wide_k // heads, wide_v // heads
    taps_n = conv_query.shape[2]
    block = w_query.shape[0]
    tensor_pos = lax.axis_index("tensor")
    head_start = tensor_pos * heads

    row_count = inputs.shape[1]
    positions = tensor_pos * row_count + jnp.arange(row_count, dtype=jnp.int32)
    valid_rows = (positions < lengths[0]).astype(F32)[:, None]

    small = jnp.concatenate(
        [w_beta.reshape(-1), w_alpha.reshape(-1), conv_query.reshape(-1), conv_key.reshape(-1), conv_value.reshape(-1)]
    )[None]
    small = lax.all_gather(small, "dp", axis=0, tiled=True)
    cuts = [0]
    for part in (w_beta, w_alpha, conv_query, conv_key, conv_value):
        cuts.append(cuts[-1] + part.size)
    pieces = [small[:, a:b] for a, b in zip(cuts[:-1], cuts[1:])]
    full_ab = rows.reorder(
        jnp.concatenate([p.reshape(dp_size * block, heads) for p in pieces[:2]], axis=1), 0
    )
    full_ab = jnp.pad(full_ab, ((0, 0), (0, LANES - 2 * heads)))

    def tap_table(piece, size):
        table = piece.reshape(size, heads, taps_n).astype(F32)
        return jnp.pad(jnp.transpose(table, (2, 1, 0)).reshape(taps_n, heads * size), ((0, 8 - taps_n), (0, 0)))

    tq, tk, tv = tap_table(pieces[2], dk), tap_table(pieces[3], dk), tap_table(pieces[4], dv)
    alog_local = lax.dynamic_slice_in_dim(a_log, head_start, heads)
    dtb_local = lax.dynamic_slice_in_dim(dt_bias, head_start, heads)
    par = jnp.pad(jnp.stack([alog_local, dtb_local]), ((0, 6), (heads, LANES - 2 * heads)))
    gain = head_gain[None]

    local_rows = rows.reorder(inputs[0], 1).astype(F32)
    gain_one = rows.reorder(norm1_gain[None], 1)[0]
    gain_two = rows.reorder(norm2_gain[None], 1)[0]
    normed_one, norm_one_back = jax.vjp(rms_apply, local_rows, gain_one)
    rows_one = tensor_gather(normed_one.astype(BF))
    full_qk = rows.gather(jnp.concatenate([w_query, w_key], axis=1))
    full_value = rows.gather(w_value)
    full_outgate = rows.gather(w_outgate)
    full_out = rows.gather(w_out)
    full_gate = rows.gather(w_gate)
    full_up = rows.gather(w_up)
    full_down = rows.gather(w_down)
    grad_after = valid_rows * rows.reorder(cotangent[0], 1).astype(F32)
    incoming_ffn = tensor_gather(grad_after.astype(BF))

    ab_raw = plain_dot(rows_one, full_ab)
    qk_raw = plain_dot(rows_one, full_qk)
    v_raw = plain_dot(rows_one, full_value)
    og_raw = plain_dot(rows_one, full_outgate)
    core_in = (qk_raw, v_raw, og_raw, ab_raw, tq, tk, tv, par, gain)
    head_bf, delta_out, new_values, inverses, states = mixer_forward(*core_in)
    after_mix = local_rows + tensor_scatter(dot_rows(head_bf, full_out))
    normed_two, norm_two_back = jax.vjp(rms_apply, after_mix, gain_two)
    rows_two = tensor_gather(normed_two.astype(BF))
    gate_pre = plain_dot(rows_two, full_gate)
    up_pre = plain_dot(rows_two, full_up)
    hidden, swiglu_back = jax.vjp(swiglu, gate_pre, up_pre)
    hidden_bf = hidden.astype(BF)
    ffn_part = tensor_scatter(dot_rows(hidden_bf, full_down).astype(BF)).astype(F32)
    outputs = rows.restore(((after_mix + ffn_part) * valid_rows).astype(BF), 1)[None]

    grad_hidden = plain_dot(incoming_ffn, full_down)
    out_down = rows.scatter(incoming_ffn, hidden_bf)
    grad_gate_pre, grad_up_pre = swiglu_back(grad_hidden)
    gate_low = grad_gate_pre.astype(BF)
    up_low = grad_up_pre.astype(BF)
    grad_normed_two = tensor_scatter(dot_rows(gate_low, full_gate) + dot_rows(up_low, full_up))
    out_gate = rows.scatter(rows_two, gate_low)
    out_up = rows.scatter(rows_two, up_low)
    grad_mid, grad_norm2 = norm_two_back(grad_normed_two)
    grad_mid = grad_mid + grad_after
    incoming_mix = tensor_gather(grad_mid.astype(BF))

    grad_head = plain_dot(incoming_mix, full_out)
    out_out = rows.scatter(incoming_mix, head_bf)
    qk_low, v_low, og_low, ab_low, dtq, dtk, dtv, dpar, dgain = mixer_backward(
        *core_in, grad_head, delta_out, new_values, inverses, states
    )
    summed = dot_rows(qk_low, full_qk) + dot_rows(v_low, full_value)
    summed = summed + dot_rows(og_low, full_outgate) + dot_rows(ab_low, full_ab)
    grad_normed_one = tensor_scatter(summed.astype(BF)).astype(F32)
    out_qk = rows.scatter(rows_one, qk_low)
    out_value = rows.scatter(rows_one, v_low)
    out_outgate = rows.scatter(rows_one, og_low)
    grad_first, grad_norm1 = norm_one_back(grad_normed_one)
    grad_inputs = rows.restore(grad_mid + grad_first, 1)[None]

    grad_ab = rows.restore(dot_tokens(rows_one, ab_low)[:, : 2 * heads], 0)
    grad_beta, grad_alpha = grad_ab[:, :heads], grad_ab[:, heads:]

    def tap_grad(table, size):
        return jnp.transpose(table[:taps_n].reshape(taps_n, heads, size), (2, 1, 0))

    small_out = [grad_beta, grad_alpha, tap_grad(dtq, dk), tap_grad(dtk, dk), tap_grad(dtv, dv)]
    small_sum = lax.psum_scatter(
        jnp.concatenate([p.reshape(dp_size, -1) for p in small_out], axis=1), "dp", scatter_dimension=0, tiled=True
    )[0]
    shapes = (w_beta, w_alpha, conv_query, conv_key, conv_value)
    out_beta, out_alpha, out_cq, out_ck, out_cv = (
        small_sum[a:b].reshape(like.shape) for a, b, like in zip(cuts[:-1], cuts[1:], shapes)
    )
    alog_full = lax.dynamic_update_slice_in_dim(
        jnp.zeros_like(a_log), dpar[0, heads : 2 * heads], head_start, 0
    )
    dtb_full = lax.dynamic_update_slice_in_dim(
        jnp.zeros_like(dt_bias), dpar[1, heads : 2 * heads], head_start, 0
    )
    norm1_sum, norm2_sum, hgain_sum, alog_sum, dtb_sum = lax.psum(
        (
            rows.restore(grad_norm1[None], 1)[0], rows.restore(grad_norm2[None], 1)[0], dgain[0],
            alog_full, dtb_full,
        ),
        ("dp", "tensor"),
    )
    return (
        outputs, grad_inputs, norm1_sum, out_qk[:, :wide_k], out_qk[:, wide_k:], out_value, out_outgate,
        out_beta, out_alpha, out_cq, out_ck, out_cv, alog_sum, dtb_sum, hgain_sum, out_out, norm2_sum,
        out_gate, out_up, out_down,
    )


def solution(mesh):
    mat, cube, whole = P("dp", "tensor"), P("dp", "tensor", None), P()
    in_specs = (
        (cube, cube, P("dp"), whole) + (mat,) * 6 + (cube,) * 3 + (whole,) * 3 + (mat, whole) + (mat,) * 3
    )
    out_specs = (
        (cube, cube, whole) + (mat,) * 6 + (cube,) * 3 + (whole,) * 3 + (mat, whole) + (mat,) * 3
    )
    return jax.shard_map(
        functools.partial(shards, mesh.shape["dp"]), mesh=mesh, in_specs=in_specs, out_specs=out_specs,
        check_vma=False,
    )
```

```python
import functools

import jax
import jax.numpy as jnp
from jax import lax
from jax.experimental import pallas as pl
from jax.experimental.pallas import tpu as pltpu
from jax.sharding import PartitionSpec as P

CH = 128
HALO = 8
LANES = 128
F32 = jnp.float32
BF = jnp.bfloat16


def mm(a, b, dims=((1,), (0,))):
    return lax.dot_general(a, b, (dims, ((), ())), preferred_element_type=F32)


NT = ((1,), (1,))
TN = ((0,), (0,))


def split(x):
    hi = x.astype(BF)
    return hi, (x - hi.astype(F32)).astype(BF)


def mm3(a, b):
    return mm(a[0], b[0]) + (mm(a[0], b[1]) + mm(a[1], b[0]))


def exact_mm(a, b):
    return lax.dot_general(
        a, b, (((1,), (0,)), ((), ())), precision=lax.Precision.HIGHEST, preferred_element_type=F32
    )


def unit_lower_inverse(mats):
    n = mats[0].shape[0]
    row = lax.broadcasted_iota(jnp.int32, (n, n), 0)
    col = lax.broadcasted_iota(jnp.int32, (n, n), 1)

    def off_block(size):
        same = (row // (2 * size)) == (col // (2 * size))
        return same & ((row // size) % 2 == 1) & ((col // size) % 2 == 0)

    eye = jnp.where(row == col, 1.0, 0.0)
    inv = [eye - jnp.where(off_block(1), a, 0.0) for a in mats]
    size = 2
    while size < n:
        mask = off_block(size)
        halves = [split(x) for x in inv]
        low = [split(jnp.where(mask, a, 0.0)) for a in mats]
        mid = [split(mm3(b, x)) for b, x in zip(low, halves)]
        inv = [x - mm3(xs, y) for x, xs, y in zip(inv, halves, mid)]
        size *= 2
    return inv


def softplus(x):
    return jnp.maximum(x, 0.0) + jnp.log1p(jnp.exp(-jnp.abs(x)))


def sigmoid(x):
    return 1.0 / (1.0 + jnp.exp(-x))


def conv_of(buf, taps, rows):
    out = buf[HALO - 3 : HALO - 3 + rows, :] * taps[0:1, :]
    for i in range(1, 4):
        out = out + buf[HALO - 3 + i : HALO - 3 + i + rows, :] * taps[i : i + 1, :]
    return out


def decay_tables(ab, par, rows):
    beta = sigmoid(ab)
    decay = -jnp.exp(par[0:1, :]) * softplus(ab + par[1:2, :])
    row = lax.broadcasted_iota(jnp.int32, (rows, rows), 0)
    col = lax.broadcasted_iota(jnp.int32, (rows, rows), 1)
    run = exact_mm(jnp.where(row >= col, 1.0, 0.0), decay)
    return beta, decay, run, jnp.transpose(run), row, col


def fwd_body(
    heads, dk, dv, q_ref, k_ref, v_ref, og_ref, ab_ref, tq_ref, tk_ref, tv_ref, par_ref, gain_ref,
    head_ref, o_ref, u_ref, t_ref, s_ref, qb, kb, vb, state,
):
    rows = CH

    @pl.when(pl.program_id(0) == 0)
    def _():
        for buf in (qb, kb, vb):
            buf[0:HALO, :] = jnp.zeros((HALO, buf.shape[1]), F32)
        state[...] = jnp.zeros_like(state)

    hs = range(heads)
    raw = []
    for buf, ref, taps in ((qb, q_ref, tq_ref), (kb, k_ref, tk_ref), (vb, v_ref, tv_ref)):
        buf[HALO : HALO + rows, :] = ref[...]
        raw.append(conv_of(buf, taps, rows))
        buf[0:HALO, :] = buf[rows : rows + HALO, :]
    zq, zk, zv = raw
    beta, _, run, run_t, row, col = decay_tables(ab_ref[...], par_ref, rows)
    low_inc = row >= col
    low_strict = row > col
    scale = dk ** (-0.5)

    def unit(z):
        y = z * sigmoid(z)
        return y * lax.rsqrt(jnp.sum(y * y, axis=-1, keepdims=True) + 1e-6)

    q = [unit(zq[:, h * dk : (h + 1) * dk]) * scale for h in hs]
    k = [unit(zk[:, h * dk : (h + 1) * dk]) for h in hs]
    qk_b = [(a.astype(BF), b.astype(BF)) for a, b in zip(q, k)]
    bt = [beta[:, h : h + 1] for h in hs]
    g_col = [run[:, heads + h : heads + h + 1] for h in hs]
    g_row = [run_t[heads + h : heads + h + 1, :] for h in hs]
    dec = [jnp.where(low_inc, jnp.exp(jnp.where(low_inc, g_col[h] - g_row[h], 0.0)), 0.0) for h in hs]
    kk = [mm(qk_b[h][1], qk_b[h][1], NT) for h in hs]
    inv = unit_lower_inverse([jnp.where(low_strict, bt[h] * dec[h] * kk[h], 0.0) for h in hs])
    inv_b = [x.astype(BF) for x in inv]
    p_b = [(mm(qk_b[h][0], qk_b[h][1], NT) * dec[h]).astype(BF) for h in hs]
    start = [jnp.exp(g) for g in g_col]
    end = [run[rows - 1 : rows, heads + h : heads + h + 1] for h in hs]
    s0 = [state[h] for h in hs]
    s0_b = [x.astype(BF) for x in s0]
    for h in hs:
        t_ref[:, h * rows : (h + 1) * rows] = inv_b[h]
        s_ref[:, h * dv : (h + 1) * dv] = s0_b[h]
    rhs = []
    for h in hs:
        z = zv[:, h * dv : (h + 1) * dv]
        val = z * sigmoid(z)
        rhs.append((bt[h] * val - (bt[h] * start[h]) * mm(qk_b[h][1], s0_b[h])).astype(BF))
    u_b = [mm(inv_b[h], rhs[h]).astype(BF) for h in hs]
    for h in hs:
        u_ref[:, h * dv : (h + 1) * dv] = u_b[h]
        tail = (k[h] * jnp.exp(end[h] - g_col[h])).astype(BF)
        state[h] = jnp.exp(end[h]) * s0[h] + mm(tail, u_b[h], TN)
    for h in hs:
        o = start[h] * mm(qk_b[h][0], s0_b[h]) + mm(p_b[h], u_b[h])
        o_ref[:, h * dv : (h + 1) * dv] = o
        og = og_ref[:, h * dv : (h + 1) * dv]
        r = lax.rsqrt(jnp.mean(o * o, axis=-1, keepdims=True) + 1e-5)
        head_ref[:, h * dv : (h + 1) * dv] = (o * r * gain_ref[...] * (og * sigmoid(og))).astype(BF)


def bwd_body(
    heads, dk, dv, q_ref, k_ref, v_ref, og_ref, ab_ref, qh_ref, kh_ref, vh_ref,
    tq_ref, tk_ref, tv_ref, par_ref, gain_ref, g_ref, o_ref, u_ref, t_ref, s_ref,
    draw_ref, dab_ref, dtq_ref, dtk_ref, dtv_ref, dpar_ref, dgain_ref,
    qb, kb, vb, qn, kn, vn, dstate,
):
    rows = CH
    step = pl.program_id(0)
    first = step == 0
    is_top = step == pl.num_programs(0) - 1

    @pl.when(first)
    def _():
        for buf in (qn, kn, vn):
            buf[rows : rows + HALO, :] = jnp.zeros((HALO, buf.shape[1]), F32)
        for ref in (dtq_ref, dtk_ref, dtv_ref, dpar_ref, dgain_ref, dstate):
            ref[...] = jnp.zeros_like(ref)

    hs = range(heads)
    raw = []
    for buf, ref, halo, taps in (
        (qb, q_ref, qh_ref, tq_ref), (kb, k_ref, kh_ref, tk_ref), (vb, v_ref, vh_ref, tv_ref)
    ):
        buf[0:HALO, :] = jnp.where(is_top, 0.0, halo[...])
        buf[HALO : HALO + rows, :] = ref[...]
        raw.append(conv_of(buf, taps, rows))
    zq, zk, zv = raw
    ab = ab_ref[...]
    beta, decay, run, run_t, row, col = decay_tables(ab, par_ref, rows)
    low_inc = row >= col
    low_strict = row > col
    scale = dk ** (-0.5)

    def unit(z):
        sg = sigmoid(z)
        y = z * sg
        n = lax.rsqrt(jnp.sum(y * y, axis=-1, keepdims=True) + 1e-6)
        return y * n, n, sg * (1.0 + z * (1.0 - sg))

    qu = [unit(zq[:, h * dk : (h + 1) * dk]) for h in hs]
    ku = [unit(zk[:, h * dk : (h + 1) * dk]) for h in hs]
    q = [x[0] * scale for x in qu]
    k = [x[0] for x in ku]
    q_b = [x.astype(BF) for x in q]
    k_b = [x.astype(BF) for x in k]
    bt = [beta[:, h : h + 1] for h in hs]
    g_col = [run[:, heads + h : heads + h + 1] for h in hs]
    g_row = [run_t[heads + h : heads + h + 1, :] for h in hs]
    dec = [jnp.where(low_inc, jnp.exp(jnp.where(low_inc, g_col[h] - g_row[h], 0.0)), 0.0) for h in hs]
    start = [jnp.exp(g) for g in g_col]
    end = [run[rows - 1 : rows, heads + h : heads + h + 1] for h in hs]
    tail = [jnp.exp(end[h] - g_col[h]) for h in hs]
    dkk = [mm(k_b[h], k_b[h], NT) * dec[h] for h in hs]
    prob = [mm(q_b[h], k_b[h], NT) * dec[h] for h in hs]
    u_b = [u_ref[:, h * dv : (h + 1) * dv] for h in hs]
    s0_b = [s_ref[:, h * dv : (h + 1) * dv] for h in hs]
    ds1 = [dstate[h] for h in hs]
    ds1_b = [x.astype(BF) for x in ds1]

    gain = gain_ref[...]
    og_at = 2 * heads * dk + heads * dv
    do_b = []
    dgain = jnp.zeros_like(gain)
    for h in hs:
        sl = slice(h * dv, (h + 1) * dv)
        o = o_ref[:, sl]
        og = og_ref[:, sl]
        g = g_ref[:, sl]
        r = lax.rsqrt(jnp.mean(o * o, axis=-1, keepdims=True) + 1e-5)
        sg = sigmoid(og)
        gor = g * (o * r)
        dgain = dgain + jnp.sum(gor * (og * sg), axis=0, keepdims=True)
        draw_ref[:, og_at + h * dv : og_at + (h + 1) * dv] = (gor * gain * (sg * (1.0 + og * (1.0 - sg)))).astype(BF)
        m = g * gain * (og * sg)
        d_o = r * m - o * (r * r * r * jnp.mean(m * o, axis=-1, keepdims=True))
        do_b.append(d_o.astype(BF))
    dgain_ref[...] += dgain

    d_u = [
        mm(prob[h].astype(BF), do_b[h], TN) + mm((k[h] * tail[h]).astype(BF), ds1_b[h]) for h in hs
    ]
    d_r = [mm(t_ref[:, h * rows : (h + 1) * rows], d_u[h].astype(BF), TN) for h in hs]
    dr_b = [x.astype(BF) for x in d_r]
    for h in hs:
        left = jnp.concatenate(
            [(q[h] * start[h]).astype(BF), (k[h] * (-(bt[h] * start[h]))).astype(BF)], axis=0
        )
        right = jnp.concatenate([do_b[h], dr_b[h]], axis=0)
        dstate[h] = jnp.exp(end[h]) * ds1[h] + mm(left, right, TN)

    lane = lax.broadcasted_iota(jnp.int32, (rows, LANES), 1)
    sub = lax.broadcasted_iota(jnp.int32, (LANES, rows), 0)
    dab_cols = jnp.zeros((rows, LANES), F32)
    dg_cols = jnp.zeros((rows, LANES), F32)
    dg_rows = jnp.zeros((LANES, rows), F32)
    dend = jnp.zeros((1, LANES), F32)
    lane_one = lax.broadcasted_iota(jnp.int32, (1, LANES), 1)
    for h in hs:
        sl = slice(h * dv, (h + 1) * dv)
        ks = slice(h * dk, (h + 1) * dk)
        d_p = jnp.where(low_inc, mm(do_b[h], u_b[h], NT), 0.0)
        d_a = jnp.where(low_strict, -mm(dr_b[h], u_b[h], NT), 0.0)
        pp = d_p * prob[h]
        dqk_b = (d_p * dec[h]).astype(BF)
        ad = d_a * dkk[h]
        d_kk = d_a * (bt[h] * dec[h])
        d_kk = (d_kk + jnp.transpose(d_kk)).astype(BF)
        y = mm(do_b[h], s0_b[h], NT)
        x = mm(dr_b[h], s0_b[h], NT)
        z = mm(u_b[h], ds1_b[h], NT)
        dq = mm(dqk_b, k_b[h]) + start[h] * y
        bstart = bt[h] * start[h]
        kx = jnp.sum(k[h] * x, axis=-1, keepdims=True)
        kz = tail[h] * jnp.sum(k[h] * z, axis=-1, keepdims=True)
        dkey = mm(d_kk, k_b[h]) + mm(dqk_b, q_b[h], TN) - bstart * x + tail[h] * z
        zval = zv[:, sl]
        sgv = sigmoid(zval)
        val = zval * sgv
        ad_row = jnp.sum(ad, axis=-1, keepdims=True)
        d_beta = jnp.sum(d_r[h] * val, axis=-1, keepdims=True) - start[h] * kx + ad_row
        d_g = (
            jnp.sum(pp, axis=-1, keepdims=True)
            + bt[h] * ad_row
            + start[h] * jnp.sum(q[h] * y, axis=-1, keepdims=True)
            - bstart * kx
            - kz
        )
        d_g_row = -jnp.sum(pp + bt[h] * ad, axis=0, keepdims=True)
        d_end = jnp.sum(kz, axis=0, keepdims=True) + jnp.exp(end[h]) * jnp.sum(
            jnp.sum(s0_b[h].astype(F32) * ds1[h], axis=-1, keepdims=True), axis=0, keepdims=True
        )
        dab_cols = dab_cols + jnp.where(lane == h, d_beta, 0.0)
        dg_cols = dg_cols + jnp.where(lane == heads + h, d_g, 0.0)
        dg_rows = dg_rows + jnp.where(sub == heads + h, d_g_row, 0.0)
        dend = dend + jnp.where(lane_one == heads + h, d_end, 0.0)
        vn[0:rows, sl] = (bt[h] * d_r[h]) * (sgv * (1.0 + zval * (1.0 - sgv)))
        for buf, du, (un, n, slope) in ((qn, dq * scale, qu[h]), (kn, dkey, ku[h])):
            dy = n * (du - un * jnp.sum(un * du, axis=-1, keepdims=True))
            buf[0:rows, ks] = dy * slope

    d_run = dg_cols + jnp.transpose(dg_rows)
    d_decay = exact_mm(jnp.where(col >= row, 1.0, 0.0), d_run) + dend
    pick = (lane >= heads) & (lane < 2 * heads)
    d_decay = jnp.where(pick, d_decay, 0.0)
    d_alpha = d_decay * (-jnp.exp(par_ref[0:1, :])) * sigmoid(ab + par_ref[1:2, :])
    dpar_ref[0:1, :] += jnp.sum(d_decay * decay, axis=0, keepdims=True)
    dpar_ref[1:2, :] += jnp.sum(d_alpha, axis=0, keepdims=True)
    dab_ref[...] = (dab_cols * beta * (1.0 - beta) + d_alpha).astype(BF)

    wide = heads * dk
    for buf, cur, taps, out, at, dtap in (
        (qn, qb, tq_ref, draw_ref, 0, dtq_ref),
        (kn, kb, tk_ref, draw_ref, wide, dtk_ref),
        (vn, vb, tv_ref, draw_ref, 2 * wide, dtv_ref),
    ):
        here = cur[HALO : HALO + rows, :]
        total = None
        for i in range(4):
            moved = buf[3 - i : 3 - i + rows, :]
            term = moved * taps[i : i + 1, :]
            total = term if total is None else total + term
            dtap[i : i + 1, :] += jnp.sum(here * moved, axis=0, keepdims=True)
        out[:, at : at + total.shape[1]] = total.astype(BF)
        buf[rows : rows + HALO, :] = buf[0:HALO, :]


def mixer_specs(heads, dk, dv, at):
    wide_k, wide_v = heads * dk, heads * dv
    full = lambda shape: pl.BlockSpec(shape, lambda c: (0,) * len(shape))
    return {
        "q": pl.BlockSpec((CH, wide_k), lambda c: (at(c), 0)),
        "k": pl.BlockSpec((CH, wide_k), lambda c: (at(c), 1)),
        "val": pl.BlockSpec((CH, wide_v), lambda c: (at(c), 2 * wide_k // wide_v)),
        "og": pl.BlockSpec((CH, wide_v), lambda c: (at(c), 2 * wide_k // wide_v + 1)),
        "raw": pl.BlockSpec((CH, 2 * (wide_k + wide_v)), lambda c: (at(c), 0)),
        "v": pl.BlockSpec((CH, wide_v), lambda c: (at(c), 0)),
        "ab": pl.BlockSpec((CH, LANES), lambda c: (at(c), 0)),
        "t": pl.BlockSpec((CH, heads * CH), lambda c: (at(c), 0)),
        "s": pl.BlockSpec((None, dk, wide_v), lambda c: (at(c), 0, 0)),
        "tk": full((8, wide_k)),
        "tv": full((8, wide_v)),
        "par": full((8, LANES)),
        "gain": full((1, dv)),
    }


def mixer_forward(raw, ab, tq, tk, tv, par, gain):
    length, wide_k, wide_v = raw.shape[0], tq.shape[1], tv.shape[1]
    dv = gain.shape[1]
    heads = wide_v // dv
    dk = wide_k // heads
    steps = length // CH
    sp = mixer_specs(heads, dk, dv, lambda c: c)
    return pl.pallas_call(
        functools.partial(fwd_body, heads, dk, dv),
        grid=(steps,),
        in_specs=[sp[n] for n in ("q", "k", "val", "og", "ab", "tk", "tk", "tv", "par", "gain")],
        out_specs=[sp[n] for n in ("v", "v", "v", "t", "s")],
        out_shape=[
            jax.ShapeDtypeStruct((length, wide_v), BF),
            jax.ShapeDtypeStruct((length, wide_v), F32),
            jax.ShapeDtypeStruct((length, wide_v), BF),
            jax.ShapeDtypeStruct((length, heads * CH), BF),
            jax.ShapeDtypeStruct((steps, dk, wide_v), BF),
        ],
        scratch_shapes=[
            pltpu.VMEM((CH + HALO, wide_k), F32),
            pltpu.VMEM((CH + HALO, wide_k), F32),
            pltpu.VMEM((CH + HALO, wide_v), F32),
            pltpu.VMEM((heads, dk, dv), F32),
        ],
        compiler_params=pltpu.CompilerParams(
            dimension_semantics=("arbitrary",), vmem_limit_bytes=40 << 20
        ),
        cost_estimate=pl.CostEstimate(flops=20_000_000_000, bytes_accessed=40_000_000, transcendentals=6_000_000),
        name="mixer_forward",
    )(raw, raw, raw, raw, ab, tq, tk, tv, par, gain)


def mixer_backward(raw, ab, tq, tk, tv, par, gain, grad, o, u, t, s):
    length, wide_k, wide_v = raw.shape[0], tq.shape[1], tv.shape[1]
    dv = gain.shape[1]
    heads = wide_v // dv
    dk = wide_k // heads
    steps = length // CH
    at = lambda c: steps - 1 - c
    sp = mixer_specs(heads, dk, dv, at)
    before = lambda c: jnp.maximum(at(c) * (CH // HALO) - 1, 0)
    hq = pl.BlockSpec((HALO, wide_k), lambda c: (before(c), 0))
    hk = pl.BlockSpec((HALO, wide_k), lambda c: (before(c), 1))
    hv = pl.BlockSpec((HALO, wide_v), lambda c: (before(c), 2 * wide_k // wide_v))
    names = ("q", "k", "val", "og", "ab")
    rest = ("tk", "tk", "tv", "par", "gain", "v", "v", "v", "t", "s")
    return pl.pallas_call(
        functools.partial(bwd_body, heads, dk, dv),
        grid=(steps,),
        in_specs=[sp[n] for n in names] + [hq, hk, hv] + [sp[n] for n in rest],
        out_specs=[sp[n] for n in ("raw", "ab", "tk", "tk", "tv", "par", "gain")],
        out_shape=[
            jax.ShapeDtypeStruct((length, 2 * (wide_k + wide_v)), BF),
            jax.ShapeDtypeStruct((length, LANES), BF),
            jax.ShapeDtypeStruct((8, wide_k), F32),
            jax.ShapeDtypeStruct((8, wide_k), F32),
            jax.ShapeDtypeStruct((8, wide_v), F32),
            jax.ShapeDtypeStruct((8, LANES), F32),
            jax.ShapeDtypeStruct((1, dv), F32),
        ],
        scratch_shapes=[
            pltpu.VMEM((CH + HALO, wide_k), F32),
            pltpu.VMEM((CH + HALO, wide_k), F32),
            pltpu.VMEM((CH + HALO, wide_v), F32),
            pltpu.VMEM((CH + HALO, wide_k), F32),
            pltpu.VMEM((CH + HALO, wide_k), F32),
            pltpu.VMEM((CH + HALO, wide_v), F32),
            pltpu.VMEM((heads, dk, dv), F32),
        ],
        compiler_params=pltpu.CompilerParams(
            dimension_semantics=("arbitrary",), vmem_limit_bytes=48 << 20
        ),
        cost_estimate=pl.CostEstimate(flops=40_000_000_000, bytes_accessed=60_000_000, transcendentals=9_000_000),
        name="mixer_backward",
    )(
        raw, raw, raw, raw, ab, raw, raw, raw, tq, tk, tv, par, gain, grad, o, u, t, s
    )


def on_dp(index):
    return {"dp": index}


def greet(peers):
    barrier = pltpu.get_barrier_semaphore()
    for peer in peers:
        pl.semaphore_signal(barrier, inc=1, device_id=on_dp(peer))
    pl.semaphore_wait(barrier, len(peers))


GATHER_CHUNKS = 8


def gather_body(w_ref, small_ref, full_ref, all_ref, right_s, left_s, swap_s, arrive, few_s, few_r, local):
    me = lax.axis_index("dp")
    outer, side = me // 2, me % 2
    block = w_ref.shape[0]
    part = block // GATHER_CHUNKS
    greet([(me + j) % 8 for j in range(1, 8)])
    keep = pltpu.make_async_copy(w_ref, full_ref.at[pl.ds(0, block)], local.at[0])
    keep.start()
    keep_few = pltpu.make_async_copy(small_ref, all_ref.at[0], local.at[1])
    keep_few.start()

    def few(j):
        peer = (me + j) % 8
        slot = (outer - peer // 2 + 4) % 4 + 4 * ((side + peer % 2) % 2)
        return pltpu.make_async_remote_copy(
            small_ref, all_ref.at[slot], few_s.at[j - 1], few_r.at[j - 1], device_id=on_dp(peer)
        )

    for j in range(1, 8):
        few(j).start()

    def spot(slot, c):
        return full_ref.at[pl.ds(slot * block + c * part, part)]

    def source(slot, c):
        return w_ref.at[pl.ds(c * part, part)] if slot == 0 else spot(slot, c)

    def to_right(h, c):
        return pltpu.make_async_remote_copy(
            source((4 - h) % 4, c), spot(3 - h, c), right_s.at[h, c], arrive.at[3 - h, c], device_id=on_dp((me + 2) % 8)
        )

    def to_left(h, c):
        return pltpu.make_async_remote_copy(
            source(h, c), spot(h + 1, c), left_s.at[h, c], arrive.at[h + 1, c], device_id=on_dp((me + 6) % 8)
        )

    def to_side(slot, c):
        return pltpu.make_async_remote_copy(
            source(slot, c), spot(4 + slot, c), swap_s.at[slot, c], arrive.at[4 + slot, c],
            device_id=on_dp(me + 1 - 2 * side),
        )

    def landed(slot, c):
        pltpu.make_async_copy(spot(slot, c), spot(slot, c), arrive.at[slot, c]).wait()

    def step(i, carry):
        @pl.when(i < GATHER_CHUNKS)
        def _():
            to_side(0, i).start()

            @pl.when(outer < 3)
            def _():
                to_right(0, i).start()

            @pl.when(outer > 0)
            def _():
                to_left(0, i).start()

        for h in range(1, 4):
            c = i - h

            @pl.when((c >= 0) & (c < GATHER_CHUNKS) & (outer >= h))
            def _():
                landed(4 - h, c)
                if h < 3:
                    @pl.when(outer < 3)
                    def _():
                        to_right(h, c).start()

                to_side(4 - h, c).start()

            @pl.when((c >= 0) & (c < GATHER_CHUNKS) & (outer + h < 4))
            def _():
                landed(h, c)
                if h < 3:
                    @pl.when(outer > 0)
                    def _():
                        to_left(h, c).start()

                to_side(h, c).start()

        return carry

    lax.fori_loop(0, GATHER_CHUNKS + 3, step, 0)

    def finish(c, carry):
        for slot in range(4):
            to_side(slot, c).wait_send()
            landed(4 + slot, c)
        for h in range(3):
            @pl.when((outer >= h) & (outer < 3))
            def _():
                to_right(h, c).wait_send()

            @pl.when((outer + h < 4) & (outer > 0))
            def _():
                to_left(h, c).wait_send()

        return carry

    lax.fori_loop(0, GATHER_CHUNKS, finish, 0)
    for j in range(1, 8):
        few(j).wait()
    keep.wait()
    keep_few.wait()


def ring_gather(w, small):
    n = GATHER_CHUNKS
    any_ref = pl.BlockSpec(memory_space=pl.ANY)
    return pl.pallas_call(
        gather_body,
        in_specs=[any_ref] * 2,
        out_specs=[any_ref] * 2,
        out_shape=[
            jax.ShapeDtypeStruct((8 * w.shape[0], w.shape[1]), w.dtype),
            jax.ShapeDtypeStruct((8,) + small.shape, small.dtype),
        ],
        scratch_shapes=[
            pltpu.SemaphoreType.DMA((3, n)),
            pltpu.SemaphoreType.DMA((3, n)),
            pltpu.SemaphoreType.DMA((4, n)),
            pltpu.SemaphoreType.DMA((8, n)),
            pltpu.SemaphoreType.DMA((7,)),
            pltpu.SemaphoreType.DMA((7,)),
            pltpu.SemaphoreType.DMA((2,)),
        ],
        compiler_params=pltpu.CompilerParams(collective_id=0, has_side_effects=True),
        cost_estimate=pl.CostEstimate(flops=0, bytes_accessed=400_000_000, transcendentals=0),
        name="ring_gather",
    )(w, small)


def plain_dot(left_mat, right_mat):
    return jnp.dot(left_mat, right_mat, preferred_element_type=F32)


def dot_rows(left_mat, right_mat):
    return lax.dot_general(left_mat, right_mat, (((1,), (1,)), ((), ())), preferred_element_type=F32)


def dot_tokens(left_mat, right_mat):
    return lax.dot_general(left_mat, right_mat, (((0,), (0,)), ((), ())), preferred_element_type=F32)


def rms_apply(values, gain_vec):
    return values * lax.rsqrt(jnp.mean(values * values, axis=-1, keepdims=True) + 1e-05) * gain_vec


def swiglu(gate_pre, up_pre):
    return jax.nn.silu(gate_pre) * up_pre


class RingRows:
    def __init__(self, dp_size):
        self.outer = dp_size // 2
        self.index = lax.axis_index("dp")

    def _roll(self, x, axis, blocks):
        size = x.shape[axis] // self.outer * blocks
        return jnp.concatenate(
            [lax.slice_in_dim(x, size, None, axis=axis), lax.slice_in_dim(x, 0, size, axis=axis)], axis
        )

    def reorder(self, x, axis):
        outer_at, pair_at = self.index // 2, self.index % 2
        size = x.shape[axis] // (2 * self.outer)
        cut = [lax.slice_in_dim(x, b * size, (b + 1) * size, axis=axis) for b in range(2 * self.outer)]
        even, odd = jnp.concatenate(cut[0::2], axis), jnp.concatenate(cut[1::2], axis)
        sides = [jnp.where(pair_at == 0, even, odd), jnp.where(pair_at == 0, odd, even)]
        bit = 1
        while bit < self.outer:
            sides = [jnp.where((outer_at // bit) % 2 == 1, self._roll(s, axis, bit), s) for s in sides]
            bit *= 2
        return jnp.concatenate(sides, axis)

    def restore(self, x, axis):
        outer_at, pair_at = self.index // 2, self.index % 2
        half = x.shape[axis] // 2
        sides = [lax.slice_in_dim(x, 0, half, axis=axis), lax.slice_in_dim(x, half, None, axis=axis)]
        bit = 1
        while bit < self.outer:
            sides = [
                jnp.where((outer_at // bit) % 2 == 1, self._roll(s, axis, self.outer - bit), s) for s in sides
            ]
            bit *= 2
        even = jnp.where(pair_at == 0, sides[0], sides[1])
        odd = jnp.where(pair_at == 0, sides[1], sides[0])
        size = half // self.outer
        cut = []
        for b in range(self.outer):
            cut += [lax.slice_in_dim(s, b * size, (b + 1) * size, axis=axis) for s in (even, odd)]
        return jnp.concatenate(cut, axis)

    def _swap(self, x):
        return lax.ppermute(x, "dp", [(i, i ^ 1) for i in range(2 * self.outer)])

    def _from(self, x, steps):
        n = 2 * self.outer
        return lax.ppermute(x, "dp", [((i + 2 * steps) % n, i) for i in range(n)])

    def along(self, block):
        return [block] + [self._from(block, k) for k in range(1, self.outer)]

    def across(self, blocks):
        return blocks + [self._swap(b) for b in blocks]

    def gather_first(self, w, small):
        return ring_gather(w, small)

    def scatter_small(self, parts):
        pair = parts[: self.outer] + self._swap(parts[self.outer :])
        n = 2 * self.outer
        total = pair[:1]
        for k in range(1, self.outer):
            total = total + lax.ppermute(pair[k : k + 1], "dp", [(i, (i + 2 * k) % n) for i in range(n)])
        return total[0]

    def sum_all(self, vec, tensor_size):
        for axis, size in (("tensor", tensor_size), ("dp", 2 * self.outer)):
            step = 1
            while step < size:
                vec = vec + lax.ppermute(vec, axis, [(i, i ^ step) for i in range(size)])
                step *= 2
        return vec

    def begin(self, left, right):
        return self._swap(dot_tokens(left[:, left.shape[1] // 2 :], right).astype(BF))

    def middle(self, left, right, came):
        mine = dot_tokens(left[:, : left.shape[1] // 2], right)
        return (mine + came.astype(F32)).astype(BF)

    def end(self, pair):
        size = pair.shape[0] // self.outer
        n = 2 * self.outer
        total = pair[:size].astype(F32)
        for k in range(1, self.outer):
            piece = pair[k * size : (k + 1) * size]
            total = total + lax.ppermute(piece, "dp", [(i, (i + 2 * k) % n) for i in range(n)]).astype(F32)
        return total

    def along(self, block):
        return [block] + [self._from(block, k) for k in range(1, self.outer)]

    def across(self, blocks):
        return blocks + [self._swap(b) for b in blocks]

    def gather_first(self, w, small):
        return ring_gather(w, small)

    def scatter_small(self, parts):
        pair = parts[: self.outer] + self._swap(parts[self.outer :])
        n = 2 * self.outer
        total = pair[:1]
        for k in range(1, self.outer):
            total = total + lax.ppermute(pair[k : k + 1], "dp", [(i, (i + 2 * k) % n) for i in range(n)])
        return total[0]

    def sum_all(self, vec, tensor_size):
        for axis, size in (("tensor", tensor_size), ("dp", 2 * self.outer)):
            step = 1
            while step < size:
                vec = vec + lax.ppermute(vec, axis, [(i, i ^ step) for i in range(size)])
                step *= 2
        return vec

    def scatter(self, left, right):
        half = left.shape[1] // 2
        sent = dot_tokens(left[:, half:], right).astype(BF)
        came = self._swap(sent)
        pair = (dot_tokens(left[:, :half], right) + came.astype(F32)).astype(BF)
        size = half // self.outer
        n = 2 * self.outer
        total = pair[:size].astype(F32)
        for k in range(1, self.outer):
            piece = pair[k * size : (k + 1) * size]
            total = total + lax.ppermute(
                piece, "dp", [(i, (i + 2 * k) % n) for i in range(n)]
            ).astype(F32)
        return total


class PlainRows:
    def reorder(self, x, axis):
        return x

    def restore(self, x, axis):
        return x

    def along(self, block):
        return [block]

    def across(self, blocks):
        return [lax.all_gather(blocks[0], "dp", axis=0, tiled=True)]

    def begin(self, left, right):
        return dot_tokens(left, right).astype(BF)

    def middle(self, left, right, came):
        return came

    def end(self, pair):
        return lax.psum_scatter(pair, "dp", scatter_dimension=0, tiled=True).astype(F32)

    def gather_first(self, w, small):
        return lax.all_gather(w, "dp", axis=0, tiled=True), lax.all_gather(small, "dp", axis=0)

    def scatter_small(self, parts):
        return lax.psum_scatter(parts, "dp", scatter_dimension=0, tiled=True)[0]

    def sum_all(self, vec, tensor_size):
        return lax.psum(vec, ("dp", "tensor"))

    def scatter(self, left, right):
        full = dot_tokens(left, right).astype(BF)
        return lax.psum_scatter(full, "dp", scatter_dimension=0, tiled=True).astype(F32)


def tie(value, *others):
    return lax.optimization_barrier((value, others))[0]


def tensor_gather(x):
    return lax.all_gather(x, "tensor", axis=0, tiled=True)


def tensor_scatter(x):
    return lax.psum_scatter(x, "tensor", scatter_dimension=0, tiled=True)


def shards(
    dp_size, tensor_size, inputs, cotangent, lengths, norm1_gain, w_query, w_key, w_value, w_outgate, w_beta, w_alpha,
    conv_query, conv_key, conv_value, a_log, dt_bias, head_gain, w_out, norm2_gain, w_gate, w_up, w_down,
):
    rows = RingRows(dp_size) if dp_size == 8 else PlainRows()
    heads = w_beta.shape[1]
    wide_k, wide_v = w_query.shape[1], w_value.shape[1]
    dk, dv = wide_k // heads, wide_v // heads
    taps_n = conv_query.shape[2]
    block = w_query.shape[0]
    tensor_pos = lax.axis_index("tensor")
    head_start = tensor_pos * heads

    row_count = inputs.shape[1]
    positions = tensor_pos * row_count + jnp.arange(row_count, dtype=jnp.int32)
    valid_rows = (positions < lengths[0]).astype(F32)[:, None]

    small = jnp.concatenate(
        [w_beta.reshape(-1), w_alpha.reshape(-1), conv_query.reshape(-1), conv_key.reshape(-1), conv_value.reshape(-1)]
    )
    cuts = [0]
    for part in (w_beta, w_alpha, conv_query, conv_key, conv_value):
        cuts.append(cuts[-1] + part.size)
    small = jnp.pad(small, (0, -small.size % (32 * LANES))).reshape(-1, LANES)
    full_raw, small = rows.gather_first(
        jnp.concatenate([w_query, w_key, w_value, w_outgate], axis=1), small
    )
    small = small.reshape(dp_size, -1)
    pieces = [small[:, a:b] for a, b in zip(cuts[:-1], cuts[1:])]
    full_ab = jnp.concatenate([p.reshape(dp_size * block, heads) for p in pieces[:2]], axis=1)
    full_ab = jnp.pad(full_ab, ((0, 0), (0, LANES - 2 * heads)))

    def tap_table(piece, size):
        table = rows.restore(piece, 0).reshape(size, heads, taps_n).astype(F32)
        return jnp.pad(jnp.transpose(table, (2, 1, 0)).reshape(taps_n, heads * size), ((0, 8 - taps_n), (0, 0)))

    tq, tk, tv = tap_table(pieces[2], dk), tap_table(pieces[3], dk), tap_table(pieces[4], dv)
    alog_local = lax.dynamic_slice_in_dim(a_log, head_start, heads)
    dtb_local = lax.dynamic_slice_in_dim(dt_bias, head_start, heads)
    par = jnp.pad(jnp.stack([alog_local, dtb_local]), ((0, 6), (heads, LANES - 2 * heads)))
    gain = head_gain[None]

    local_rows = rows.reorder(inputs[0], 1).astype(F32)
    gain_one = rows.reorder(norm1_gain[None], 1)[0]
    gain_two = rows.reorder(norm2_gain[None], 1)[0]
    normed_one, norm_one_back = jax.vjp(rms_apply, local_rows, gain_one)
    rows_one = tensor_gather(normed_one.astype(BF))
    line_out = rows.along(tie(w_out, full_raw))
    line_gate = rows.along(tie(w_gate, full_raw))
    grad_after = valid_rows * rows.reorder(cotangent[0], 1).astype(F32)
    incoming_ffn = tensor_gather(grad_after.astype(BF))

    ab_raw = plain_dot(rows_one, full_ab)
    core_in = (plain_dot(rows_one, full_raw), ab_raw, tq, tk, tv, par, gain)
    head_bf, delta_out, new_values, inverses, states = mixer_forward(*core_in)
    line_out = tie(line_out, head_bf)
    line_up = rows.along(tie(w_up, line_out))
    full_out = jnp.concatenate(rows.across(line_out), axis=0)
    mixed = dot_rows(head_bf, full_out).astype(BF)
    line_gate = tie(line_gate, mixed)
    line_down = rows.along(tie(w_down, line_gate))
    all_gate = rows.across(line_gate)
    after_mix = local_rows + tensor_scatter(mixed).astype(F32)
    normed_two, norm_two_back = jax.vjp(rms_apply, after_mix, gain_two)
    normed_two = normed_two.astype(BF)
    all_up = rows.across(tie(line_up, normed_two))
    rows_two = tensor_gather(normed_two)
    full_gate = jnp.concatenate(tie(all_gate, normed_two), axis=0)
    gate_pre = plain_dot(rows_two, full_gate)
    all_down = rows.across(tie(line_down, gate_pre))
    full_up = jnp.concatenate(tie(all_up, gate_pre), axis=0)
    up_pre = plain_dot(rows_two, full_up)
    hidden, swiglu_back = jax.vjp(swiglu, gate_pre, up_pre)
    hidden_bf = hidden.astype(BF)

    swap_down = rows.begin(incoming_ffn, hidden_bf)
    full_down = jnp.concatenate(tie(all_down, hidden_bf), axis=0)
    grad_hidden = plain_dot(incoming_ffn, full_down)
    grad_gate_pre, grad_up_pre = swiglu_back(grad_hidden)
    gate_low = grad_gate_pre.astype(BF)
    up_low = grad_up_pre.astype(BF)
    back_two = (dot_rows(gate_low, full_gate) + dot_rows(up_low, full_up)).astype(BF)
    grad_normed_two = tensor_scatter(back_two)
    late_two = tie(rows_two, back_two)
    swap_gate = rows.begin(late_two, gate_low)
    swap_up = rows.begin(late_two, up_low)
    pair_down = rows.middle(tie(incoming_ffn, back_two), hidden_bf, swap_down)
    grad_normed_two = tie(grad_normed_two, pair_down).astype(F32)
    out_down = rows.end(pair_down)
    grad_mid, grad_norm2 = norm_two_back(grad_normed_two)
    grad_mid = grad_mid + grad_after
    grad_mix = grad_mid.astype(BF)
    incoming_mix = tensor_gather(grad_mix)

    grad_head = plain_dot(incoming_mix, full_out)
    pair_gate = rows.middle(late_two, gate_low, tie(swap_gate, grad_head))
    out_gate = rows.end(pair_gate)
    swap_out = rows.begin(incoming_mix, head_bf)
    grad_head = tie(grad_head, pair_gate)
    raw_low, ab_low, dtq, dtk, dtv, dpar, dgain = mixer_backward(
        *core_in, grad_head, delta_out, new_values, inverses, states
    )
    ffn_part = tensor_scatter(dot_rows(tie(hidden_bf, grad_mix), full_down).astype(BF)).astype(F32)
    outputs = rows.restore(((after_mix + ffn_part) * valid_rows).astype(BF), 1)[None]
    pair_up = rows.middle(late_two, up_low, tie(swap_up, raw_low))
    out_up = rows.end(pair_up)
    raw_low = tie(raw_low, pair_up)
    summed = (dot_rows(raw_low, full_raw) + dot_rows(ab_low, full_ab)).astype(BF)
    grad_normed_one = tensor_scatter(summed)
    pair_out = rows.middle(incoming_mix, head_bf, tie(swap_out, summed))
    out_out = rows.end(pair_out)
    wide = 2 * wide_k
    late_raw = tie(raw_low, summed)
    parts = [late_raw[:, :wide], late_raw[:, wide : wide + wide_v], late_raw[:, wide + wide_v :]]
    swaps = [rows.begin(rows_one, p) for p in parts]
    out_qk, out_value, out_outgate = (
        rows.end(rows.middle(rows_one, p, came)) for p, came in zip(parts, swaps)
    )
    grad_first, grad_norm1 = norm_one_back(tie(grad_normed_one, swaps).astype(F32))
    grad_inputs = rows.restore(grad_mid + grad_first, 1)[None]

    grad_ab = dot_tokens(rows_one, ab_low)[:, : 2 * heads]

    def tap_grad(table, size):
        grad = jnp.transpose(table[:taps_n].reshape(taps_n, heads, size), (2, 1, 0))
        return rows.reorder(grad.reshape(dp_size, -1), 0)

    small_out = [grad_ab[:, :heads].reshape(dp_size, -1), grad_ab[:, heads:].reshape(dp_size, -1)]
    small_out += [tap_grad(dtq, dk), tap_grad(dtk, dk), tap_grad(dtv, dv)]
    small_sum = rows.scatter_small(jnp.concatenate(small_out, axis=1))
    shapes = (w_beta, w_alpha, conv_query, conv_key, conv_value)
    out_beta, out_alpha, out_cq, out_ck, out_cv = (
        small_sum[a:b].reshape(like.shape) for a, b, like in zip(cuts[:-1], cuts[1:], shapes)
    )
    alog_full, dtb_full = (
        lax.dynamic_update_slice_in_dim(jnp.zeros_like(a_log), dpar[i, heads : 2 * heads], head_start, 0)
        for i in range(2)
    )
    vec = [rows.restore(grad_norm1[None], 1)[0], rows.restore(grad_norm2[None], 1)[0], dgain[0], alog_full, dtb_full]
    total = rows.sum_all(jnp.concatenate(vec), tensor_size)
    ends = [0]
    for part in vec:
        ends.append(ends[-1] + part.size)
    norm1_sum, norm2_sum, hgain_sum, alog_sum, dtb_sum = (total[a:b] for a, b in zip(ends[:-1], ends[1:]))
    return (
        outputs, grad_inputs, norm1_sum, out_qk[:, :wide_k], out_qk[:, wide_k:], out_value, out_outgate,
        out_beta, out_alpha, out_cq, out_ck, out_cv, alog_sum, dtb_sum, hgain_sum, out_out, norm2_sum,
        out_gate, out_up, out_down,
    )


def solution(mesh):
    mat, cube, whole = P("dp", "tensor"), P("dp", "tensor", None), P()
    in_specs = (
        (cube, cube, P("dp"), whole) + (mat,) * 6 + (cube,) * 3 + (whole,) * 3 + (mat, whole) + (mat,) * 3
    )
    out_specs = (
        (cube, cube, whole) + (mat,) * 6 + (cube,) * 3 + (whole,) * 3 + (mat, whole) + (mat,) * 3
    )
    return jax.shard_map(
        functools.partial(shards, mesh.shape["dp"], mesh.shape["tensor"]), mesh=mesh, in_specs=in_specs, out_specs=out_specs,
        check_vma=False,
    )
```

```python
import functools

import jax
import jax.numpy as jnp
from jax import lax
from jax.experimental import pallas as pl
from jax.experimental.pallas import tpu as pltpu
from jax.sharding import PartitionSpec as P

CH = 128
HALO = 8
LANES = 128
F32 = jnp.float32
BF = jnp.bfloat16


def mm(a, b, dims=((1,), (0,))):
    return lax.dot_general(a, b, (dims, ((), ())), preferred_element_type=F32)


NT = ((1,), (1,))
TN = ((0,), (0,))


def split(x):
    hi = x.astype(BF)
    return hi, (x - hi.astype(F32)).astype(BF)


def mm3(a, b):
    return mm(a[0], b[0]) + (mm(a[0], b[1]) + mm(a[1], b[0]))


def exact_mm(a, b):
    return lax.dot_general(
        a, b, (((1,), (0,)), ((), ())), precision=lax.Precision.HIGHEST, preferred_element_type=F32
    )


def unit_lower_inverse(mats):
    n = mats[0].shape[0]
    row = lax.broadcasted_iota(jnp.int32, (n, n), 0)
    col = lax.broadcasted_iota(jnp.int32, (n, n), 1)

    def off_block(size):
        same = (row // (2 * size)) == (col // (2 * size))
        return same & ((row // size) % 2 == 1) & ((col // size) % 2 == 0)

    eye = jnp.where(row == col, 1.0, 0.0)
    inv = [eye - jnp.where(off_block(1), a, 0.0) for a in mats]
    size = 2
    while size < n:
        mask = off_block(size)
        halves = [split(x) for x in inv]
        low = [split(jnp.where(mask, a, 0.0)) for a in mats]
        mid = [split(mm3(b, x)) for b, x in zip(low, halves)]
        inv = [x - mm3(xs, y) for x, xs, y in zip(inv, halves, mid)]
        size *= 2
    return inv


def softplus(x):
    return jnp.maximum(x, 0.0) + jnp.log1p(jnp.exp(-jnp.abs(x)))


def sigmoid(x):
    return 1.0 / (1.0 + jnp.exp(-x))


def conv_of(buf, taps, rows):
    out = buf[HALO - 3 : HALO - 3 + rows, :] * taps[0:1, :]
    for i in range(1, 4):
        out = out + buf[HALO - 3 + i : HALO - 3 + i + rows, :] * taps[i : i + 1, :]
    return out


def decay_tables(ab, par, rows):
    beta = sigmoid(ab)
    decay = -jnp.exp(par[0:1, :]) * softplus(ab + par[1:2, :])
    row = lax.broadcasted_iota(jnp.int32, (rows, rows), 0)
    col = lax.broadcasted_iota(jnp.int32, (rows, rows), 1)
    run = exact_mm(jnp.where(row >= col, 1.0, 0.0), decay)
    return beta, decay, run, jnp.transpose(run), row, col


def fwd_body(
    heads, dk, dv, q_ref, k_ref, v_ref, og_ref, ab_ref, tq_ref, tk_ref, tv_ref, par_ref, gain_ref,
    head_ref, o_ref, u_ref, t_ref, s_ref, qb, kb, vb, state,
):
    rows = CH

    @pl.when(pl.program_id(0) == 0)
    def _():
        for buf in (qb, kb, vb):
            buf[0:HALO, :] = jnp.zeros((HALO, buf.shape[1]), F32)
        state[...] = jnp.zeros_like(state)

    hs = range(heads)
    raw = []
    for buf, ref, taps in ((qb, q_ref, tq_ref), (kb, k_ref, tk_ref), (vb, v_ref, tv_ref)):
        buf[HALO : HALO + rows, :] = ref[...]
        raw.append(conv_of(buf, taps, rows))
        buf[0:HALO, :] = buf[rows : rows + HALO, :]
    zq, zk, zv = raw
    beta, _, run, run_t, row, col = decay_tables(ab_ref[...], par_ref, rows)
    low_inc = row >= col
    low_strict = row > col
    scale = dk ** (-0.5)

    def unit(z):
        y = z * sigmoid(z)
        return y * lax.rsqrt(jnp.sum(y * y, axis=-1, keepdims=True) + 1e-6)

    q = [unit(zq[:, h * dk : (h + 1) * dk]) * scale for h in hs]
    k = [unit(zk[:, h * dk : (h + 1) * dk]) for h in hs]
    qk_b = [(a.astype(BF), b.astype(BF)) for a, b in zip(q, k)]
    bt = [beta[:, h : h + 1] for h in hs]
    g_col = [run[:, heads + h : heads + h + 1] for h in hs]
    g_row = [run_t[heads + h : heads + h + 1, :] for h in hs]
    dec = [jnp.where(low_inc, jnp.exp(jnp.where(low_inc, g_col[h] - g_row[h], 0.0)), 0.0) for h in hs]
    kk = [mm(qk_b[h][1], qk_b[h][1], NT) for h in hs]
    inv = unit_lower_inverse([jnp.where(low_strict, bt[h] * dec[h] * kk[h], 0.0) for h in hs])
    inv_b = [x.astype(BF) for x in inv]
    p_b = [(mm(qk_b[h][0], qk_b[h][1], NT) * dec[h]).astype(BF) for h in hs]
    start = [jnp.exp(g) for g in g_col]
    end = [run[rows - 1 : rows, heads + h : heads + h + 1] for h in hs]
    s0 = [state[h] for h in hs]
    s0_b = [x.astype(BF) for x in s0]
    for h in hs:
        t_ref[:, h * rows : (h + 1) * rows] = inv_b[h]
        s_ref[:, h * dv : (h + 1) * dv] = s0_b[h]
    rhs = []
    for h in hs:
        z = zv[:, h * dv : (h + 1) * dv]
        val = z * sigmoid(z)
        rhs.append((bt[h] * val - (bt[h] * start[h]) * mm(qk_b[h][1], s0_b[h])).astype(BF))
    u_b = [mm(inv_b[h], rhs[h]).astype(BF) for h in hs]
    for h in hs:
        u_ref[:, h * dv : (h + 1) * dv] = u_b[h]
        tail = (k[h] * jnp.exp(end[h] - g_col[h])).astype(BF)
        state[h] = jnp.exp(end[h]) * s0[h] + mm(tail, u_b[h], TN)
    for h in hs:
        o = start[h] * mm(qk_b[h][0], s0_b[h]) + mm(p_b[h], u_b[h])
        o_ref[:, h * dv : (h + 1) * dv] = o
        og = og_ref[:, h * dv : (h + 1) * dv]
        r = lax.rsqrt(jnp.mean(o * o, axis=-1, keepdims=True) + 1e-5)
        head_ref[:, h * dv : (h + 1) * dv] = (o * r * gain_ref[...] * (og * sigmoid(og))).astype(BF)


def bwd_body(
    heads, dk, dv, q_ref, k_ref, v_ref, og_ref, ab_ref, qh_ref, kh_ref, vh_ref,
    tq_ref, tk_ref, tv_ref, par_ref, gain_ref, g_ref, o_ref, u_ref, t_ref, s_ref,
    draw_ref, dab_ref, dtq_ref, dtk_ref, dtv_ref, dpar_ref, dgain_ref,
    qb, kb, vb, qn, kn, vn, dstate,
):
    rows = CH
    step = pl.program_id(0)
    first = step == 0
    is_top = step == pl.num_programs(0) - 1

    @pl.when(first)
    def _():
        for buf in (qn, kn, vn):
            buf[rows : rows + HALO, :] = jnp.zeros((HALO, buf.shape[1]), F32)
        for ref in (dtq_ref, dtk_ref, dtv_ref, dpar_ref, dgain_ref, dstate):
            ref[...] = jnp.zeros_like(ref)

    hs = range(heads)
    raw = []
    for buf, ref, halo, taps in (
        (qb, q_ref, qh_ref, tq_ref), (kb, k_ref, kh_ref, tk_ref), (vb, v_ref, vh_ref, tv_ref)
    ):
        buf[0:HALO, :] = jnp.where(is_top, 0.0, halo[...])
        buf[HALO : HALO + rows, :] = ref[...]
        raw.append(conv_of(buf, taps, rows))
    zq, zk, zv = raw
    ab = ab_ref[...]
    beta, decay, run, run_t, row, col = decay_tables(ab, par_ref, rows)
    low_inc = row >= col
    low_strict = row > col
    scale = dk ** (-0.5)

    def unit(z):
        sg = sigmoid(z)
        y = z * sg
        n = lax.rsqrt(jnp.sum(y * y, axis=-1, keepdims=True) + 1e-6)
        return y * n, n, sg * (1.0 + z * (1.0 - sg))

    qu = [unit(zq[:, h * dk : (h + 1) * dk]) for h in hs]
    ku = [unit(zk[:, h * dk : (h + 1) * dk]) for h in hs]
    q = [x[0] * scale for x in qu]
    k = [x[0] for x in ku]
    q_b = [x.astype(BF) for x in q]
    k_b = [x.astype(BF) for x in k]
    bt = [beta[:, h : h + 1] for h in hs]
    g_col = [run[:, heads + h : heads + h + 1] for h in hs]
    g_row = [run_t[heads + h : heads + h + 1, :] for h in hs]
    dec = [jnp.where(low_inc, jnp.exp(jnp.where(low_inc, g_col[h] - g_row[h], 0.0)), 0.0) for h in hs]
    start = [jnp.exp(g) for g in g_col]
    end = [run[rows - 1 : rows, heads + h : heads + h + 1] for h in hs]
    tail = [jnp.exp(end[h] - g_col[h]) for h in hs]
    dkk = [mm(k_b[h], k_b[h], NT) * dec[h] for h in hs]
    prob = [mm(q_b[h], k_b[h], NT) * dec[h] for h in hs]
    u_b = [u_ref[:, h * dv : (h + 1) * dv] for h in hs]
    s0_b = [s_ref[:, h * dv : (h + 1) * dv] for h in hs]
    ds1 = [dstate[h] for h in hs]
    ds1_b = [x.astype(BF) for x in ds1]

    gain = gain_ref[...]
    og_at = 2 * heads * dk + heads * dv
    do_b = []
    dgain = jnp.zeros_like(gain)
    for h in hs:
        sl = slice(h * dv, (h + 1) * dv)
        o = o_ref[:, sl]
        og = og_ref[:, sl]
        g = g_ref[:, sl]
        r = lax.rsqrt(jnp.mean(o * o, axis=-1, keepdims=True) + 1e-5)
        sg = sigmoid(og)
        gor = g * (o * r)
        dgain = dgain + jnp.sum(gor * (og * sg), axis=0, keepdims=True)
        draw_ref[:, og_at + h * dv : og_at + (h + 1) * dv] = (gor * gain * (sg * (1.0 + og * (1.0 - sg)))).astype(BF)
        m = g * gain * (og * sg)
        d_o = r * m - o * (r * r * r * jnp.mean(m * o, axis=-1, keepdims=True))
        do_b.append(d_o.astype(BF))
    dgain_ref[...] += dgain

    d_u = [
        mm(prob[h].astype(BF), do_b[h], TN) + mm((k[h] * tail[h]).astype(BF), ds1_b[h]) for h in hs
    ]
    d_r = [mm(t_ref[:, h * rows : (h + 1) * rows], d_u[h].astype(BF), TN) for h in hs]
    dr_b = [x.astype(BF) for x in d_r]
    for h in hs:
        left = jnp.concatenate(
            [(q[h] * start[h]).astype(BF), (k[h] * (-(bt[h] * start[h]))).astype(BF)], axis=0
        )
        right = jnp.concatenate([do_b[h], dr_b[h]], axis=0)
        dstate[h] = jnp.exp(end[h]) * ds1[h] + mm(left, right, TN)

    lane = lax.broadcasted_iota(jnp.int32, (rows, LANES), 1)
    sub = lax.broadcasted_iota(jnp.int32, (LANES, rows), 0)
    dab_cols = jnp.zeros((rows, LANES), F32)
    dg_cols = jnp.zeros((rows, LANES), F32)
    dg_rows = jnp.zeros((LANES, rows), F32)
    dend = jnp.zeros((1, LANES), F32)
    lane_one = lax.broadcasted_iota(jnp.int32, (1, LANES), 1)
    for h in hs:
        sl = slice(h * dv, (h + 1) * dv)
        ks = slice(h * dk, (h + 1) * dk)
        d_p = jnp.where(low_inc, mm(do_b[h], u_b[h], NT), 0.0)
        d_a = jnp.where(low_strict, -mm(dr_b[h], u_b[h], NT), 0.0)
        pp = d_p * prob[h]
        dqk_b = (d_p * dec[h]).astype(BF)
        ad = d_a * dkk[h]
        d_kk = d_a * (bt[h] * dec[h])
        d_kk = (d_kk + jnp.transpose(d_kk)).astype(BF)
        y = mm(do_b[h], s0_b[h], NT)
        x = mm(dr_b[h], s0_b[h], NT)
        z = mm(u_b[h], ds1_b[h], NT)
        dq = mm(dqk_b, k_b[h]) + start[h] * y
        bstart = bt[h] * start[h]
        kx = jnp.sum(k[h] * x, axis=-1, keepdims=True)
        kz = tail[h] * jnp.sum(k[h] * z, axis=-1, keepdims=True)
        dkey = mm(d_kk, k_b[h]) + mm(dqk_b, q_b[h], TN) - bstart * x + tail[h] * z
        zval = zv[:, sl]
        sgv = sigmoid(zval)
        val = zval * sgv
        ad_row = jnp.sum(ad, axis=-1, keepdims=True)
        d_beta = jnp.sum(d_r[h] * val, axis=-1, keepdims=True) - start[h] * kx + ad_row
        d_g = (
            jnp.sum(pp, axis=-1, keepdims=True)
            + bt[h] * ad_row
            + start[h] * jnp.sum(q[h] * y, axis=-1, keepdims=True)
            - bstart * kx
            - kz
        )
        d_g_row = -jnp.sum(pp + bt[h] * ad, axis=0, keepdims=True)
        d_end = jnp.sum(kz, axis=0, keepdims=True) + jnp.exp(end[h]) * jnp.sum(
            jnp.sum(s0_b[h].astype(F32) * ds1[h], axis=-1, keepdims=True), axis=0, keepdims=True
        )
        dab_cols = dab_cols + jnp.where(lane == h, d_beta, 0.0)
        dg_cols = dg_cols + jnp.where(lane == heads + h, d_g, 0.0)
        dg_rows = dg_rows + jnp.where(sub == heads + h, d_g_row, 0.0)
        dend = dend + jnp.where(lane_one == heads + h, d_end, 0.0)
        vn[0:rows, sl] = (bt[h] * d_r[h]) * (sgv * (1.0 + zval * (1.0 - sgv)))
        for buf, du, (un, n, slope) in ((qn, dq * scale, qu[h]), (kn, dkey, ku[h])):
            dy = n * (du - un * jnp.sum(un * du, axis=-1, keepdims=True))
            buf[0:rows, ks] = dy * slope

    d_run = dg_cols + jnp.transpose(dg_rows)
    d_decay = exact_mm(jnp.where(col >= row, 1.0, 0.0), d_run) + dend
    pick = (lane >= heads) & (lane < 2 * heads)
    d_decay = jnp.where(pick, d_decay, 0.0)
    d_alpha = d_decay * (-jnp.exp(par_ref[0:1, :])) * sigmoid(ab + par_ref[1:2, :])
    dpar_ref[0:1, :] += jnp.sum(d_decay * decay, axis=0, keepdims=True)
    dpar_ref[1:2, :] += jnp.sum(d_alpha, axis=0, keepdims=True)
    dab_ref[...] = (dab_cols * beta * (1.0 - beta) + d_alpha).astype(BF)

    wide = heads * dk
    for buf, cur, taps, out, at, dtap in (
        (qn, qb, tq_ref, draw_ref, 0, dtq_ref),
        (kn, kb, tk_ref, draw_ref, wide, dtk_ref),
        (vn, vb, tv_ref, draw_ref, 2 * wide, dtv_ref),
    ):
        here = cur[HALO : HALO + rows, :]
        total = None
        for i in range(4):
            moved = buf[3 - i : 3 - i + rows, :]
            term = moved * taps[i : i + 1, :]
            total = term if total is None else total + term
            dtap[i : i + 1, :] += jnp.sum(here * moved, axis=0, keepdims=True)
        out[:, at : at + total.shape[1]] = total.astype(BF)
        buf[rows : rows + HALO, :] = buf[0:HALO, :]


def mixer_specs(heads, dk, dv, at):
    wide_k, wide_v = heads * dk, heads * dv
    full = lambda shape: pl.BlockSpec(shape, lambda c: (0,) * len(shape))
    return {
        "q": pl.BlockSpec((CH, wide_k), lambda c: (at(c), 0)),
        "k": pl.BlockSpec((CH, wide_k), lambda c: (at(c), 1)),
        "val": pl.BlockSpec((CH, wide_v), lambda c: (at(c), 2 * wide_k // wide_v)),
        "og": pl.BlockSpec((CH, wide_v), lambda c: (at(c), 2 * wide_k // wide_v + 1)),
        "raw": pl.BlockSpec((CH, 2 * (wide_k + wide_v)), lambda c: (at(c), 0)),
        "v": pl.BlockSpec((CH, wide_v), lambda c: (at(c), 0)),
        "ab": pl.BlockSpec((CH, LANES), lambda c: (at(c), 0)),
        "t": pl.BlockSpec((CH, heads * CH), lambda c: (at(c), 0)),
        "s": pl.BlockSpec((None, dk, wide_v), lambda c: (at(c), 0, 0)),
        "tk": full((8, wide_k)),
        "tv": full((8, wide_v)),
        "par": full((8, LANES)),
        "gain": full((1, dv)),
    }


def fwd_gather_body(heads, dk, dv, *refs):
    ins, w_ref, outs, full_ref, rest = refs[:10], refs[10], refs[11:16], refs[16], refs[17:]
    step, steps = pl.program_id(0), pl.num_programs(0)
    gather = Gather(w_ref, full_ref, *rest[4:])

    @pl.when(step == 0)
    def _():
        greet_near(gather.me, gather.outer, gather.side)
        gather.begin()

    gather.step(step)
    fwd_body(heads, dk, dv, *ins, *outs, *rest[:4])

    @pl.when(step == steps - 1)
    def _():
        gather.steps(steps, CHUNKS + 3)
        gather.finish()


def bwd_scatter_body(heads, dk, dv, *refs):
    ins, pair, outs, own, rest = refs[:18], refs[18:20], refs[20:27], refs[27], refs[28:]
    step, steps = pl.program_id(0), pl.num_programs(0)
    scatter = Scatter(*pair, own, *rest[7:])

    @pl.when(step == 0)
    def _():
        greet_near(scatter.me, scatter.outer, scatter.side)
        scatter.begin()

    scatter.step(step)
    bwd_body(heads, dk, dv, *ins, *outs, *rest[:7])

    @pl.when(step == steps - 1)
    def _():
        scatter.steps(steps, CHUNKS + 3)
        scatter.finish()


def mixer_forward(raw, ab, tq, tk, tv, par, gain, w=None, ident=None):
    length, wide_k, wide_v = raw.shape[0], tq.shape[1], tv.shape[1]
    dv = gain.shape[1]
    heads = wide_v // dv
    dk = wide_k // heads
    steps = length // CH
    sp = mixer_specs(heads, dk, dv, lambda c: c)
    any_ref = [pl.BlockSpec(memory_space=pl.ANY)]
    fused = w is not None
    return pl.pallas_call(
        functools.partial(fwd_gather_body if fused else fwd_body, heads, dk, dv),
        grid=(steps,),
        in_specs=[sp[n] for n in ("q", "k", "val", "og", "ab", "tk", "tk", "tv", "par", "gain")] + any_ref * fused,
        out_specs=[sp[n] for n in ("v", "v", "v", "t", "s")] + any_ref * fused,
        out_shape=[
            jax.ShapeDtypeStruct((length, wide_v), BF),
            jax.ShapeDtypeStruct((length, wide_v), F32),
            jax.ShapeDtypeStruct((length, wide_v), BF),
            jax.ShapeDtypeStruct((length, heads * CH), BF),
            jax.ShapeDtypeStruct((steps, dk, wide_v), BF),
        ]
        + [jax.ShapeDtypeStruct((8 * w.shape[0], w.shape[1]), w.dtype) for _ in any_ref * fused],
        scratch_shapes=[
            pltpu.VMEM((CH + HALO, wide_k), F32),
            pltpu.VMEM((CH + HALO, wide_k), F32),
            pltpu.VMEM((CH + HALO, wide_v), F32),
            pltpu.VMEM((heads, dk, dv), F32),
        ]
        + gather_sems() * fused,
        compiler_params=pltpu.CompilerParams(
            dimension_semantics=("arbitrary",), vmem_limit_bytes=40 << 20, collective_id=ident,
            has_side_effects=fused,
        ),
        cost_estimate=pl.CostEstimate(flops=20_000_000_000, bytes_accessed=40_000_000, transcendentals=6_000_000),
        name="mixer_forward",
    )(raw, raw, raw, raw, ab, tq, tk, tv, par, gain, *([w] * fused))


def mixer_backward(raw, ab, tq, tk, tv, par, gain, grad, o, u, t, s, left=None, right=None, ident=None):
    length, wide_k, wide_v = raw.shape[0], tq.shape[1], tv.shape[1]
    dv = gain.shape[1]
    heads = wide_v // dv
    dk = wide_k // heads
    steps = length // CH
    at = lambda c: steps - 1 - c
    sp = mixer_specs(heads, dk, dv, at)
    before = lambda c: jnp.maximum(at(c) * (CH // HALO) - 1, 0)
    hq = pl.BlockSpec((HALO, wide_k), lambda c: (before(c), 0))
    hk = pl.BlockSpec((HALO, wide_k), lambda c: (before(c), 1))
    hv = pl.BlockSpec((HALO, wide_v), lambda c: (before(c), 2 * wide_k // wide_v))
    names = ("q", "k", "val", "og", "ab")
    rest = ("tk", "tk", "tv", "par", "gain", "v", "v", "v", "t", "s")
    fused = left is not None
    pair, own, extra = [], [], []
    if fused:
        whole = lambda x: pl.BlockSpec(x.shape, lambda c: (0, 0), pipeline_mode=pl.Buffered(1))
        mine = (left.shape[1] // 8, right.shape[1])
        pair = [whole(left), whole(right)]
        own = [pl.BlockSpec(mine, lambda c: (0, 0))]
        extra = scatter_scratch(*mine)
    return pl.pallas_call(
        functools.partial(bwd_scatter_body if fused else bwd_body, heads, dk, dv),
        grid=(steps,),
        in_specs=[sp[n] for n in names] + [hq, hk, hv] + [sp[n] for n in rest] + pair,
        out_specs=[sp[n] for n in ("raw", "ab", "tk", "tk", "tv", "par", "gain")] + own,
        out_shape=[
            jax.ShapeDtypeStruct((length, 2 * (wide_k + wide_v)), BF),
            jax.ShapeDtypeStruct((length, LANES), BF),
            jax.ShapeDtypeStruct((8, wide_k), F32),
            jax.ShapeDtypeStruct((8, wide_k), F32),
            jax.ShapeDtypeStruct((8, wide_v), F32),
            jax.ShapeDtypeStruct((8, LANES), F32),
            jax.ShapeDtypeStruct((1, dv), F32),
        ]
        + [jax.ShapeDtypeStruct(spec.block_shape, F32) for spec in own],
        scratch_shapes=[
            pltpu.VMEM((CH + HALO, wide_k), F32),
            pltpu.VMEM((CH + HALO, wide_k), F32),
            pltpu.VMEM((CH + HALO, wide_v), F32),
            pltpu.VMEM((CH + HALO, wide_k), F32),
            pltpu.VMEM((CH + HALO, wide_k), F32),
            pltpu.VMEM((CH + HALO, wide_v), F32),
            pltpu.VMEM((heads, dk, dv), F32),
        ]
        + extra,
        compiler_params=pltpu.CompilerParams(
            dimension_semantics=("arbitrary",), vmem_limit_bytes=60 << 20, collective_id=ident,
            has_side_effects=fused,
        ),
        cost_estimate=pl.CostEstimate(flops=40_000_000_000, bytes_accessed=60_000_000, transcendentals=9_000_000),
        name="mixer_backward",
    )(
        raw, raw, raw, raw, ab, raw, raw, raw, tq, tk, tv, par, gain, grad, o, u, t, s,
        *([left, right] if fused else []),
    )


def on_dp(index):
    return {"dp": index}


def greet_all(me):
    barrier = pltpu.get_barrier_semaphore()
    for j in range(1, 8):
        pl.semaphore_signal(barrier, inc=1, device_id=on_dp((me + j) % 8))
    pl.semaphore_wait(barrier, 7)


def greet_near(me, outer, side):
    barrier = pltpu.get_barrier_semaphore()
    pl.semaphore_signal(barrier, inc=1, device_id=on_dp(me + 1 - 2 * side))

    @pl.when(outer < 3)
    def _():
        pl.semaphore_signal(barrier, inc=1, device_id=on_dp((me + 2) % 8))

    @pl.when(outer > 0)
    def _():
        pl.semaphore_signal(barrier, inc=1, device_id=on_dp((me + 6) % 8))

    pl.semaphore_wait(barrier, 1 + (outer + 2) // 3 + (5 - outer) // 3)


CHUNKS = 8


def gather_sems():
    return [
        pltpu.SemaphoreType.DMA((3, CHUNKS)),
        pltpu.SemaphoreType.DMA((3, CHUNKS)),
        pltpu.SemaphoreType.DMA((4, CHUNKS)),
        pltpu.SemaphoreType.DMA((8, CHUNKS)),
        pltpu.SemaphoreType.DMA,
    ]


class Gather:
    def __init__(self, w_ref, full_ref, right_s, left_s, swap_s, arrive, local):
        self.w, self.full, self.sems, self.arrive = w_ref, full_ref, (right_s, left_s, swap_s), arrive
        self.me = lax.axis_index("dp")
        self.outer, self.side = self.me // 2, self.me % 2
        self.block = w_ref.shape[0]
        self.part = self.block // CHUNKS
        self.keep = pltpu.make_async_copy(w_ref, full_ref.at[pl.ds(0, self.block)], local)

    def spot(self, slot, c):
        return self.full.at[pl.ds(slot * self.block + c * self.part, self.part)]

    def source(self, slot, c):
        return self.w.at[pl.ds(c * self.part, self.part)] if slot == 0 else self.spot(slot, c)

    def copy(self, slot, to, c, sem, index, peer):
        return pltpu.make_async_remote_copy(
            self.source(slot, c), self.spot(to, c), sem.at[index, c], self.arrive.at[to, c], device_id=on_dp(peer)
        )

    def to_right(self, h, c):
        return self.copy((4 - h) % 4, 3 - h, c, self.sems[0], h, (self.me + 2) % 8)

    def to_left(self, h, c):
        return self.copy(h, h + 1, c, self.sems[1], h, (self.me + 6) % 8)

    def to_side(self, slot, c):
        return self.copy(slot, 4 + slot, c, self.sems[2], slot, self.me + 1 - 2 * self.side)

    def landed(self, slot, c):
        pltpu.make_async_copy(self.spot(slot, c), self.spot(slot, c), self.arrive.at[slot, c]).wait()

    def begin(self):
        self.keep.start()

    def step(self, i):
        outer = self.outer

        @pl.when(i < CHUNKS)
        def _():
            self.to_side(0, i).start()

            @pl.when(outer < 3)
            def _():
                self.to_right(0, i).start()

            @pl.when(outer > 0)
            def _():
                self.to_left(0, i).start()

        for h in range(1, 4):
            c = i - h

            @pl.when((c >= 0) & (c < CHUNKS) & (outer >= h))
            def _():
                self.landed(4 - h, c)
                if h < 3:
                    @pl.when(outer < 3)
                    def _():
                        self.to_right(h, c).start()

                self.to_side(4 - h, c).start()

            @pl.when((c >= 0) & (c < CHUNKS) & (outer + h < 4))
            def _():
                self.landed(h, c)
                if h < 3:
                    @pl.when(outer > 0)
                    def _():
                        self.to_left(h, c).start()

                self.to_side(h, c).start()

    def finish(self):
        outer = self.outer

        def one(c, carry):
            for slot in range(4):
                self.to_side(slot, c).wait_send()
                self.landed(4 + slot, c)
            for h in range(3):
                @pl.when((outer >= h) & (outer < 3))
                def _():
                    self.to_right(h, c).wait_send()

                @pl.when((outer + h < 4) & (outer > 0))
                def _():
                    self.to_left(h, c).wait_send()

            return carry

        lax.fori_loop(0, CHUNKS, one, 0)
        self.keep.wait()

    def steps(self, first, last):
        def one(i, carry):
            self.step(i)
            return carry

        lax.fori_loop(first, last, one, 0)


def gather_small_body(w_ref, small_ref, full_ref, all_ref, *sems):
    gather = Gather(w_ref, full_ref, *sems[:5])
    few_s, few_r, local = sems[5:]
    me, outer, side = gather.me, gather.outer, gather.side
    greet_all(me)
    gather.begin()
    keep = pltpu.make_async_copy(small_ref, all_ref.at[0], local)
    keep.start()

    def few(j):
        peer = (me + j) % 8
        slot = (outer - peer // 2 + 4) % 4 + 4 * ((side + peer % 2) % 2)
        return pltpu.make_async_remote_copy(
            small_ref, all_ref.at[slot], few_s.at[j - 1], few_r.at[j - 1], device_id=on_dp(peer)
        )

    for j in range(1, 8):
        few(j).start()
    gather.steps(0, CHUNKS + 3)
    gather.finish()
    for j in range(1, 8):
        few(j).wait()
    keep.wait()


def gather_body(w_ref, full_ref, *sems):
    gather = Gather(w_ref, full_ref, *sems)
    greet_near(gather.me, gather.outer, gather.side)
    gather.begin()
    gather.steps(0, CHUNKS + 3)
    gather.finish()


def ring_gather(w, ident, small=None):
    any_ref = pl.BlockSpec(memory_space=pl.ANY)
    full = jax.ShapeDtypeStruct((8 * w.shape[0], w.shape[1]), w.dtype)
    params = pltpu.CompilerParams(collective_id=ident, has_side_effects=True)
    cost = pl.CostEstimate(flops=0, bytes_accessed=150 * w.size, transcendentals=0)
    if small is None:
        return pl.pallas_call(
            gather_body, in_specs=[any_ref], out_specs=any_ref, out_shape=full, scratch_shapes=gather_sems(),
            compiler_params=params, cost_estimate=cost, name=f"ring_gather_{ident}",
        )(w)
    return pl.pallas_call(
        gather_small_body,
        in_specs=[any_ref] * 2,
        out_specs=[any_ref] * 2,
        out_shape=[full, jax.ShapeDtypeStruct((8,) + small.shape, small.dtype)],
        scratch_shapes=gather_sems()
        + [pltpu.SemaphoreType.DMA((7,)), pltpu.SemaphoreType.DMA((7,)), pltpu.SemaphoreType.DMA],
        compiler_params=params, cost_estimate=cost, name=f"ring_gather_{ident}",
    )(w, small)


def scatter_sems():
    return [pltpu.SemaphoreType.DMA((4, CHUNKS)) for _ in range(6)]


class Scatter:
    def __init__(self, left, right, out, mine, came, from_left, from_right, *sems):
        self.left, self.right, self.out, self.mine, self.came = left, right, out, mine, came
        self.acc = (from_left, from_right)
        self.swap_s, self.swap_r, self.send_l, self.recv_l, self.send_r, self.recv_r = sems
        self.me = lax.axis_index("dp")
        self.outer, self.side = self.me // 2, self.me % 2
        self.block, self.cols = out.shape
        self.part = self.block // CHUNKS

    def dots(self, half):
        tile = self.cols if self.cols <= 1536 else 1024

        def one(k, carry):
            at = pl.multiple_of((4 * half + k) * self.block, self.block)
            rows = self.left[:, pl.ds(at, self.block)]
            for j in range(0, self.cols, tile):
                self.mine[pl.ds(at, self.block), j : j + tile] = mm(rows, self.right[:, j : j + tile], TN).astype(BF)
            return carry

        lax.fori_loop(0, 4, one, 0)

    def rows(self, slot, c):
        return pl.ds(pl.multiple_of(slot * self.block + c * self.part, self.part), self.part)

    def swap(self, slot, c):
        return pltpu.make_async_remote_copy(
            self.mine.at[self.rows(4 + slot, c)], self.came.at[self.rows(slot, c)],
            self.swap_s.at[slot, c], self.swap_r.at[slot, c], device_id=on_dp(self.me + 1 - 2 * self.side),
        )

    def onward(self, way, dest, c):
        ref, rows = self.acc[way], self.rows(dest, c)
        send, recv = ((self.send_l, self.recv_l), (self.send_r, self.recv_r))[way]
        peer = (self.me + (2, 6)[way]) % 8
        return pltpu.make_async_remote_copy(
            ref.at[rows], ref.at[rows], send.at[dest, c], recv.at[dest, c], device_id=on_dp(peer)
        )

    def arrived(self, way, dest, c):
        ref, rows = self.acc[way], self.rows(dest, c)
        recv = (self.recv_l, self.recv_r)[way]
        pltpu.make_async_copy(ref.at[rows], ref.at[rows], recv.at[dest, c]).wait()

    def pair(self, slot, c):
        return self.mine[self.rows(slot, c), :].astype(F32) + self.came[self.rows(slot, c), :].astype(F32)

    def begin(self):
        self.dots(1)

        def one(c, carry):
            for slot in range(4):
                self.swap(slot, c).start()
            return carry

        lax.fori_loop(0, CHUNKS, one, 0)
        self.dots(0)

    def step(self, i):
        outer = self.outer

        @pl.when(i < CHUNKS)
        def _():
            for slot in range(4):
                self.swap(slot, i).wait_recv()

        for way in range(2):
            behind = outer if way == 0 else 3 - outer
            c = i - behind
            for dest in range(4):
                ahead = (outer < dest) if way == 0 else (outer > dest)

                @pl.when((c >= 0) & (c < CHUNKS) & ahead)
                def _():
                    total = self.pair((dest - outer + 4) % 4, c)
                    ref, rows = self.acc[way], self.rows(dest, c)

                    @pl.when(behind == 0)
                    def _():
                        ref[rows, :] = total.astype(BF)

                    @pl.when(behind > 0)
                    def _():
                        self.arrived(way, dest, c)
                        ref[rows, :] = (total + ref[rows, :].astype(F32)).astype(BF)

                    self.onward(way, dest, c).start()

        c = i - 3

        @pl.when((c >= 0) & (c < CHUNKS))
        def _():
            at = pl.ds(pl.multiple_of(c * self.part, self.part), self.part)
            self.out[at, :] = self.pair(0, c)
            for way in range(2):
                @pl.when((outer if way == 0 else 3 - outer) > 0)
                def _():
                    self.arrived(way, outer, c)
                    self.out[at, :] += self.acc[way][self.rows(outer, c), :].astype(F32)

    def steps(self, first, last):
        def one(i, carry):
            self.step(i)
            return carry

        lax.fori_loop(first, last, one, 0)

    def finish(self):
        outer = self.outer

        def one(c, carry):
            for slot in range(4):
                self.swap(slot, c).wait_send()
            for way in range(2):
                for dest in range(4):
                    ahead = (outer < dest) if way == 0 else (outer > dest)

                    @pl.when(ahead)
                    def _():
                        self.onward(way, dest, c).wait_send()

            return carry

        lax.fori_loop(0, CHUNKS, one, 0)


def scatter_scratch(block, cols):
    return [
        pltpu.VMEM((8 * block, cols), BF),
        pltpu.VMEM((4 * block, cols), BF),
        pltpu.VMEM((4 * block, cols), BF),
        pltpu.VMEM((4 * block, cols), BF),
    ] + scatter_sems()


def scatter_body(left_ref, right_ref, out_ref, *scratch):
    scatter = Scatter(left_ref, right_ref, out_ref, *scratch)
    greet_near(scatter.me, scatter.outer, scatter.side)
    scatter.begin()
    scatter.steps(0, CHUNKS + 3)
    scatter.finish()


def scatter_last_body(t_size, left_ref, right_ref, few_ref, tap_ref, vec_ref, out_ref, few_out, tap_out, vec_out, *scratch):
    few_in, tap_in, vec_t, vec_d, few_sem, tap_sem, t_sem, d_sem = scratch[-8:]
    scatter = Scatter(left_ref, right_ref, out_ref, *scratch[:-8])
    me, outer, side = scatter.me, scatter.outer, scatter.side
    mine = lax.axis_index("tensor")
    barrier = pltpu.get_barrier_semaphore()
    for j in range(1, t_size):
        pl.semaphore_signal(barrier, inc=1, device_id={"tensor": (mine + j) % t_size})
    for j in range(1, 8):
        pl.semaphore_signal(barrier, inc=1, device_id=on_dp((me + j) % 8))
    pl.semaphore_wait(barrier, 6 + t_size)

    def few(j):
        peer = (me + j) % 8
        slot = (peer // 2 - outer + 4) % 4 + 4 * ((side + peer % 2) % 2)
        return pltpu.make_async_remote_copy(
            few_ref.at[slot], few_in.at[j], few_sem.at[0, j], few_sem.at[1, j], device_id=on_dp(peer)
        )

    def tap(j):
        peer = (me + j) % 8
        return pltpu.make_async_remote_copy(
            tap_ref.at[peer], tap_in.at[j], tap_sem.at[0, j], tap_sem.at[1, j], device_id=on_dp(peer)
        )

    def across(j):
        return pltpu.make_async_remote_copy(
            vec_ref, vec_t.at[mine], t_sem.at[0, j], t_sem.at[1, j], device_id={"tensor": (mine + j) % t_size}
        )

    def along(j):
        return pltpu.make_async_remote_copy(
            vec_d.at[me], vec_d.at[me], d_sem.at[0, j], d_sem.at[1, j], device_id=on_dp((me + j) % 8)
        )

    for j in range(1, t_size):
        across(j).start()
    for j in range(1, 8):
        few(j).start()
        tap(j).start()
    scatter.begin()
    vec_t[mine] = vec_ref[...]
    for j in range(1, t_size):
        pltpu.make_async_copy(vec_ref, vec_t.at[(mine + t_size - j) % t_size], t_sem.at[1, j]).wait()
    total = vec_t[0]
    for j in range(1, t_size):
        total = total + vec_t[j]
    vec_d[me] = total
    for j in range(1, 8):
        along(j).start()
    scatter.steps(0, CHUNKS + 3)
    few_total, tap_total = few_ref[0], tap_ref[me]
    for j in range(1, 8):
        few(j).wait_recv()
        few_total = few_total + few_in[j]
        tap(j).wait_recv()
        tap_total = tap_total + tap_in[j]
    few_out[...] = few_total
    tap_out[...] = tap_total
    for j in range(1, 8):
        pltpu.make_async_copy(vec_d.at[me], vec_d.at[(me + 8 - j) % 8], d_sem.at[1, j]).wait()
    total = vec_d[0]
    for j in range(1, 8):
        total = total + vec_d[j]
    vec_out[...] = total
    for j in range(1, t_size):
        across(j).wait_send()
    for j in range(1, 8):
        few(j).wait_send()
        tap(j).wait_send()
        along(j).wait_send()
    scatter.finish()


def ring_scatter_last(left, right, few, taps, vec, t_size, ident):
    block, cols = left.shape[1] // 8, right.shape[1]
    vmem = pl.BlockSpec(memory_space=pltpu.VMEM)
    return pl.pallas_call(
        functools.partial(scatter_last_body, t_size),
        in_specs=[vmem] * 5,
        out_specs=[vmem] * 4,
        out_shape=[
            jax.ShapeDtypeStruct((block, cols), F32),
            jax.ShapeDtypeStruct(few.shape[1:], F32),
            jax.ShapeDtypeStruct(taps.shape[1:], F32),
            jax.ShapeDtypeStruct(vec.shape, F32),
        ],
        scratch_shapes=scatter_scratch(block, cols)
        + [
            pltpu.VMEM(few.shape, F32),
            pltpu.VMEM(taps.shape, F32),
            pltpu.VMEM((t_size,) + vec.shape, F32),
            pltpu.VMEM((8,) + vec.shape, F32),
            pltpu.SemaphoreType.DMA((2, 8)),
            pltpu.SemaphoreType.DMA((2, 8)),
            pltpu.SemaphoreType.DMA((2, t_size)),
            pltpu.SemaphoreType.DMA((2, 8)),
        ],
        compiler_params=pltpu.CompilerParams(
            collective_id=ident, has_side_effects=True, vmem_limit_bytes=60 << 20
        ),
        cost_estimate=pl.CostEstimate(flops=0, bytes_accessed=1200 * block * cols, transcendentals=0),
        name=f"ring_scatter_{ident}",
    )(left, right, few, taps, vec)


def ring_scatter(left, right, ident):
    block, cols = left.shape[1] // 8, right.shape[1]
    vmem = pl.BlockSpec(memory_space=pltpu.VMEM)
    return pl.pallas_call(
        scatter_body,
        in_specs=[vmem] * 2,
        out_specs=vmem,
        out_shape=jax.ShapeDtypeStruct((block, cols), F32),
        scratch_shapes=scatter_scratch(block, cols),
        compiler_params=pltpu.CompilerParams(
            collective_id=ident, has_side_effects=True, vmem_limit_bytes=60 << 20
        ),
        cost_estimate=pl.CostEstimate(flops=0, bytes_accessed=1200 * block * cols, transcendentals=0),
        name=f"ring_scatter_{ident}",
    )(left, right)


def plain_dot(left_mat, right_mat):
    return jnp.dot(left_mat, right_mat, preferred_element_type=F32)


def dot_rows(left_mat, right_mat):
    return lax.dot_general(left_mat, right_mat, (((1,), (1,)), ((), ())), preferred_element_type=F32)


def dot_tokens(left_mat, right_mat):
    return lax.dot_general(left_mat, right_mat, (((0,), (0,)), ((), ())), preferred_element_type=F32)


def rms_apply(values, gain_vec):
    return values * lax.rsqrt(jnp.mean(values * values, axis=-1, keepdims=True) + 1e-05) * gain_vec


def swiglu(gate_pre, up_pre):
    return jax.nn.silu(gate_pre) * up_pre


class RingRows:
    def __init__(self, dp_size):
        self.outer = dp_size // 2
        self.index = lax.axis_index("dp")

    def _roll(self, x, axis, blocks):
        size = x.shape[axis] // self.outer * blocks
        return jnp.concatenate(
            [lax.slice_in_dim(x, size, None, axis=axis), lax.slice_in_dim(x, 0, size, axis=axis)], axis
        )

    def reorder(self, x, axis):
        outer_at, pair_at = self.index // 2, self.index % 2
        size = x.shape[axis] // (2 * self.outer)
        cut = [lax.slice_in_dim(x, b * size, (b + 1) * size, axis=axis) for b in range(2 * self.outer)]
        even, odd = jnp.concatenate(cut[0::2], axis), jnp.concatenate(cut[1::2], axis)
        sides = [jnp.where(pair_at == 0, even, odd), jnp.where(pair_at == 0, odd, even)]
        bit = 1
        while bit < self.outer:
            sides = [jnp.where((outer_at // bit) % 2 == 1, self._roll(s, axis, bit), s) for s in sides]
            bit *= 2
        return jnp.concatenate(sides, axis)

    def restore(self, x, axis):
        outer_at, pair_at = self.index // 2, self.index % 2
        half = x.shape[axis] // 2
        sides = [lax.slice_in_dim(x, 0, half, axis=axis), lax.slice_in_dim(x, half, None, axis=axis)]
        bit = 1
        while bit < self.outer:
            sides = [
                jnp.where((outer_at // bit) % 2 == 1, self._roll(s, axis, self.outer - bit), s) for s in sides
            ]
            bit *= 2
        even = jnp.where(pair_at == 0, sides[0], sides[1])
        odd = jnp.where(pair_at == 0, sides[1], sides[0])
        size = half // self.outer
        cut = []
        for b in range(self.outer):
            cut += [lax.slice_in_dim(s, b * size, (b + 1) * size, axis=axis) for s in (even, odd)]
        return jnp.concatenate(cut, axis)

    def _swap(self, x):
        return lax.ppermute(x, "dp", [(i, i ^ 1) for i in range(2 * self.outer)])

    def gather_first(self, w, small):
        return ring_gather(w, 0, small)

    def gather(self, w, ident):
        return ring_gather(w, ident)

    def scatter(self, left, right, ident):
        return ring_scatter(left, right, ident)

    def forward(self, core_in, w, ident):
        return mixer_forward(*core_in, w, ident)

    def backward(self, core_in, saved, left, right, ident):
        return mixer_backward(*core_in, *saved, left, right, ident)

    def scatter_last(self, left, right, few, taps, vec, tensor_size, ident):
        return ring_scatter_last(left, right, few, taps, vec, tensor_size, ident)


class PlainRows:
    def reorder(self, x, axis):
        return x

    def restore(self, x, axis):
        return x

    def gather(self, w, ident):
        return lax.all_gather(w, "dp", axis=0, tiled=True)

    def scatter(self, left, right, ident):
        full = dot_tokens(left, right).astype(BF)
        return lax.psum_scatter(full, "dp", scatter_dimension=0, tiled=True).astype(F32)

    def gather_first(self, w, small):
        return lax.all_gather(w, "dp", axis=0, tiled=True), lax.all_gather(small, "dp", axis=0)

    def forward(self, core_in, w, ident):
        return [*mixer_forward(*core_in), self.gather(w, ident)]

    def backward(self, core_in, saved, left, right, ident):
        return [*mixer_backward(*core_in, *saved), self.scatter(left, right, ident)]

    def scatter_last(self, left, right, few, taps, vec, tensor_size, ident):
        few, taps = (lax.psum_scatter(x, "dp", scatter_dimension=0, tiled=True)[0] for x in (few, taps))
        return self.scatter(left, right, ident), few, taps, lax.psum(vec, ("dp", "tensor"))


def tie(value, *others):
    return lax.optimization_barrier((value, others))[0]


def tensor_gather(x):
    return lax.all_gather(x, "tensor", axis=0, tiled=True)


def tensor_scatter(x):
    return lax.psum_scatter(x, "tensor", scatter_dimension=0, tiled=True)


def shards(
    dp_size, tensor_size, inputs, cotangent, lengths, norm1_gain, w_query, w_key, w_value, w_outgate, w_beta, w_alpha,
    conv_query, conv_key, conv_value, a_log, dt_bias, head_gain, w_out, norm2_gain, w_gate, w_up, w_down,
):
    rows = RingRows(dp_size) if dp_size == 8 else PlainRows()
    heads = w_beta.shape[1]
    wide_k, wide_v = w_query.shape[1], w_value.shape[1]
    dk, dv = wide_k // heads, wide_v // heads
    taps_n = conv_query.shape[2]
    block = w_query.shape[0]
    tensor_pos = lax.axis_index("tensor")
    head_start = tensor_pos * heads

    row_count = inputs.shape[1]
    positions = tensor_pos * row_count + jnp.arange(row_count, dtype=jnp.int32)
    valid_rows = (positions < lengths[0]).astype(F32)[:, None]

    small = jnp.concatenate(
        [w_beta.reshape(-1), w_alpha.reshape(-1), conv_query.reshape(-1), conv_key.reshape(-1), conv_value.reshape(-1)]
    )
    cuts = [0]
    for part in (w_beta, w_alpha, conv_query, conv_key, conv_value):
        cuts.append(cuts[-1] + part.size)
    small = jnp.pad(small, (0, -small.size % (32 * LANES))).reshape(-1, LANES)
    full_raw, small = rows.gather_first(
        jnp.concatenate([w_query, w_key, w_value, w_outgate], axis=1), small
    )
    small = small.reshape(dp_size, -1)
    pieces = [small[:, a:b] for a, b in zip(cuts[:-1], cuts[1:])]
    full_ab = jnp.concatenate([p.reshape(dp_size * block, heads) for p in pieces[:2]], axis=1)
    full_ab = jnp.pad(full_ab, ((0, 0), (0, LANES - 2 * heads)))

    def tap_table(piece, size):
        table = rows.restore(piece, 0).reshape(size, heads, taps_n).astype(F32)
        return jnp.pad(jnp.transpose(table, (2, 1, 0)).reshape(taps_n, heads * size), ((0, 8 - taps_n), (0, 0)))

    tq, tk, tv = tap_table(pieces[2], dk), tap_table(pieces[3], dk), tap_table(pieces[4], dv)
    alog_local = lax.dynamic_slice_in_dim(a_log, head_start, heads)
    dtb_local = lax.dynamic_slice_in_dim(dt_bias, head_start, heads)
    par = jnp.pad(jnp.stack([alog_local, dtb_local]), ((0, 6), (heads, LANES - 2 * heads)))
    gain = head_gain[None]

    local_rows = rows.reorder(inputs[0], 1).astype(F32)
    gain_one = rows.reorder(norm1_gain[None], 1)[0]
    gain_two = rows.reorder(norm2_gain[None], 1)[0]
    normed_one, norm_one_back = jax.vjp(rms_apply, local_rows, gain_one)
    rows_one = tensor_gather(normed_one.astype(BF))
    grad_after = valid_rows * rows.reorder(cotangent[0], 1).astype(F32)
    incoming_ffn = tensor_gather(grad_after.astype(BF))

    ab_raw = plain_dot(rows_one, full_ab)
    core_in = (plain_dot(rows_one, full_raw), ab_raw, tq, tk, tv, par, gain)
    head_bf, delta_out, new_values, inverses, states, full_out = rows.forward(core_in, w_out, 1)
    mixed = dot_rows(head_bf, full_out).astype(BF)
    full_gate = rows.gather(tie(w_gate, mixed), 2)
    after_mix = local_rows + tie(tensor_scatter(mixed), full_gate).astype(F32)
    normed_two, norm_two_back = jax.vjp(rms_apply, after_mix, gain_two)
    normed_two = normed_two.astype(BF)
    full_up = rows.gather(tie(w_up, normed_two), 3)
    rows_two = tie(tensor_gather(normed_two), full_up)
    gate_pre = plain_dot(rows_two, full_gate)
    up_pre = plain_dot(rows_two, full_up)
    hidden, swiglu_back = jax.vjp(swiglu, gate_pre, up_pre)
    hidden_bf = hidden.astype(BF)
    full_down = rows.gather(tie(w_down, full_up), 4)

    grad_hidden = plain_dot(incoming_ffn, full_down)
    grad_gate_pre, grad_up_pre = swiglu_back(grad_hidden)
    gate_low = grad_gate_pre.astype(BF)
    up_low = grad_up_pre.astype(BF)
    back_two = (dot_rows(gate_low, full_gate) + dot_rows(up_low, full_up)).astype(BF)
    out_down = rows.scatter(tie(incoming_ffn, back_two), hidden_bf, 5)
    grad_normed_two = tie(tensor_scatter(back_two), out_down).astype(F32)
    grad_mid, grad_norm2 = norm_two_back(grad_normed_two)
    grad_mid = grad_mid + grad_after
    grad_mix = grad_mid.astype(BF)
    out_gate = rows.scatter(tie(rows_two, grad_mix), gate_low, 6)
    incoming_mix = tie(tensor_gather(grad_mix), out_gate)

    ffn_out = dot_rows(tie(hidden_bf, incoming_mix), full_down).astype(BF)
    ffn_part = tensor_scatter(ffn_out).astype(F32)
    grad_head = tie(plain_dot(incoming_mix, full_out), ffn_out)
    raw_low, ab_low, dtq, dtk, dtv, dpar, dgain, out_up = rows.backward(
        core_in, (grad_head, delta_out, new_values, inverses, states), rows_two, up_low, 7
    )
    outputs = rows.restore(((after_mix + ffn_part) * valid_rows).astype(BF), 1)[None]
    summed = (dot_rows(raw_low, full_raw) + dot_rows(ab_low, full_ab)).astype(BF)
    grad_normed_one = tensor_scatter(summed)
    out_out = rows.scatter(tie(incoming_mix, summed), head_bf, 8)
    grad_first, grad_norm1 = norm_one_back(tie(grad_normed_one, out_out).astype(F32))
    grad_inputs = rows.restore(grad_mid + grad_first, 1)[None]

    def in_lanes(x, lead):
        return jnp.pad(x, ((0, 0), (0, -x.shape[1] % (8 * LANES)))).reshape(lead + (-1, LANES))

    grad_ab = dot_tokens(rows_one, ab_low)[:, : 2 * heads]
    few = [grad_ab[:, :heads].reshape(dp_size, -1), grad_ab[:, heads:].reshape(dp_size, -1)]

    def tap_grad(table, size):
        return jnp.transpose(table[:taps_n].reshape(taps_n, heads, size), (2, 1, 0)).reshape(dp_size, -1)

    taps = [tap_grad(dtq, dk), tap_grad(dtk, dk), tap_grad(dtv, dv)]
    alog_full, dtb_full = (
        lax.dynamic_update_slice_in_dim(jnp.zeros_like(a_log), dpar[i, heads : 2 * heads], head_start, 0)
        for i in range(2)
    )
    vec = [rows.restore(grad_norm1[None], 1)[0], rows.restore(grad_norm2[None], 1)[0], dgain[0], alog_full, dtb_full]
    few, taps, vec_in = (jnp.concatenate(x, axis=-1) for x in (few, taps, vec))
    out_raw, few_sum, tap_sum, vec_sum = rows.scatter_last(
        tie(rows_one, out_out), raw_low, in_lanes(few, (dp_size,)), in_lanes(taps, (dp_size,)),
        in_lanes(vec_in[None], ()), tensor_size, 9,
    )
    wide = 2 * wide_k
    out_qk, out_value, out_outgate = out_raw[:, :wide], out_raw[:, wide : wide + wide_v], out_raw[:, wide + wide_v :]

    def pieces_of(total, like):
        flat, found, at = total.reshape(-1), [], 0
        for part in like:
            found.append(flat[at : at + part.size].reshape(part.shape))
            at += part.size
        return found

    out_beta, out_alpha = pieces_of(few_sum, (w_beta, w_alpha))
    out_cq, out_ck, out_cv = pieces_of(tap_sum, (conv_query, conv_key, conv_value))
    norm1_sum, norm2_sum, hgain_sum, alog_sum, dtb_sum = pieces_of(vec_sum, vec)
    return (
        outputs, grad_inputs, norm1_sum, out_qk[:, :wide_k], out_qk[:, wide_k:], out_value, out_outgate,
        out_beta, out_alpha, out_cq, out_ck, out_cv, alog_sum, dtb_sum, hgain_sum, out_out, norm2_sum,
        out_gate, out_up, out_down,
    )


def solution(mesh):
    mat, cube, whole = P("dp", "tensor"), P("dp", "tensor", None), P()
    in_specs = (
        (cube, cube, P("dp"), whole) + (mat,) * 6 + (cube,) * 3 + (whole,) * 3 + (mat, whole) + (mat,) * 3
    )
    out_specs = (
        (cube, cube, whole) + (mat,) * 6 + (cube,) * 3 + (whole,) * 3 + (mat, whole) + (mat,) * 3
    )
    return jax.shard_map(
        functools.partial(shards, mesh.shape["dp"], mesh.shape["tensor"]), mesh=mesh, in_specs=in_specs, out_specs=out_specs,
        check_vma=False,
    )
```

```python
import functools

import jax
import jax.numpy as jnp
from jax import lax
from jax.experimental import pallas as pl
from jax.experimental.pallas import tpu as pltpu
from jax.sharding import PartitionSpec as P

CH = 128
HALO = 8
LANES = 128
F32 = jnp.float32
BF = jnp.bfloat16


def mm(a, b, dims=((1,), (0,))):
    return lax.dot_general(a, b, (dims, ((), ())), preferred_element_type=F32)


NT = ((1,), (1,))
TN = ((0,), (0,))


def split(x):
    hi = x.astype(BF)
    return hi, (x - hi.astype(F32)).astype(BF)


def mm3(a, b):
    return mm(a[0], b[0]) + (mm(a[0], b[1]) + mm(a[1], b[0]))


def exact_mm(a, b):
    return lax.dot_general(
        a, b, (((1,), (0,)), ((), ())), precision=lax.Precision.HIGHEST, preferred_element_type=F32
    )


def unit_lower_inverse(mats):
    n = mats[0].shape[0]
    row = lax.broadcasted_iota(jnp.int32, (n, n), 0)
    col = lax.broadcasted_iota(jnp.int32, (n, n), 1)

    def off_block(size):
        same = (row // (2 * size)) == (col // (2 * size))
        return same & ((row // size) % 2 == 1) & ((col // size) % 2 == 0)

    eye = jnp.where(row == col, 1.0, 0.0)
    inv = [eye - jnp.where(off_block(1), a, 0.0) for a in mats]
    size = 2
    while size < n:
        mask = off_block(size)
        halves = [split(x) for x in inv]
        low = [split(jnp.where(mask, a, 0.0)) for a in mats]
        mid = [split(mm3(b, x)) for b, x in zip(low, halves)]
        inv = [x - mm3(xs, y) for x, xs, y in zip(inv, halves, mid)]
        size *= 2
    return inv


def softplus(x):
    return jnp.maximum(x, 0.0) + jnp.log1p(jnp.exp(-jnp.abs(x)))


def sigmoid(x):
    return 1.0 / (1.0 + jnp.exp(-x))


def conv_of(buf, taps, rows):
    out = buf[HALO - 3 : HALO - 3 + rows, :] * taps[0:1, :]
    for i in range(1, 4):
        out = out + buf[HALO - 3 + i : HALO - 3 + i + rows, :] * taps[i : i + 1, :]
    return out


def decay_tables(ab, par, rows):
    beta = sigmoid(ab)
    decay = -jnp.exp(par[0:1, :]) * softplus(ab + par[1:2, :])
    row = lax.broadcasted_iota(jnp.int32, (rows, rows), 0)
    col = lax.broadcasted_iota(jnp.int32, (rows, rows), 1)
    run = exact_mm(jnp.where(row >= col, 1.0, 0.0), decay)
    return beta, decay, run, jnp.transpose(run), row, col


def fwd_body(
    heads, dk, dv, q_ref, k_ref, v_ref, og_ref, ab_ref, tq_ref, tk_ref, tv_ref, par_ref, gain_ref,
    head_ref, o_ref, u_ref, t_ref, s_ref, qb, kb, vb, state,
):
    rows = CH

    @pl.when(pl.program_id(0) == 0)
    def _():
        for buf in (qb, kb, vb):
            buf[0:HALO, :] = jnp.zeros((HALO, buf.shape[1]), F32)
        state[...] = jnp.zeros_like(state)

    hs = range(heads)
    raw = []
    for buf, ref, taps in ((qb, q_ref, tq_ref), (kb, k_ref, tk_ref), (vb, v_ref, tv_ref)):
        buf[HALO : HALO + rows, :] = ref[...]
        raw.append(conv_of(buf, taps, rows))
        buf[0:HALO, :] = buf[rows : rows + HALO, :]
    zq, zk, zv = raw
    beta, _, run, run_t, row, col = decay_tables(ab_ref[...], par_ref, rows)
    low_inc = row >= col
    low_strict = row > col
    scale = dk ** (-0.5)

    def unit(z):
        y = z * sigmoid(z)
        return y * lax.rsqrt(jnp.sum(y * y, axis=-1, keepdims=True) + 1e-6)

    q = [unit(zq[:, h * dk : (h + 1) * dk]) * scale for h in hs]
    k = [unit(zk[:, h * dk : (h + 1) * dk]) for h in hs]
    qk_b = [(a.astype(BF), b.astype(BF)) for a, b in zip(q, k)]
    bt = [beta[:, h : h + 1] for h in hs]
    g_col = [run[:, heads + h : heads + h + 1] for h in hs]
    g_row = [run_t[heads + h : heads + h + 1, :] for h in hs]
    dec = [jnp.where(low_inc, jnp.exp(jnp.where(low_inc, g_col[h] - g_row[h], 0.0)), 0.0) for h in hs]
    kk = [mm(qk_b[h][1], qk_b[h][1], NT) for h in hs]
    inv = unit_lower_inverse([jnp.where(low_strict, bt[h] * dec[h] * kk[h], 0.0) for h in hs])
    inv_b = [x.astype(BF) for x in inv]
    p_b = [(mm(qk_b[h][0], qk_b[h][1], NT) * dec[h]).astype(BF) for h in hs]
    start = [jnp.exp(g) for g in g_col]
    end = [run[rows - 1 : rows, heads + h : heads + h + 1] for h in hs]
    s0 = [state[h] for h in hs]
    s0_b = [x.astype(BF) for x in s0]
    for h in hs:
        t_ref[:, h * rows : (h + 1) * rows] = inv_b[h]
        s_ref[:, h * dv : (h + 1) * dv] = s0_b[h]
    rhs = []
    for h in hs:
        z = zv[:, h * dv : (h + 1) * dv]
        val = z * sigmoid(z)
        rhs.append((bt[h] * val - (bt[h] * start[h]) * mm(qk_b[h][1], s0_b[h])).astype(BF))
    u_b = [mm(inv_b[h], rhs[h]).astype(BF) for h in hs]
    for h in hs:
        u_ref[:, h * dv : (h + 1) * dv] = u_b[h]
        tail = (k[h] * jnp.exp(end[h] - g_col[h])).astype(BF)
        state[h] = jnp.exp(end[h]) * s0[h] + mm(tail, u_b[h], TN)
    for h in hs:
        o = start[h] * mm(qk_b[h][0], s0_b[h]) + mm(p_b[h], u_b[h])
        o_ref[:, h * dv : (h + 1) * dv] = o
        og = og_ref[:, h * dv : (h + 1) * dv]
        r = lax.rsqrt(jnp.mean(o * o, axis=-1, keepdims=True) + 1e-5)
        head_ref[:, h * dv : (h + 1) * dv] = (o * r * gain_ref[...] * (og * sigmoid(og))).astype(BF)


def bwd_body(
    heads, dk, dv, q_ref, k_ref, v_ref, og_ref, ab_ref, qh_ref, kh_ref, vh_ref,
    tq_ref, tk_ref, tv_ref, par_ref, gain_ref, g_ref, o_ref, u_ref, t_ref, s_ref,
    draw_ref, dab_ref, dtq_ref, dtk_ref, dtv_ref, dpar_ref, dgain_ref,
    qb, kb, vb, qn, kn, vn, dstate, between=lambda part: None,
):
    rows = CH
    step = pl.program_id(0)
    first = step == 0
    is_top = step == pl.num_programs(0) - 1

    @pl.when(first)
    def _():
        for buf in (qn, kn, vn):
            buf[rows : rows + HALO, :] = jnp.zeros((HALO, buf.shape[1]), F32)
        for ref in (dtq_ref, dtk_ref, dtv_ref, dpar_ref, dgain_ref, dstate):
            ref[...] = jnp.zeros_like(ref)

    hs = range(heads)
    raw = []
    for buf, ref, halo, taps in (
        (qb, q_ref, qh_ref, tq_ref), (kb, k_ref, kh_ref, tk_ref), (vb, v_ref, vh_ref, tv_ref)
    ):
        buf[0:HALO, :] = jnp.where(is_top, 0.0, halo[...])
        buf[HALO : HALO + rows, :] = ref[...]
        raw.append(conv_of(buf, taps, rows))
    zq, zk, zv = raw
    ab = ab_ref[...]
    beta, decay, run, run_t, row, col = decay_tables(ab, par_ref, rows)
    low_inc = row >= col
    low_strict = row > col
    scale = dk ** (-0.5)

    def unit(z):
        sg = sigmoid(z)
        y = z * sg
        n = lax.rsqrt(jnp.sum(y * y, axis=-1, keepdims=True) + 1e-6)
        return y * n, n, sg * (1.0 + z * (1.0 - sg))

    qu = [unit(zq[:, h * dk : (h + 1) * dk]) for h in hs]
    ku = [unit(zk[:, h * dk : (h + 1) * dk]) for h in hs]
    q = [x[0] * scale for x in qu]
    k = [x[0] for x in ku]
    q_b = [x.astype(BF) for x in q]
    k_b = [x.astype(BF) for x in k]
    bt = [beta[:, h : h + 1] for h in hs]
    g_col = [run[:, heads + h : heads + h + 1] for h in hs]
    g_row = [run_t[heads + h : heads + h + 1, :] for h in hs]
    dec = [jnp.where(low_inc, jnp.exp(jnp.where(low_inc, g_col[h] - g_row[h], 0.0)), 0.0) for h in hs]
    start = [jnp.exp(g) for g in g_col]
    end = [run[rows - 1 : rows, heads + h : heads + h + 1] for h in hs]
    tail = [jnp.exp(end[h] - g_col[h]) for h in hs]
    dkk = [mm(k_b[h], k_b[h], NT) * dec[h] for h in hs]
    prob = [mm(q_b[h], k_b[h], NT) * dec[h] for h in hs]
    u_b = [u_ref[:, h * dv : (h + 1) * dv] for h in hs]
    s0_b = [s_ref[:, h * dv : (h + 1) * dv] for h in hs]
    ds1 = [dstate[h] for h in hs]
    ds1_b = [x.astype(BF) for x in ds1]

    gain = gain_ref[...]
    og_at = 2 * heads * dk + heads * dv
    do_b = []
    dgain = jnp.zeros_like(gain)
    for h in hs:
        sl = slice(h * dv, (h + 1) * dv)
        o = o_ref[:, sl]
        og = og_ref[:, sl]
        g = g_ref[:, sl]
        r = lax.rsqrt(jnp.mean(o * o, axis=-1, keepdims=True) + 1e-5)
        sg = sigmoid(og)
        gor = g * (o * r)
        dgain = dgain + jnp.sum(gor * (og * sg), axis=0, keepdims=True)
        draw_ref[:, og_at + h * dv : og_at + (h + 1) * dv] = (gor * gain * (sg * (1.0 + og * (1.0 - sg)))).astype(BF)
        m = g * gain * (og * sg)
        d_o = r * m - o * (r * r * r * jnp.mean(m * o, axis=-1, keepdims=True))
        do_b.append(d_o.astype(BF))
    dgain_ref[...] += dgain

    d_u = [
        mm(prob[h].astype(BF), do_b[h], TN) + mm((k[h] * tail[h]).astype(BF), ds1_b[h]) for h in hs
    ]
    d_r = [mm(t_ref[:, h * rows : (h + 1) * rows], d_u[h].astype(BF), TN) for h in hs]
    dr_b = [x.astype(BF) for x in d_r]
    for h in hs:
        left = jnp.concatenate(
            [(q[h] * start[h]).astype(BF), (k[h] * (-(bt[h] * start[h]))).astype(BF)], axis=0
        )
        right = jnp.concatenate([do_b[h], dr_b[h]], axis=0)
        dstate[h] = jnp.exp(end[h]) * ds1[h] + mm(left, right, TN)

    between(1)
    lane = lax.broadcasted_iota(jnp.int32, (rows, LANES), 1)
    sub = lax.broadcasted_iota(jnp.int32, (LANES, rows), 0)
    dab_cols = jnp.zeros((rows, LANES), F32)
    dg_cols = jnp.zeros((rows, LANES), F32)
    dg_rows = jnp.zeros((LANES, rows), F32)
    dend = jnp.zeros((1, LANES), F32)
    lane_one = lax.broadcasted_iota(jnp.int32, (1, LANES), 1)
    for h in hs:
        sl = slice(h * dv, (h + 1) * dv)
        ks = slice(h * dk, (h + 1) * dk)
        d_p = jnp.where(low_inc, mm(do_b[h], u_b[h], NT), 0.0)
        d_a = jnp.where(low_strict, -mm(dr_b[h], u_b[h], NT), 0.0)
        pp = d_p * prob[h]
        dqk_b = (d_p * dec[h]).astype(BF)
        ad = d_a * dkk[h]
        d_kk = d_a * (bt[h] * dec[h])
        d_kk = (d_kk + jnp.transpose(d_kk)).astype(BF)
        y = mm(do_b[h], s0_b[h], NT)
        x = mm(dr_b[h], s0_b[h], NT)
        z = mm(u_b[h], ds1_b[h], NT)
        dq = mm(dqk_b, k_b[h]) + start[h] * y
        bstart = bt[h] * start[h]
        kx = jnp.sum(k[h] * x, axis=-1, keepdims=True)
        kz = tail[h] * jnp.sum(k[h] * z, axis=-1, keepdims=True)
        dkey = mm(d_kk, k_b[h]) + mm(dqk_b, q_b[h], TN) - bstart * x + tail[h] * z
        zval = zv[:, sl]
        sgv = sigmoid(zval)
        val = zval * sgv
        ad_row = jnp.sum(ad, axis=-1, keepdims=True)
        d_beta = jnp.sum(d_r[h] * val, axis=-1, keepdims=True) - start[h] * kx + ad_row
        d_g = (
            jnp.sum(pp, axis=-1, keepdims=True)
            + bt[h] * ad_row
            + start[h] * jnp.sum(q[h] * y, axis=-1, keepdims=True)
            - bstart * kx
            - kz
        )
        d_g_row = -jnp.sum(pp + bt[h] * ad, axis=0, keepdims=True)
        d_end = jnp.sum(kz, axis=0, keepdims=True) + jnp.exp(end[h]) * jnp.sum(
            jnp.sum(s0_b[h].astype(F32) * ds1[h], axis=-1, keepdims=True), axis=0, keepdims=True
        )
        dab_cols = dab_cols + jnp.where(lane == h, d_beta, 0.0)
        dg_cols = dg_cols + jnp.where(lane == heads + h, d_g, 0.0)
        dg_rows = dg_rows + jnp.where(sub == heads + h, d_g_row, 0.0)
        dend = dend + jnp.where(lane_one == heads + h, d_end, 0.0)
        vn[0:rows, sl] = (bt[h] * d_r[h]) * (sgv * (1.0 + zval * (1.0 - sgv)))
        for buf, du, (un, n, slope) in ((qn, dq * scale, qu[h]), (kn, dkey, ku[h])):
            dy = n * (du - un * jnp.sum(un * du, axis=-1, keepdims=True))
            buf[0:rows, ks] = dy * slope

    d_run = dg_cols + jnp.transpose(dg_rows)
    d_decay = exact_mm(jnp.where(col >= row, 1.0, 0.0), d_run) + dend
    pick = (lane >= heads) & (lane < 2 * heads)
    d_decay = jnp.where(pick, d_decay, 0.0)
    d_alpha = d_decay * (-jnp.exp(par_ref[0:1, :])) * sigmoid(ab + par_ref[1:2, :])
    dpar_ref[0:1, :] += jnp.sum(d_decay * decay, axis=0, keepdims=True)
    dpar_ref[1:2, :] += jnp.sum(d_alpha, axis=0, keepdims=True)
    dab_ref[...] = (dab_cols * beta * (1.0 - beta) + d_alpha).astype(BF)

    wide = heads * dk
    for buf, cur, taps, out, at, dtap in (
        (qn, qb, tq_ref, draw_ref, 0, dtq_ref),
        (kn, kb, tk_ref, draw_ref, wide, dtk_ref),
        (vn, vb, tv_ref, draw_ref, 2 * wide, dtv_ref),
    ):
        here = cur[HALO : HALO + rows, :]
        total = None
        for i in range(4):
            moved = buf[3 - i : 3 - i + rows, :]
            term = moved * taps[i : i + 1, :]
            total = term if total is None else total + term
            dtap[i : i + 1, :] += jnp.sum(here * moved, axis=0, keepdims=True)
        out[:, at : at + total.shape[1]] = total.astype(BF)
        buf[rows : rows + HALO, :] = buf[0:HALO, :]


def mixer_specs(heads, dk, dv, at):
    wide_k, wide_v = heads * dk, heads * dv
    full = lambda shape: pl.BlockSpec(shape, lambda c: (0,) * len(shape))
    return {
        "q": pl.BlockSpec((CH, wide_k), lambda c: (at(c), 0)),
        "k": pl.BlockSpec((CH, wide_k), lambda c: (at(c), 1)),
        "val": pl.BlockSpec((CH, wide_v), lambda c: (at(c), 2 * wide_k // wide_v)),
        "og": pl.BlockSpec((CH, wide_v), lambda c: (at(c), 2 * wide_k // wide_v + 1)),
        "raw": pl.BlockSpec((CH, 2 * (wide_k + wide_v)), lambda c: (at(c), 0)),
        "v": pl.BlockSpec((CH, wide_v), lambda c: (at(c), 0)),
        "ab": pl.BlockSpec((CH, LANES), lambda c: (at(c), 0)),
        "t": pl.BlockSpec((CH, heads * CH), lambda c: (at(c), 0)),
        "s": pl.BlockSpec((None, dk, wide_v), lambda c: (at(c), 0, 0)),
        "tk": full((8, wide_k)),
        "tv": full((8, wide_v)),
        "par": full((8, LANES)),
        "gain": full((1, dv)),
    }


def fwd_gather_body(heads, dk, dv, *refs):
    ins, w_ref, outs, full_ref, rest = refs[:10], refs[10], refs[11:16], refs[16], refs[17:]
    step, steps = pl.program_id(0), pl.num_programs(0)
    gather = Gather(w_ref, full_ref, *rest[4:])

    @pl.when(step == 0)
    def _():
        greet_near(gather.me, gather.outer, gather.side)
        gather.begin()

    gather.step(step)
    fwd_body(heads, dk, dv, *ins, *outs, *rest[:4])

    @pl.when(step == steps - 1)
    def _():
        gather.steps(steps, gather.STEPS)
        gather.finish()


def bwd_scatter_body(length, heads, dk, dv, *refs):
    ins, pair, outs, own, rest = refs[:18], refs[18:20], refs[20:27], refs[27], refs[28:]
    step, steps = pl.program_id(0), pl.num_programs(0)
    each = 2 * CHUNKS // (length // CH)
    scatter = Scatter(each, *pair, own, *rest[7:])

    @pl.when(step == 0)
    def _():
        greet_near(scatter.me, scatter.outer, scatter.side)
        scatter.begin()

    def between(part):
        scatter.steps((2 * step + part) * each, (2 * step + part + 1) * each)

    between(0)
    bwd_body(heads, dk, dv, *ins, *outs, *rest[:7], between)

    @pl.when(step == steps - 1)
    def _():
        scatter.steps(4 * CHUNKS, 4 * CHUNKS + 3 * each)
        scatter.finish()


def mixer_forward(raw, ab, tq, tk, tv, par, gain, w=None, ident=None):
    length, wide_k, wide_v = raw.shape[0], tq.shape[1], tv.shape[1]
    dv = gain.shape[1]
    heads = wide_v // dv
    dk = wide_k // heads
    steps = length // CH
    sp = mixer_specs(heads, dk, dv, lambda c: c)
    any_ref = [pl.BlockSpec(memory_space=pl.ANY)]
    fused = w is not None
    return pl.pallas_call(
        functools.partial(fwd_gather_body if fused else fwd_body, heads, dk, dv),
        grid=(steps,),
        in_specs=[sp[n] for n in ("q", "k", "val", "og", "ab", "tk", "tk", "tv", "par", "gain")] + any_ref * fused,
        out_specs=[sp[n] for n in ("v", "v", "v", "t", "s")] + any_ref * fused,
        out_shape=[
            jax.ShapeDtypeStruct((length, wide_v), BF),
            jax.ShapeDtypeStruct((length, wide_v), F32),
            jax.ShapeDtypeStruct((length, wide_v), BF),
            jax.ShapeDtypeStruct((length, heads * CH), BF),
            jax.ShapeDtypeStruct((steps, dk, wide_v), BF),
        ]
        + [jax.ShapeDtypeStruct((8 * w.shape[0], w.shape[1]), w.dtype) for _ in any_ref * fused],
        scratch_shapes=[
            pltpu.VMEM((CH + HALO, wide_k), F32),
            pltpu.VMEM((CH + HALO, wide_k), F32),
            pltpu.VMEM((CH + HALO, wide_v), F32),
            pltpu.VMEM((heads, dk, dv), F32),
        ]
        + gather_sems() * fused,
        compiler_params=pltpu.CompilerParams(
            dimension_semantics=("arbitrary",), vmem_limit_bytes=60 << 20, collective_id=ident,
            has_side_effects=fused,
        ),
        cost_estimate=pl.CostEstimate(flops=20_000_000_000, bytes_accessed=40_000_000, transcendentals=6_000_000),
        name="mixer_forward",
    )(raw, raw, raw, raw, ab, tq, tk, tv, par, gain, *([w] * fused))


def mixer_backward(raw, ab, tq, tk, tv, par, gain, grad, o, u, t, s, left=None, right=None, ident=None):
    length, wide_k, wide_v = raw.shape[0], tq.shape[1], tv.shape[1]
    dv = gain.shape[1]
    heads = wide_v // dv
    dk = wide_k // heads
    steps = length // CH
    at = lambda c: steps - 1 - c
    sp = mixer_specs(heads, dk, dv, at)
    before = lambda c: jnp.maximum(at(c) * (CH // HALO) - 1, 0)
    hq = pl.BlockSpec((HALO, wide_k), lambda c: (before(c), 0))
    hk = pl.BlockSpec((HALO, wide_k), lambda c: (before(c), 1))
    hv = pl.BlockSpec((HALO, wide_v), lambda c: (before(c), 2 * wide_k // wide_v))
    names = ("q", "k", "val", "og", "ab")
    rest = ("tk", "tk", "tv", "par", "gain", "v", "v", "v", "t", "s")
    fused = left is not None
    pair, own, extra = [], [], []
    if fused:
        whole = lambda x: pl.BlockSpec(x.shape, lambda c: (0, 0), pipeline_mode=pl.Buffered(1))
        mine = (left.shape[1] // 8, right.shape[1])
        pair = [whole(left), whole(right)]
        own = [pl.BlockSpec(mine, lambda c: (0, 0))]
        extra = scatter_scratch(*mine)
    return pl.pallas_call(
        functools.partial(*([bwd_scatter_body, length] if fused else [bwd_body]), heads, dk, dv),
        grid=(steps,),
        in_specs=[sp[n] for n in names] + [hq, hk, hv] + [sp[n] for n in rest] + pair,
        out_specs=[sp[n] for n in ("raw", "ab", "tk", "tk", "tv", "par", "gain")] + own,
        out_shape=[
            jax.ShapeDtypeStruct((length, 2 * (wide_k + wide_v)), BF),
            jax.ShapeDtypeStruct((length, LANES), BF),
            jax.ShapeDtypeStruct((8, wide_k), F32),
            jax.ShapeDtypeStruct((8, wide_k), F32),
            jax.ShapeDtypeStruct((8, wide_v), F32),
            jax.ShapeDtypeStruct((8, LANES), F32),
            jax.ShapeDtypeStruct((1, dv), F32),
        ]
        + [jax.ShapeDtypeStruct(spec.block_shape, F32) for spec in own],
        scratch_shapes=[
            pltpu.VMEM((CH + HALO, wide_k), F32),
            pltpu.VMEM((CH + HALO, wide_k), F32),
            pltpu.VMEM((CH + HALO, wide_v), F32),
            pltpu.VMEM((CH + HALO, wide_k), F32),
            pltpu.VMEM((CH + HALO, wide_k), F32),
            pltpu.VMEM((CH + HALO, wide_v), F32),
            pltpu.VMEM((heads, dk, dv), F32),
        ]
        + extra,
        compiler_params=pltpu.CompilerParams(
            dimension_semantics=("arbitrary",), vmem_limit_bytes=60 << 20, collective_id=ident,
            has_side_effects=fused,
        ),
        cost_estimate=pl.CostEstimate(flops=40_000_000_000, bytes_accessed=60_000_000, transcendentals=9_000_000),
        name="mixer_backward",
    )(
        raw, raw, raw, raw, ab, raw, raw, raw, tq, tk, tv, par, gain, grad, o, u, t, s,
        *([left, right] if fused else []),
    )


def on_dp(index):
    return {"dp": index}


def greet_all(me):
    barrier = pltpu.get_barrier_semaphore()
    for j in range(1, 8):
        pl.semaphore_signal(barrier, inc=1, device_id=on_dp((me + j) % 8))
    pl.semaphore_wait(barrier, 7)


def greet_near(me, outer, side):
    barrier = pltpu.get_barrier_semaphore()
    pl.semaphore_signal(barrier, inc=1, device_id=on_dp(me + 1 - 2 * side))

    @pl.when(outer < 3)
    def _():
        pl.semaphore_signal(barrier, inc=1, device_id=on_dp((me + 2) % 8))

    @pl.when(outer > 0)
    def _():
        pl.semaphore_signal(barrier, inc=1, device_id=on_dp((me + 6) % 8))

    pl.semaphore_wait(barrier, 1 + (outer + 2) // 3 + (5 - outer) // 3)


CHUNKS = 8
LAG = 2


CROSS_FIRST = 1


def gather_sems():
    return [
        pltpu.SemaphoreType.DMA((6, CHUNKS)),
        pltpu.SemaphoreType.DMA((6, CHUNKS)),
        pltpu.SemaphoreType.DMA((4, CHUNKS)),
        pltpu.SemaphoreType.DMA((8, CHUNKS)),
        pltpu.SemaphoreType.DMA,
    ]


class Gather:
    STEPS = CHUNKS + 4

    def __init__(self, w_ref, full_ref, right_s, left_s, swap_s, arrive, local):
        self.w, self.full, self.sems, self.arrive = w_ref, full_ref, (right_s, left_s, swap_s), arrive
        self.me = lax.axis_index("dp")
        self.outer, self.side = self.me // 2, self.me % 2
        self.block = w_ref.shape[0]
        self.part = self.block // CHUNKS
        self.keep = pltpu.make_async_copy(w_ref, full_ref.at[pl.ds(0, self.block)], local)

    def spot(self, slot, c):
        return self.full.at[pl.ds(slot * self.block + c * self.part, self.part)]

    def source(self, slot, c):
        return self.w.at[pl.ds(c * self.part, self.part)] if slot == 0 else self.spot(slot, c)

    def copy(self, slot, to, c, sem, index, peer):
        return pltpu.make_async_remote_copy(
            self.source(slot, c), self.spot(to, c), sem.at[index, c], self.arrive.at[to, c], device_id=on_dp(peer)
        )

    def along(self, way, far, h, c):
        slot, to = ((4 - h) % 4, 3 - h) if way == 0 else (h, h + 1)
        peer = (self.me + (2, 6)[way]) % 8
        return self.copy(slot + 4 * far, to + 4 * far, c, self.sems[way], h + 3 * far, peer)

    def to_side(self, slot, c):
        return self.copy(slot, 4 + slot, c, self.sems[2], slot, self.me + 1 - 2 * self.side)

    def landed(self, slot, c):
        pltpu.make_async_copy(self.spot(slot, c), self.spot(slot, c), self.arrive.at[slot, c]).wait()

    def begin(self):
        self.keep.start()

    def go_on(self, way, far, h, c):
        if h < 3:
            @pl.when((self.outer < 3) if way == 0 else (self.outer > 0))
            def _():
                self.along(way, far, h, c).start()

    def step(self, i):
        @pl.when(i < CHUNKS)
        def _():
            self.to_side(0, i).start()
            for way in range(2):
                self.go_on(way, 0, 0, i)

        far_at = i - 1

        @pl.when((far_at >= 0) & (far_at < CROSS_FIRST))
        def _():
            self.landed(4, far_at)
            for way in range(2):
                self.go_on(way, 1, 0, far_at)

        for far in range(2):
            last = CROSS_FIRST if far else CHUNKS
            for h in range(1, 4):
                c = i - h - far
                for way in range(2):
                    behind = self.outer if way == 0 else 3 - self.outer
                    slot = 4 - h if way == 0 else h

                    @pl.when((c >= 0) & (c < last) & (behind >= h))
                    def _():
                        self.landed(slot + 4 * far, c)
                        self.go_on(way, far, h, c)
                        if not far:
                            @pl.when(c >= CROSS_FIRST)
                            def _():
                                self.to_side(slot, c).start()

    def finish(self):
        def one(c, carry):
            self.to_side(0, c).wait_send()

            @pl.when(c >= CROSS_FIRST)
            def _():
                self.landed(4, c)
                for slot in range(1, 4):
                    self.to_side(slot, c).wait_send()
                    self.landed(4 + slot, c)

            for way in range(2):
                behind = self.outer if way == 0 else 3 - self.outer
                for h in range(3):
                    for far in range(2):
                        @pl.when((behind >= h) & (c < (CROSS_FIRST if far else CHUNKS)))
                        def _():
                            @pl.when((self.outer < 3) if way == 0 else (self.outer > 0))
                            def _():
                                self.along(way, far, h, c).wait_send()

            return carry

        lax.fori_loop(0, CHUNKS, one, 0)
        self.keep.wait()

    def steps(self, first, last):
        def one(i, carry):
            self.step(i)
            return carry

        lax.fori_loop(first, last, one, 0)


def gather_small_body(w_ref, small_ref, full_ref, all_ref, *sems):
    gather = Gather(w_ref, full_ref, *sems[:5])
    few_s, few_r, local = sems[5:]
    me, outer, side = gather.me, gather.outer, gather.side
    greet_all(me)
    gather.begin()
    keep = pltpu.make_async_copy(small_ref, all_ref.at[0], local)
    keep.start()

    def few(j):
        peer = (me + j) % 8
        slot = (outer - peer // 2 + 4) % 4 + 4 * ((side + peer % 2) % 2)
        return pltpu.make_async_remote_copy(
            small_ref, all_ref.at[slot], few_s.at[j - 1], few_r.at[j - 1], device_id=on_dp(peer)
        )

    for j in range(1, 8):
        few(j).start()
    gather.steps(0, gather.STEPS)
    gather.finish()
    for j in range(1, 8):
        few(j).wait()
    keep.wait()


def gather_body(w_ref, full_ref, *sems):
    gather = Gather(w_ref, full_ref, *sems)
    greet_near(gather.me, gather.outer, gather.side)
    gather.begin()
    gather.steps(0, gather.STEPS)
    gather.finish()


def ring_gather(w, ident, small=None):
    any_ref = pl.BlockSpec(memory_space=pl.ANY)
    full = jax.ShapeDtypeStruct((8 * w.shape[0], w.shape[1]), w.dtype)
    params = pltpu.CompilerParams(collective_id=ident, has_side_effects=True)
    cost = pl.CostEstimate(flops=0, bytes_accessed=150 * w.size, transcendentals=0)
    if small is None:
        return pl.pallas_call(
            gather_body, in_specs=[any_ref], out_specs=any_ref, out_shape=full, scratch_shapes=gather_sems(),
            compiler_params=params, cost_estimate=cost, name=f"ring_gather_{ident}",
        )(w)
    return pl.pallas_call(
        gather_small_body,
        in_specs=[any_ref] * 2,
        out_specs=[any_ref] * 2,
        out_shape=[full, jax.ShapeDtypeStruct((8,) + small.shape, small.dtype)],
        scratch_shapes=gather_sems()
        + [pltpu.SemaphoreType.DMA((7,)), pltpu.SemaphoreType.DMA((7,)), pltpu.SemaphoreType.DMA],
        compiler_params=params, cost_estimate=cost, name=f"ring_gather_{ident}",
    )(w, small)


def scatter_sems():
    return [pltpu.SemaphoreType.DMA((4, CHUNKS)) for _ in range(6)]


class Scatter:
    def __init__(self, lag, left, right, out, mine, came, from_left, from_right, *sems):
        self.lag = lag
        self.left, self.right, self.mine, self.came = left, right, mine, came
        self.outs = out if isinstance(out, tuple) else (out,)
        self.acc = (from_left, from_right)
        self.swap_s, self.swap_r, self.send_l, self.recv_l, self.send_r, self.recv_r = sems
        self.me = lax.axis_index("dp")
        self.outer, self.side = self.me // 2, self.me % 2
        self.block, self.cols = self.outs[0].shape[0], right.shape[1]
        self.part = self.block // CHUNKS

    def dot(self, slot):
        tile = self.cols if self.cols <= 1536 else 1024
        at = pl.multiple_of(slot * self.block, self.block)
        rows = self.left[:, pl.ds(at, self.block)]
        for j in range(0, self.cols, tile):
            self.mine[pl.ds(at, self.block), j : j + tile] = mm(rows, self.right[:, j : j + tile], TN).astype(BF)

    def item(self, t):
        dest = (3 * (t // CHUNKS)) % 4
        return dest, (dest - self.outer + 4) % 4, t % CHUNKS

    def rows(self, slot, c):
        return pl.ds(pl.multiple_of(slot * self.block + c * self.part, self.part), self.part)

    def swap(self, slot, c):
        return pltpu.make_async_remote_copy(
            self.mine.at[self.rows(4 + slot, c)], self.came.at[self.rows(slot, c)],
            self.swap_s.at[slot, c], self.swap_r.at[slot, c], device_id=on_dp(self.me + 1 - 2 * self.side),
        )

    def onward(self, way, dest, c):
        ref, rows = self.acc[way], self.rows(dest - 1 + way, c)
        send, recv = ((self.send_l, self.recv_l), (self.send_r, self.recv_r))[way]
        peer = (self.me + (2, 6)[way]) % 8
        return pltpu.make_async_remote_copy(
            ref.at[rows], ref.at[rows], send.at[dest, c], recv.at[dest, c], device_id=on_dp(peer)
        )

    def arrived(self, way, dest, c):
        ref, rows = self.acc[way], self.rows(dest - 1 + way, c)
        recv = (self.recv_l, self.recv_r)[way]
        pltpu.make_async_copy(ref.at[rows], ref.at[rows], recv.at[dest, c]).wait()

    def pair(self, slot, c):
        return self.mine[self.rows(slot, c), :].astype(F32) + self.came[self.rows(slot, c), :].astype(F32)

    def begin(self):
        def send(j, carry):
            _, slot, _ = self.item(j * CHUNKS)
            self.dot(4 + slot)

            def one(c, carry):
                self.swap(slot, c).start()
                return carry

            return lax.fori_loop(0, CHUNKS, one, carry)

        lax.fori_loop(0, 4, send, 0)

    def step(self, t):
        outer = self.outer
        items = 4 * CHUNKS

        @pl.when(t < items)
        def _():
            _, slot, c = self.item(t)

            @pl.when(c == 0)
            def _():
                self.dot(slot)

            self.swap(slot, c).wait_recv()

        for way in range(2):
            behind = outer if way == 0 else 3 - outer
            at = t - behind * self.lag
            dest, slot, c = self.item((at + 2 * items) % items)
            ahead = (outer < dest) if way == 0 else (outer > dest)

            @pl.when((at >= 0) & (at < items) & ahead)
            def _():
                total = self.pair(slot, c)
                ref, rows = self.acc[way], self.rows(dest - 1 + way, c)

                @pl.when(behind == 0)
                def _():
                    ref[rows, :] = total.astype(BF)

                @pl.when(behind > 0)
                def _():
                    self.arrived(way, dest, c)
                    ref[rows, :] = (total + ref[rows, :].astype(F32)).astype(BF)

                self.onward(way, dest, c).start()

        at = t - 3 * self.lag
        dest, _, c = self.item((at + 2 * items) % items)

        @pl.when((at >= 0) & (dest == outer))
        def _():
            rows = pl.ds(pl.multiple_of(c * self.part, self.part), self.part)
            total = self.pair(0, c)
            spans, start = [], 0
            for out in self.outs:
                spans.append((out, slice(start, start + out.shape[1])))
                start += out.shape[1]
            for out, cols in spans:
                out[rows, :] = total[:, cols]
            for way in range(2):
                @pl.when((outer if way == 0 else 3 - outer) > 0)
                def _():
                    self.arrived(way, outer, c)
                    for out, cols in spans:
                        out[rows, :] += self.acc[way][self.rows(outer - 1 + way, c), cols].astype(F32)

    def steps(self, first, last):
        def one(i, carry):
            self.step(i)
            return carry

        lax.fori_loop(first, last, one, 0)

    def finish(self):
        outer = self.outer

        def one(c, carry):
            for slot in range(4):
                self.swap(slot, c).wait_send()
            for way in range(2):
                for dest in range(4):
                    ahead = (outer < dest) if way == 0 else (outer > dest)

                    @pl.when(ahead)
                    def _():
                        self.onward(way, dest, c).wait_send()

            return carry

        lax.fori_loop(0, CHUNKS, one, 0)


def scatter_scratch(block, cols):
    return [
        pltpu.VMEM((8 * block, cols), BF),
        pltpu.VMEM((4 * block, cols), BF),
        pltpu.VMEM((3 * block, cols), BF),
        pltpu.VMEM((3 * block, cols), BF),
    ] + scatter_sems()


def scatter_body(left_ref, right_ref, out_ref, *scratch):
    scatter = Scatter(LAG, left_ref, right_ref, out_ref, *scratch)
    greet_near(scatter.me, scatter.outer, scatter.side)
    scatter.begin()
    scatter.steps(0, 4 * CHUNKS + 3 * LAG)
    scatter.finish()


def scatter_last_body(
    t_size, left_ref, right_ref, ab_ref, few_ref, tap_ref, rest_ref, z_ref, mid_ref, gain_ref, fab_ref, full_ref,
    out_q, out_k, out_v, out_g, few_out, tap_out, vec_out, grad_ref, *scratch,
):
    w_buf, sum_out, sum_in, few_in, tap_in, vec, vec_t, vec_d = scratch[:8]
    w_sem, s_sem, few_sem, tap_sem, t_sem, d_sem = scratch[8:14]
    scatter = Scatter(LAG, left_ref, right_ref, (out_q, out_k, out_v, out_g), *scratch[14:])
    me, outer, side, block = scatter.me, scatter.outer, scatter.side, scatter.block
    mine = lax.axis_index("tensor")
    tokens = z_ref.shape[0]
    barrier = pltpu.get_barrier_semaphore()
    for j in range(1, t_size):
        pl.semaphore_signal(barrier, inc=1, device_id={"tensor": (mine + j) % t_size})
    for j in range(1, 8):
        pl.semaphore_signal(barrier, inc=1, device_id=on_dp((me + j) % 8))
    pl.semaphore_wait(barrier, 6 + t_size)

    def few(j):
        peer = (me + j) % 8
        slot = (peer // 2 - outer + 4) % 4 + 4 * ((side + peer % 2) % 2)
        return pltpu.make_async_remote_copy(
            few_ref.at[slot], few_in.at[j], few_sem.at[0, j], few_sem.at[1, j], device_id=on_dp(peer)
        )

    def tap(j):
        peer = (me + j) % 8
        return pltpu.make_async_remote_copy(
            tap_ref.at[peer], tap_in.at[j], tap_sem.at[0, j], tap_sem.at[1, j], device_id=on_dp(peer)
        )

    def across(j):
        return pltpu.make_async_remote_copy(
            vec, vec_t.at[mine], t_sem.at[0, j], t_sem.at[1, j], device_id={"tensor": (mine + j) % t_size}
        )

    def along(j):
        return pltpu.make_async_remote_copy(
            vec_d.at[me], vec_d.at[me], d_sem.at[0, j], d_sem.at[1, j], device_id=on_dp((me + j) % 8)
        )

    def load(n):
        return pltpu.make_async_copy(full_ref.at[pl.ds(n * block, block)], w_buf.at[n % 2], w_sem.at[n % 2])

    def share(j, n):
        return pltpu.make_async_remote_copy(
            sum_out.at[j, n], sum_in.at[j - 1, n], s_sem.at[0, j, n], s_sem.at[1, j, n],
            device_id={"tensor": (mine + j) % t_size},
        )

    load(0).start()
    scatter.begin()
    for j in range(1, 8):
        few(j).start()
        tap(j).start()

    def tile(n, carry):
        scatter.step(n)

        @pl.when(n < 7)
        def _():
            load(n + 1).start()

        load(n).wait()
        w = w_buf[n % 2]
        w_few = fab_ref[pl.ds(pl.multiple_of(n * block, block), block), :]
        for j in range(t_size):
            rows = pl.ds(pl.multiple_of(((mine + j) % t_size) * tokens, tokens), tokens)
            sum_out[j, n] = (mm(right_ref[rows, :], w, NT) + mm(ab_ref[rows, :], w_few, NT)).astype(BF)
            if j:
                share(j, n).start()
        return carry

    lax.fori_loop(0, 8, tile, 0)
    scatter.steps(8, 3 * CHUNKS)

    def land(n, carry):
        for j in range(1, t_size):
            share(j, n).wait_recv()
        return carry

    lax.fori_loop(0, 8, land, 0)
    size = 32

    def norm(i, carry):
        at = pl.ds(pl.multiple_of(i * size, size), size)
        squares, inner = 0.0, 0.0
        for n in range(8):
            cols = slice(n * block, (n + 1) * block)
            z = z_ref[at, cols]
            m = sum_out[0, n, at, :].astype(F32)
            for j in range(1, t_size):
                m = m + sum_in[j - 1, n, at, :].astype(F32)
            squares = squares + jnp.sum(z * z, axis=-1, keepdims=True)
            inner = inner + jnp.sum(m * gain_ref[:, cols] * z, axis=-1, keepdims=True)
        width = 8 * block
        r = lax.rsqrt(squares / width + 1e-05)
        pull = r * r * r * (inner / width)
        found = []
        for n in range(8):
            cols = slice(n * block, (n + 1) * block)
            z = z_ref[at, cols]
            m = sum_out[0, n, at, :].astype(F32)
            for j in range(1, t_size):
                m = m + sum_in[j - 1, n, at, :].astype(F32)
            home = 2 * ((outer + n) % 4) + (side + n // 4) % 2
            to = pl.ds(pl.multiple_of(home * block, block), block)
            grad_ref[at, to] = mid_ref[at, cols] + r * (m * gain_ref[:, cols]) - z * pull
            found.append(carry[n] + jnp.sum(m * (z * r), axis=0, keepdims=True))
        return tuple(found)

    parts = lax.fori_loop(0, tokens // size, norm, tuple(jnp.zeros((1, block), F32) for _ in range(8)))
    per = block // LANES
    for n in range(8):
        home = 2 * ((outer + n) % 4) + (side + n // 4) % 2
        for k in range(per):
            vec[pl.ds(home * per + k, 1), :] = parts[n][:, k * LANES : (k + 1) * LANES]
    vec[8 * per :, :] = rest_ref[...]
    for j in range(1, t_size):
        across(j).start()
    vec_t[mine] = vec[...]
    scatter.steps(3 * CHUNKS, 3 * CHUNKS + 4)
    for j in range(1, t_size):
        pltpu.make_async_copy(vec, vec_t.at[(mine + t_size - j) % t_size], t_sem.at[1, j]).wait()
    total = vec_t[0]
    for j in range(1, t_size):
        total = total + vec_t[j]
    vec_d[me] = total
    for j in range(1, 8):
        along(j).start()
    scatter.steps(3 * CHUNKS + 4, 4 * CHUNKS + 3 * LAG)
    few_total, tap_total = few_ref[0], tap_ref[me]
    for j in range(1, 8):
        few(j).wait_recv()
        few_total = few_total + few_in[j]
        tap(j).wait_recv()
        tap_total = tap_total + tap_in[j]
    few_out[...] = few_total
    tap_out[...] = tap_total
    for j in range(1, 8):
        pltpu.make_async_copy(vec_d.at[me], vec_d.at[(me + 8 - j) % 8], d_sem.at[1, j]).wait()
    total = vec_d[0]
    for j in range(1, 8):
        total = total + vec_d[j]
    vec_out[...] = total
    for j in range(1, t_size):
        across(j).wait_send()
    for j in range(1, 8):
        few(j).wait_send()
        tap(j).wait_send()
        along(j).wait_send()

    def sent(n, carry):
        for j in range(1, t_size):
            share(j, n).wait_send()
        return carry

    lax.fori_loop(0, 8, sent, 0)
    scatter.finish()


def ring_scatter_last(left, right, ab, few, taps, rest, z, mid, gain, full_ab, full, widths, t_size, ident):
    width, cols, tokens = left.shape[1], right.shape[1], z.shape[0]
    block = width // 8
    vec = (width // LANES + rest.shape[0], LANES)
    vmem = pl.BlockSpec(memory_space=pltpu.VMEM)
    pair = pltpu.SemaphoreType.DMA((2, 8))
    return pl.pallas_call(
        functools.partial(scatter_last_body, t_size),
        in_specs=[vmem] * 10 + [pl.BlockSpec(memory_space=pl.ANY)],
        out_specs=[vmem] * 8,
        out_shape=[jax.ShapeDtypeStruct((block, w), F32) for w in widths]
        + [
            jax.ShapeDtypeStruct(few.shape[1:], F32),
            jax.ShapeDtypeStruct(taps.shape[1:], F32),
            jax.ShapeDtypeStruct(vec, F32),
            jax.ShapeDtypeStruct(z.shape, F32),
        ],
        scratch_shapes=[
            pltpu.VMEM((2, block, cols), BF),
            pltpu.VMEM((t_size, 8, tokens, block), BF),
            pltpu.VMEM((t_size - 1, 8, tokens, block), BF),
            pltpu.VMEM(few.shape, F32),
            pltpu.VMEM(taps.shape, F32),
            pltpu.VMEM(vec, F32),
            pltpu.VMEM((t_size,) + vec, F32),
            pltpu.VMEM((8,) + vec, F32),
            pltpu.SemaphoreType.DMA((2,)),
            pltpu.SemaphoreType.DMA((2, t_size, 8)),
            pair,
            pair,
            pltpu.SemaphoreType.DMA((2, t_size)),
            pair,
        ]
        + scatter_scratch(block, cols),
        compiler_params=pltpu.CompilerParams(
            collective_id=ident, has_side_effects=True, vmem_limit_bytes=63 << 20
        ),
        cost_estimate=pl.CostEstimate(flops=0, bytes_accessed=1200 * block * cols, transcendentals=0),
        name=f"ring_scatter_{ident}",
    )(left, right, ab, few, taps, rest, z, mid, gain, full_ab, full)


def ring_scatter(left, right, ident):
    block, cols = left.shape[1] // 8, right.shape[1]
    vmem = pl.BlockSpec(memory_space=pltpu.VMEM)
    return pl.pallas_call(
        scatter_body,
        in_specs=[vmem] * 2,
        out_specs=vmem,
        out_shape=jax.ShapeDtypeStruct((block, cols), F32),
        scratch_shapes=scatter_scratch(block, cols),
        compiler_params=pltpu.CompilerParams(
            collective_id=ident, has_side_effects=True, vmem_limit_bytes=60 << 20
        ),
        cost_estimate=pl.CostEstimate(flops=0, bytes_accessed=1200 * block * cols, transcendentals=0),
        name=f"ring_scatter_{ident}",
    )(left, right)


FFN_ROWS = 256


def col_tiles(n, want):
    return [(at, min(want, n - at)) for at in range(0, n, want)]


def ffn_forward_body(x_ref, gate_ref, up_ref, w_ref, act_ref, slope_ref, hid_ref, full_ref, *sems):
    step, steps = pl.program_id(0), pl.num_programs(0)
    gather = Gather(w_ref, full_ref, *sems)

    @pl.when(step == 0)
    def _():
        greet_near(gather.me, gather.outer, gather.side)
        gather.begin()

    x = x_ref[...]
    for part, (at, wide) in enumerate(col_tiles(gate_ref.shape[1], 512)):
        gather.step(3 * step + part)
        gate = mm(x, gate_ref[:, at : at + wide])
        up = mm(x, up_ref[:, at : at + wide])
        sg = sigmoid(gate)
        act = gate * sg
        act_ref[:, at : at + wide] = act.astype(BF)
        slope_ref[:, at : at + wide] = (up * (sg * (1.0 + gate * (1.0 - sg)))).astype(BF)
        hid_ref[:, at : at + wide] = (act * up).astype(BF)

    @pl.when(step == steps - 1)
    def _():
        gather.finish()


def ffn_forward(x, full_gate, full_up, w, ident):
    length, ff = x.shape[0], full_gate.shape[1]
    any_ref = pl.BlockSpec(memory_space=pl.ANY)
    once = pl.BlockSpec(full_gate.shape, lambda c: (0, 0), pipeline_mode=pl.Buffered(1))
    tile = pl.BlockSpec((FFN_ROWS, ff), lambda c: (c, 0))
    return pl.pallas_call(
        ffn_forward_body,
        grid=(length // FFN_ROWS,),
        in_specs=[pl.BlockSpec((FFN_ROWS, x.shape[1]), lambda c: (c, 0)), once, once, any_ref],
        out_specs=[tile] * 3 + [any_ref],
        out_shape=[jax.ShapeDtypeStruct((length, ff), BF)] * 3
        + [jax.ShapeDtypeStruct((8 * w.shape[0], w.shape[1]), w.dtype)],
        scratch_shapes=gather_sems(),
        compiler_params=pltpu.CompilerParams(
            dimension_semantics=("arbitrary",), vmem_limit_bytes=60 << 20, collective_id=ident, has_side_effects=True
        ),
        cost_estimate=pl.CostEstimate(flops=70_000_000_000, bytes_accessed=30_000_000, transcendentals=1_500_000),
        name="ffn_forward",
    )(x, full_gate, full_up, w)


def ffn_backward_body(
    left_ref, hid_ref, act_ref, slope_ref, down_ref, gate_ref, up_ref,
    glow_ref, ulow_ref, back_ref, ffn_ref, out_ref, *scratch,
):
    step, steps = pl.program_id(0), pl.num_programs(0)
    scatter = Scatter(4, left_ref, hid_ref, out_ref, *scratch)

    @pl.when(step == 0)
    def _():
        greet_near(scatter.me, scatter.outer, scatter.side)
        scatter.begin()

    rows = pl.ds(pl.multiple_of(step * FFN_ROWS, FFN_ROWS), FFN_ROWS)
    x = left_ref[rows, :]
    for at, wide in col_tiles(down_ref.shape[1], 512):
        cols = slice(at, at + wide)
        grad = mm(x, down_ref[:, cols])
        glow_ref[:, cols] = (grad * slope_ref[:, cols].astype(F32)).astype(BF)
        ulow_ref[:, cols] = (grad * act_ref[:, cols].astype(F32)).astype(BF)
    hid = hid_ref[rows, :]
    glow, ulow = glow_ref[...], ulow_ref[...]
    for part, (at, wide) in enumerate(col_tiles(down_ref.shape[0], 512)):
        scatter.steps(8 * step + 2 * part, 8 * step + 2 * part + 2)
        cols = slice(at, at + wide)
        back_ref[:, cols] = (mm(glow, gate_ref[cols, :], NT) + mm(ulow, up_ref[cols, :], NT)).astype(BF)
        ffn_ref[:, cols] = mm(hid, down_ref[cols, :], NT).astype(BF)

    @pl.when(step == steps - 1)
    def _():
        scatter.steps(4 * CHUNKS, 4 * CHUNKS + 12)
        scatter.finish()


def ffn_backward(left, hidden, act, slope, full_down, full_gate, full_up, ident):
    (length, width), ff = left.shape, hidden.shape[1]
    once = lambda x: pl.BlockSpec(x.shape, lambda c: (0, 0), pipeline_mode=pl.Buffered(1))
    tile = pl.BlockSpec((FFN_ROWS, ff), lambda c: (c, 0))
    wide = pl.BlockSpec((FFN_ROWS, width), lambda c: (c, 0))
    mine = (width // 8, ff)
    return pl.pallas_call(
        ffn_backward_body,
        grid=(length // FFN_ROWS,),
        in_specs=[once(left), once(hidden), tile, tile, once(full_down), once(full_gate), once(full_up)],
        out_specs=[tile, tile, wide, wide, pl.BlockSpec(mine, lambda c: (0, 0))],
        out_shape=[jax.ShapeDtypeStruct((length, ff), BF)] * 2
        + [jax.ShapeDtypeStruct((length, width), BF)] * 2
        + [jax.ShapeDtypeStruct(mine, F32)],
        scratch_shapes=scatter_scratch(*mine),
        compiler_params=pltpu.CompilerParams(
            dimension_semantics=("arbitrary",), vmem_limit_bytes=62 << 20, collective_id=ident, has_side_effects=True
        ),
        cost_estimate=pl.CostEstimate(flops=90_000_000_000, bytes_accessed=50_000_000, transcendentals=0),
        name="ffn_backward",
    )(left, hidden, act, slope, full_down, full_gate, full_up)


def plain_dot(left_mat, right_mat):
    return jnp.dot(left_mat, right_mat, preferred_element_type=F32)


def dot_rows(left_mat, right_mat):
    return lax.dot_general(left_mat, right_mat, (((1,), (1,)), ((), ())), preferred_element_type=F32)


def dot_tokens(left_mat, right_mat):
    return lax.dot_general(left_mat, right_mat, (((0,), (0,)), ((), ())), preferred_element_type=F32)


def rms_apply(values, gain_vec):
    return values * lax.rsqrt(jnp.mean(values * values, axis=-1, keepdims=True) + 1e-05) * gain_vec


class RingRows:
    def __init__(self, dp_size):
        self.outer = dp_size // 2
        self.index = lax.axis_index("dp")

    def _roll(self, x, axis, blocks):
        size = x.shape[axis] // self.outer * blocks
        return jnp.concatenate(
            [lax.slice_in_dim(x, size, None, axis=axis), lax.slice_in_dim(x, 0, size, axis=axis)], axis
        )

    def reorder(self, x, axis):
        outer_at, pair_at = self.index // 2, self.index % 2
        size = x.shape[axis] // (2 * self.outer)
        cut = [lax.slice_in_dim(x, b * size, (b + 1) * size, axis=axis) for b in range(2 * self.outer)]
        even, odd = jnp.concatenate(cut[0::2], axis), jnp.concatenate(cut[1::2], axis)
        sides = [jnp.where(pair_at == 0, even, odd), jnp.where(pair_at == 0, odd, even)]
        bit = 1
        while bit < self.outer:
            sides = [jnp.where((outer_at // bit) % 2 == 1, self._roll(s, axis, bit), s) for s in sides]
            bit *= 2
        return jnp.concatenate(sides, axis)

    def restore(self, x, axis):
        outer_at, pair_at = self.index // 2, self.index % 2
        half = x.shape[axis] // 2
        sides = [lax.slice_in_dim(x, 0, half, axis=axis), lax.slice_in_dim(x, half, None, axis=axis)]
        bit = 1
        while bit < self.outer:
            sides = [
                jnp.where((outer_at // bit) % 2 == 1, self._roll(s, axis, self.outer - bit), s) for s in sides
            ]
            bit *= 2
        even = jnp.where(pair_at == 0, sides[0], sides[1])
        odd = jnp.where(pair_at == 0, sides[1], sides[0])
        size = half // self.outer
        cut = []
        for b in range(self.outer):
            cut += [lax.slice_in_dim(s, b * size, (b + 1) * size, axis=axis) for s in (even, odd)]
        return jnp.concatenate(cut, axis)

    def _swap(self, x):
        return lax.ppermute(x, "dp", [(i, i ^ 1) for i in range(2 * self.outer)])

    def gather_first(self, w, small):
        return ring_gather(w, 0, small)

    def gather(self, w, ident):
        return ring_gather(w, ident)

    def scatter(self, left, right, ident):
        return ring_scatter(left, right, ident)

    def ffn_forward(self, x, gate, up, w, ident):
        return ffn_forward(x, gate, up, w, ident)

    def ffn_backward(self, left, hidden, act, slope, down, gate, up, ident):
        return ffn_backward(left, hidden, act, slope, down, gate, up, ident)

    def forward(self, core_in, w, ident):
        return mixer_forward(*core_in, w, ident)

    def backward(self, core_in, saved, left, right, ident):
        return mixer_backward(*core_in, *saved, left, right, ident)

    def scatter_last(self, *args):
        return ring_scatter_last(*args)


class PlainRows:
    def reorder(self, x, axis):
        return x

    def restore(self, x, axis):
        return x

    def gather(self, w, ident):
        return lax.all_gather(w, "dp", axis=0, tiled=True)

    def scatter(self, left, right, ident):
        full = dot_tokens(left, right).astype(BF)
        return lax.psum_scatter(full, "dp", scatter_dimension=0, tiled=True).astype(F32)

    def gather_first(self, w, small):
        return lax.all_gather(w, "dp", axis=0, tiled=True), lax.all_gather(small, "dp", axis=0)

    def ffn_forward(self, x, gate, up, w, ident):
        gate_pre, up_pre = plain_dot(x, gate), plain_dot(x, up)
        sg = jax.nn.sigmoid(gate_pre)
        act = gate_pre * sg
        slope = up_pre * (sg * (1.0 + gate_pre * (1.0 - sg)))
        return act.astype(BF), slope.astype(BF), (act * up_pre).astype(BF), self.gather(w, ident)

    def ffn_backward(self, left, hidden, act, slope, down, gate, up, ident):
        grad = plain_dot(left, down)
        gate_low, up_low = (grad * slope.astype(F32)).astype(BF), (grad * act.astype(F32)).astype(BF)
        back = (dot_rows(gate_low, gate) + dot_rows(up_low, up)).astype(BF)
        return gate_low, up_low, back, dot_rows(hidden, down).astype(BF), self.scatter(left, hidden, ident)

    def forward(self, core_in, w, ident):
        return [*mixer_forward(*core_in), self.gather(w, ident)]

    def backward(self, core_in, saved, left, right, ident):
        return [*mixer_backward(*core_in, *saved), self.scatter(left, right, ident)]

    def scatter_last(self, left, right, ab, few, taps, rest, z, mid, gain, full_ab, full, widths, t_size, ident):
        summed = (dot_rows(right, full) + dot_rows(ab, full_ab)).astype(BF)
        grad, grad_gain = jax.vjp(rms_apply, z, gain[0])[1](tensor_scatter(summed).astype(F32))
        few, taps = (lax.psum_scatter(x, "dp", scatter_dimension=0, tiled=True)[0] for x in (few, taps))
        vec = lax.psum(jnp.concatenate([grad_gain.reshape(-1, LANES), rest]), ("dp", "tensor"))
        out, found, at = self.scatter(left, right, ident), [], 0
        for width in widths:
            found.append(out[:, at : at + width])
            at += width
        return *found, few, taps, vec, mid + grad


def tie(value, *others):
    return lax.optimization_barrier((value, others))[0]


def tensor_gather(x):
    return lax.all_gather(x, "tensor", axis=0, tiled=True)


def tensor_scatter(x):
    return lax.psum_scatter(x, "tensor", scatter_dimension=0, tiled=True)


def shards(
    dp_size, tensor_size, inputs, cotangent, lengths, norm1_gain, w_query, w_key, w_value, w_outgate, w_beta, w_alpha,
    conv_query, conv_key, conv_value, a_log, dt_bias, head_gain, w_out, norm2_gain, w_gate, w_up, w_down,
):
    rows = RingRows(dp_size) if dp_size == 8 else PlainRows()
    heads = w_beta.shape[1]
    wide_k, wide_v = w_query.shape[1], w_value.shape[1]
    dk, dv = wide_k // heads, wide_v // heads
    taps_n = conv_query.shape[2]
    block = w_query.shape[0]
    tensor_pos = lax.axis_index("tensor")
    head_start = tensor_pos * heads

    row_count = inputs.shape[1]
    positions = tensor_pos * row_count + jnp.arange(row_count, dtype=jnp.int32)
    valid_rows = (positions < lengths[0]).astype(F32)[:, None]

    small = jnp.concatenate(
        [w_beta.reshape(-1), w_alpha.reshape(-1), conv_query.reshape(-1), conv_key.reshape(-1), conv_value.reshape(-1)]
    )
    cuts = [0]
    for part in (w_beta, w_alpha, conv_query, conv_key, conv_value):
        cuts.append(cuts[-1] + part.size)
    small = jnp.pad(small, (0, -small.size % (32 * LANES))).reshape(-1, LANES)
    full_raw, small = rows.gather_first(
        jnp.concatenate([w_query, w_key, w_value, w_outgate], axis=1), small
    )
    small = small.reshape(dp_size, -1)
    pieces = [small[:, a:b] for a, b in zip(cuts[:-1], cuts[1:])]
    full_ab = jnp.concatenate([p.reshape(dp_size * block, heads) for p in pieces[:2]], axis=1)
    full_ab = jnp.pad(full_ab, ((0, 0), (0, LANES - 2 * heads)))

    def tap_table(piece, size):
        table = rows.restore(piece, 0).reshape(size, heads, taps_n).astype(F32)
        return jnp.pad(jnp.transpose(table, (2, 1, 0)).reshape(taps_n, heads * size), ((0, 8 - taps_n), (0, 0)))

    tq, tk, tv = tap_table(pieces[2], dk), tap_table(pieces[3], dk), tap_table(pieces[4], dv)
    alog_local = lax.dynamic_slice_in_dim(a_log, head_start, heads)
    dtb_local = lax.dynamic_slice_in_dim(dt_bias, head_start, heads)
    par = jnp.pad(jnp.stack([alog_local, dtb_local]), ((0, 6), (heads, LANES - 2 * heads)))
    gain = head_gain[None]

    local_rows = rows.reorder(inputs[0], 1).astype(F32)
    gain_one = rows.reorder(norm1_gain[None], 1)[0]
    gain_two = rows.reorder(norm2_gain[None], 1)[0]
    normed_one = rms_apply(local_rows, gain_one)
    rows_one = tensor_gather(normed_one.astype(BF))
    grad_after = valid_rows * rows.reorder(cotangent[0], 1).astype(F32)
    incoming_ffn = tensor_gather(grad_after.astype(BF))

    ab_raw = plain_dot(rows_one, full_ab)
    core_in = (plain_dot(rows_one, full_raw), ab_raw, tq, tk, tv, par, gain)
    head_bf, delta_out, new_values, inverses, states, full_out = rows.forward(core_in, w_out, 1)
    mixed = dot_rows(head_bf, full_out).astype(BF)
    full_gate = rows.gather(tie(w_gate, mixed), 2)
    after_mix = local_rows + tie(tensor_scatter(mixed), full_gate).astype(F32)
    normed_two, norm_two_back = jax.vjp(rms_apply, after_mix, gain_two)
    normed_two = normed_two.astype(BF)
    full_up = rows.gather(tie(w_up, normed_two), 3)
    rows_two = tie(tensor_gather(normed_two), full_up)
    act, slope, hidden, full_down = rows.ffn_forward(rows_two, full_gate, full_up, w_down, 4)

    gate_low, up_low, back_two, ffn_out, out_down = rows.ffn_backward(
        incoming_ffn, hidden, act, slope, full_down, full_gate, full_up, 5
    )
    out_gate = rows.scatter(tie(rows_two, back_two), gate_low, 6)
    grad_normed_two = tie(tensor_scatter(back_two), out_gate).astype(F32)
    grad_mid, grad_norm2 = norm_two_back(grad_normed_two)
    grad_mid = grad_mid + grad_after
    grad_mix = grad_mid.astype(BF)
    out_up = rows.scatter(tie(rows_two, grad_mix), up_low, 7)
    incoming_mix = tie(tensor_gather(grad_mix), out_up)

    ffn_part = tensor_scatter(tie(ffn_out, incoming_mix)).astype(F32)
    outputs = rows.restore(((after_mix + ffn_part) * valid_rows).astype(BF), 1)[None]
    raw_low, ab_low, dtq, dtk, dtv, dpar, dgain, out_out = rows.backward(
        core_in, (plain_dot(incoming_mix, full_out), delta_out, new_values, inverses, states), incoming_mix, head_bf, 8
    )
    def in_lanes(x, lead):
        return jnp.pad(x, ((0, 0), (0, -x.shape[1] % (8 * LANES)))).reshape(lead + (-1, LANES))

    grad_ab = dot_tokens(rows_one, ab_low)[:, : 2 * heads]
    few = [grad_ab[:, :heads].reshape(dp_size, -1), grad_ab[:, heads:].reshape(dp_size, -1)]

    def tap_grad(table, size):
        return jnp.transpose(table[:taps_n].reshape(taps_n, heads, size), (2, 1, 0)).reshape(dp_size, -1)

    taps = [tap_grad(dtq, dk), tap_grad(dtk, dk), tap_grad(dtv, dv)]
    alog_full, dtb_full = (
        lax.dynamic_update_slice_in_dim(jnp.zeros_like(a_log), dpar[i, heads : 2 * heads], head_start, 0)
        for i in range(2)
    )
    rest = [rows.restore(grad_norm2[None], 1)[0], dgain[0], alog_full, dtb_full]
    few, taps, rest_in = (jnp.concatenate(x, axis=-1) for x in (few, taps, rest))
    out_query, out_key, out_value, out_outgate, few_sum, tap_sum, vec_sum, grad_inputs = rows.scatter_last(
        tie(rows_one, out_out), raw_low, ab_low, in_lanes(few, (dp_size,)), in_lanes(taps, (dp_size,)),
        in_lanes(rest_in[None], ()), local_rows, grad_mid, gain_one[None], full_ab, full_raw,
        (wide_k, wide_k, wide_v, wide_v), tensor_size, 9,
    )

    def pieces_of(total, like):
        flat, found, at = total.reshape(-1), [], 0
        for part in like:
            found.append(flat[at : at + part.size].reshape(part.shape))
            at += part.size
        return found

    out_beta, out_alpha = pieces_of(few_sum, (w_beta, w_alpha))
    out_cq, out_ck, out_cv = pieces_of(tap_sum, (conv_query, conv_key, conv_value))
    norm1_sum, norm2_sum, hgain_sum, alog_sum, dtb_sum = pieces_of(vec_sum, [norm1_gain] + rest)
    return (
        outputs, grad_inputs[None], norm1_sum, out_query, out_key, out_value, out_outgate,
        out_beta, out_alpha, out_cq, out_ck, out_cv, alog_sum, dtb_sum, hgain_sum, out_out, norm2_sum,
        out_gate, out_up, out_down,
    )


def solution(mesh):
    mat, cube, whole = P("dp", "tensor"), P("dp", "tensor", None), P()
    in_specs = (
        (cube, cube, P("dp"), whole) + (mat,) * 6 + (cube,) * 3 + (whole,) * 3 + (mat, whole) + (mat,) * 3
    )
    out_specs = (
        (cube, cube, whole) + (mat,) * 6 + (cube,) * 3 + (whole,) * 3 + (mat, whole) + (mat,) * 3
    )
    return jax.shard_map(
        functools.partial(shards, mesh.shape["dp"], mesh.shape["tensor"]), mesh=mesh, in_specs=in_specs, out_specs=out_specs,
        check_vma=False,
    )
```

```python
import functools

import jax
import jax.numpy as jnp
from jax import lax
from jax.experimental import pallas as pl
from jax.experimental.pallas import tpu as pltpu
from jax.sharding import PartitionSpec as P

CH = 128
HALO = 8
MIXER_CHUNKS = 4
LANES = 128
F32 = jnp.float32
BF = jnp.bfloat16


def mm(a, b, dims=((1,), (0,))):
    return lax.dot_general(a, b, (dims, ((), ())), preferred_element_type=F32)


NT = ((1,), (1,))
TN = ((0,), (0,))


def split(x):
    hi = x.astype(BF)
    return hi, (x - hi.astype(F32)).astype(BF)


def mm3(a, b):
    return mm(a[0], b[0]) + (mm(a[0], b[1]) + mm(a[1], b[0]))


def exact_mm(a, b):
    return lax.dot_general(
        a, b, (((1,), (0,)), ((), ())), precision=lax.Precision.HIGHEST, preferred_element_type=F32
    )


def unit_lower_inverse(mats):
    n = mats[0].shape[0]
    row = lax.broadcasted_iota(jnp.int32, (n, n), 0)
    col = lax.broadcasted_iota(jnp.int32, (n, n), 1)

    def off_block(size):
        same = (row // (2 * size)) == (col // (2 * size))
        return same & ((row // size) % 2 == 1) & ((col // size) % 2 == 0)

    eye = jnp.where(row == col, 1.0, 0.0)
    inv = [eye - jnp.where(off_block(1), a, 0.0) for a in mats]
    size = 2
    while size < n:
        mask = off_block(size)
        halves = [split(x) for x in inv]
        low = [split(jnp.where(mask, a, 0.0)) for a in mats]
        mid = [split(mm3(b, x)) for b, x in zip(low, halves)]
        inv = [x - mm3(xs, y) for x, xs, y in zip(inv, halves, mid)]
        size *= 2
    return inv


def softplus(x):
    return jnp.maximum(x, 0.0) + jnp.log1p(jnp.exp(-jnp.abs(x)))


def sigmoid(x):
    return 0.5 * jnp.tanh(0.5 * x) + 0.5


def conv_of(buf, taps, rows):
    out = buf[HALO - 3 : HALO - 3 + rows, :] * taps[0:1, :]
    for i in range(1, 4):
        out = out + buf[HALO - 3 + i : HALO - 3 + i + rows, :] * taps[i : i + 1, :]
    return out


def decay_tables(ab, par, rows):
    beta = sigmoid(ab)
    decay = -jnp.exp(par[0:1, :]) * softplus(ab + par[1:2, :])
    row = lax.broadcasted_iota(jnp.int32, (rows, rows), 0)
    col = lax.broadcasted_iota(jnp.int32, (rows, rows), 1)
    run = exact_mm(jnp.where(row >= col, 1.0, 0.0), decay)
    return beta, decay, run, jnp.transpose(run), row, col


def fwd_body(
    heads, dk, dv, q_ref, k_ref, v_ref, og_ref, ab_ref, tq_ref, tk_ref, tv_ref, par_ref, gain_ref,
    head_ref, o_ref, u_ref, t_ref, s_ref, qb, kb, vb, state, between=lambda part: None,
):
    rows = CH

    @pl.when(pl.program_id(0) == 0)
    def _():
        for buf in (qb, kb, vb):
            buf[0:HALO, :] = jnp.zeros((HALO, buf.shape[1]), F32)
        state[...] = jnp.zeros_like(state)

    hs = range(heads)
    raw = []
    for buf, ref, taps in ((qb, q_ref, tq_ref), (kb, k_ref, tk_ref), (vb, v_ref, tv_ref)):
        buf[HALO : HALO + rows, :] = ref[...]
        raw.append(conv_of(buf, taps, rows))
        buf[0:HALO, :] = buf[rows : rows + HALO, :]
    zq, zk, zv = raw
    beta, _, run, run_t, row, col = decay_tables(ab_ref[...], par_ref, rows)
    low_inc = row >= col
    low_strict = row > col
    scale = dk ** (-0.5)

    def unit(z):
        y = z * sigmoid(z)
        return y * lax.rsqrt(jnp.sum(y * y, axis=-1, keepdims=True) + 1e-6)

    q = [unit(zq[:, h * dk : (h + 1) * dk]) * scale for h in hs]
    k = [unit(zk[:, h * dk : (h + 1) * dk]) for h in hs]
    qk_b = [(a.astype(BF), b.astype(BF)) for a, b in zip(q, k)]
    bt = [beta[:, h : h + 1] for h in hs]
    g_col = [run[:, heads + h : heads + h + 1] for h in hs]
    g_row = [run_t[heads + h : heads + h + 1, :] for h in hs]
    dec = [jnp.where(low_inc, jnp.exp(jnp.where(low_inc, g_col[h] - g_row[h], 0.0)), 0.0) for h in hs]
    kk = [mm(qk_b[h][1], qk_b[h][1], NT) for h in hs]
    inv = unit_lower_inverse([jnp.where(low_strict, bt[h] * dec[h] * kk[h], 0.0) for h in hs])
    inv_b = [x.astype(BF) for x in inv]
    between(1)
    p_b = [(mm(qk_b[h][0], qk_b[h][1], NT) * dec[h]).astype(BF) for h in hs]
    start = [jnp.exp(g) for g in g_col]
    end = [run[rows - 1 : rows, heads + h : heads + h + 1] for h in hs]
    s0 = [state[h] for h in hs]
    s0_b = [x.astype(BF) for x in s0]
    for h in hs:
        t_ref[:, h * rows : (h + 1) * rows] = inv_b[h]
        s_ref[:, h * dv : (h + 1) * dv] = s0_b[h]
    rhs = []
    for h in hs:
        z = zv[:, h * dv : (h + 1) * dv]
        val = z * sigmoid(z)
        rhs.append((bt[h] * val - (bt[h] * start[h]) * mm(qk_b[h][1], s0_b[h])).astype(BF))
    u_b = [mm(inv_b[h], rhs[h]).astype(BF) for h in hs]
    for h in hs:
        u_ref[:, h * dv : (h + 1) * dv] = u_b[h]
        tail = (k[h] * jnp.exp(end[h] - g_col[h])).astype(BF)
        state[h] = jnp.exp(end[h]) * s0[h] + mm(tail, u_b[h], TN)
    for h in hs:
        o = start[h] * mm(qk_b[h][0], s0_b[h]) + mm(p_b[h], u_b[h])
        o_ref[:, h * dv : (h + 1) * dv] = o
        og = og_ref[:, h * dv : (h + 1) * dv]
        r = lax.rsqrt(jnp.mean(o * o, axis=-1, keepdims=True) + 1e-5)
        head_ref[:, h * dv : (h + 1) * dv] = (o * r * gain_ref[...] * (og * sigmoid(og))).astype(BF)


def bwd_body(
    heads, dk, dv, q_ref, k_ref, v_ref, og_ref, ab_ref, qh_ref, kh_ref, vh_ref,
    tq_ref, tk_ref, tv_ref, par_ref, gain_ref, g_ref, o_ref, u_ref, t_ref, s_ref,
    draw_ref, dab_ref, dtq_ref, dtk_ref, dtv_ref, dpar_ref, dgain_ref,
    qb, kb, vb, qn, kn, vn, dstate, between=lambda part: None,
):
    rows = CH
    step = pl.program_id(0)
    first = step == 0
    is_top = step == pl.num_programs(0) - 1

    @pl.when(first)
    def _():
        for buf in (qn, kn, vn):
            buf[rows : rows + HALO, :] = jnp.zeros((HALO, buf.shape[1]), F32)
        for ref in (dtq_ref, dtk_ref, dtv_ref, dpar_ref, dgain_ref, dstate):
            ref[...] = jnp.zeros_like(ref)

    hs = range(heads)
    raw = []
    for buf, ref, halo, taps in (
        (qb, q_ref, qh_ref, tq_ref), (kb, k_ref, kh_ref, tk_ref), (vb, v_ref, vh_ref, tv_ref)
    ):
        buf[0:HALO, :] = jnp.where(is_top, 0.0, halo[...])
        buf[HALO : HALO + rows, :] = ref[...]
        raw.append(conv_of(buf, taps, rows))
    zq, zk, zv = raw
    ab = ab_ref[...]
    beta, decay, run, run_t, row, col = decay_tables(ab, par_ref, rows)
    low_inc = row >= col
    low_strict = row > col
    scale = dk ** (-0.5)

    def unit(z):
        sg = sigmoid(z)
        y = z * sg
        n = lax.rsqrt(jnp.sum(y * y, axis=-1, keepdims=True) + 1e-6)
        return y * n, n, sg * (1.0 + z * (1.0 - sg))

    qu = [unit(zq[:, h * dk : (h + 1) * dk]) for h in hs]
    ku = [unit(zk[:, h * dk : (h + 1) * dk]) for h in hs]
    q = [x[0] * scale for x in qu]
    k = [x[0] for x in ku]
    q_b = [x.astype(BF) for x in q]
    k_b = [x.astype(BF) for x in k]
    bt = [beta[:, h : h + 1] for h in hs]
    g_col = [run[:, heads + h : heads + h + 1] for h in hs]
    g_row = [run_t[heads + h : heads + h + 1, :] for h in hs]
    dec = [jnp.where(low_inc, jnp.exp(jnp.where(low_inc, g_col[h] - g_row[h], 0.0)), 0.0) for h in hs]
    start = [jnp.exp(g) for g in g_col]
    end = [run[rows - 1 : rows, heads + h : heads + h + 1] for h in hs]
    tail = [jnp.exp(end[h] - g_col[h]) for h in hs]
    dkk = [mm(k_b[h], k_b[h], NT) * dec[h] for h in hs]
    prob = [mm(q_b[h], k_b[h], NT) * dec[h] for h in hs]
    u_b = [u_ref[:, h * dv : (h + 1) * dv] for h in hs]
    s0_b = [s_ref[:, h * dv : (h + 1) * dv] for h in hs]
    ds1 = [dstate[h] for h in hs]
    ds1_b = [x.astype(BF) for x in ds1]

    gain = gain_ref[...]
    og_at = 2 * heads * dk + heads * dv
    do_b = []
    dgain = jnp.zeros_like(gain)
    for h in hs:
        sl = slice(h * dv, (h + 1) * dv)
        o = o_ref[:, sl]
        og = og_ref[:, sl]
        g = g_ref[:, sl]
        r = lax.rsqrt(jnp.mean(o * o, axis=-1, keepdims=True) + 1e-5)
        sg = sigmoid(og)
        gor = g * (o * r)
        dgain = dgain + jnp.sum(gor * (og * sg), axis=0, keepdims=True)
        draw_ref[:, og_at + h * dv : og_at + (h + 1) * dv] = (gor * gain * (sg * (1.0 + og * (1.0 - sg)))).astype(BF)
        m = g * gain * (og * sg)
        d_o = r * m - o * (r * r * r * jnp.mean(m * o, axis=-1, keepdims=True))
        do_b.append(d_o.astype(BF))
    dgain_ref[...] += dgain

    d_u = [
        mm(prob[h].astype(BF), do_b[h], TN) + mm((k[h] * tail[h]).astype(BF), ds1_b[h]) for h in hs
    ]
    d_r = [mm(t_ref[:, h * rows : (h + 1) * rows], d_u[h].astype(BF), TN) for h in hs]
    dr_b = [x.astype(BF) for x in d_r]
    for h in hs:
        left = jnp.concatenate(
            [(q[h] * start[h]).astype(BF), (k[h] * (-(bt[h] * start[h]))).astype(BF)], axis=0
        )
        right = jnp.concatenate([do_b[h], dr_b[h]], axis=0)
        dstate[h] = jnp.exp(end[h]) * ds1[h] + mm(left, right, TN)

    between(1)
    lane = lax.broadcasted_iota(jnp.int32, (rows, LANES), 1)
    sub = lax.broadcasted_iota(jnp.int32, (LANES, rows), 0)
    dab_cols = jnp.zeros((rows, LANES), F32)
    dg_cols = jnp.zeros((rows, LANES), F32)
    dg_rows = jnp.zeros((LANES, rows), F32)
    dend = jnp.zeros((1, LANES), F32)
    lane_one = lax.broadcasted_iota(jnp.int32, (1, LANES), 1)
    for h in hs:
        sl = slice(h * dv, (h + 1) * dv)
        ks = slice(h * dk, (h + 1) * dk)
        d_p = jnp.where(low_inc, mm(do_b[h], u_b[h], NT), 0.0)
        d_a = jnp.where(low_strict, -mm(dr_b[h], u_b[h], NT), 0.0)
        pp = d_p * prob[h]
        dqk_b = (d_p * dec[h]).astype(BF)
        ad = d_a * dkk[h]
        d_kk = d_a * (bt[h] * dec[h])
        d_kk = (d_kk + jnp.transpose(d_kk)).astype(BF)
        y = mm(do_b[h], s0_b[h], NT)
        x = mm(dr_b[h], s0_b[h], NT)
        z = mm(u_b[h], ds1_b[h], NT)
        dq = mm(dqk_b, k_b[h]) + start[h] * y
        bstart = bt[h] * start[h]
        kx = jnp.sum(k[h] * x, axis=-1, keepdims=True)
        kz = tail[h] * jnp.sum(k[h] * z, axis=-1, keepdims=True)
        dkey = mm(d_kk, k_b[h]) + mm(dqk_b, q_b[h], TN) - bstart * x + tail[h] * z
        zval = zv[:, sl]
        sgv = sigmoid(zval)
        val = zval * sgv
        ad_row = jnp.sum(ad, axis=-1, keepdims=True)
        d_beta = jnp.sum(d_r[h] * val, axis=-1, keepdims=True) - start[h] * kx + ad_row
        d_g = (
            jnp.sum(pp, axis=-1, keepdims=True)
            + bt[h] * ad_row
            + start[h] * jnp.sum(q[h] * y, axis=-1, keepdims=True)
            - bstart * kx
            - kz
        )
        d_g_row = -jnp.sum(pp + bt[h] * ad, axis=0, keepdims=True)
        d_end = jnp.sum(kz, axis=0, keepdims=True) + jnp.exp(end[h]) * jnp.sum(
            jnp.sum(s0_b[h].astype(F32) * ds1[h], axis=-1, keepdims=True), axis=0, keepdims=True
        )
        dab_cols = dab_cols + jnp.where(lane == h, d_beta, 0.0)
        dg_cols = dg_cols + jnp.where(lane == heads + h, d_g, 0.0)
        dg_rows = dg_rows + jnp.where(sub == heads + h, d_g_row, 0.0)
        dend = dend + jnp.where(lane_one == heads + h, d_end, 0.0)
        vn[0:rows, sl] = (bt[h] * d_r[h]) * (sgv * (1.0 + zval * (1.0 - sgv)))
        for buf, du, (un, n, slope) in ((qn, dq * scale, qu[h]), (kn, dkey, ku[h])):
            dy = n * (du - un * jnp.sum(un * du, axis=-1, keepdims=True))
            buf[0:rows, ks] = dy * slope

    d_run = dg_cols + jnp.transpose(dg_rows)
    d_decay = exact_mm(jnp.where(col >= row, 1.0, 0.0), d_run) + dend
    pick = (lane >= heads) & (lane < 2 * heads)
    d_decay = jnp.where(pick, d_decay, 0.0)
    d_alpha = d_decay * (-jnp.exp(par_ref[0:1, :])) * sigmoid(ab + par_ref[1:2, :])
    dpar_ref[0:1, :] += jnp.sum(d_decay * decay, axis=0, keepdims=True)
    dpar_ref[1:2, :] += jnp.sum(d_alpha, axis=0, keepdims=True)
    dab_ref[...] = (dab_cols * beta * (1.0 - beta) + d_alpha).astype(BF)

    wide = heads * dk
    for buf, cur, taps, out, at, dtap in (
        (qn, qb, tq_ref, draw_ref, 0, dtq_ref),
        (kn, kb, tk_ref, draw_ref, wide, dtk_ref),
        (vn, vb, tv_ref, draw_ref, 2 * wide, dtv_ref),
    ):
        here = cur[HALO : HALO + rows, :]
        total = None
        for i in range(4):
            moved = buf[3 - i : 3 - i + rows, :]
            term = moved * taps[i : i + 1, :]
            total = term if total is None else total + term
            dtap[i : i + 1, :] += jnp.sum(here * moved, axis=0, keepdims=True)
        out[:, at : at + total.shape[1]] = total.astype(BF)
        buf[rows : rows + HALO, :] = buf[0:HALO, :]


def mixer_specs(heads, dk, dv, at):
    wide_k, wide_v = heads * dk, heads * dv
    full = lambda shape: pl.BlockSpec(shape, lambda c: (0,) * len(shape))
    return {
        "q": pl.BlockSpec((CH, wide_k), lambda c: (at(c), 0)),
        "k": pl.BlockSpec((CH, wide_k), lambda c: (at(c), 1)),
        "val": pl.BlockSpec((CH, wide_v), lambda c: (at(c), 2 * wide_k // wide_v)),
        "og": pl.BlockSpec((CH, wide_v), lambda c: (at(c), 2 * wide_k // wide_v + 1)),
        "raw": pl.BlockSpec((CH, 2 * (wide_k + wide_v)), lambda c: (at(c), 0)),
        "v": pl.BlockSpec((CH, wide_v), lambda c: (at(c), 0)),
        "ab": pl.BlockSpec((CH, LANES), lambda c: (at(c), 0)),
        "t": pl.BlockSpec((CH, heads * CH), lambda c: (at(c), 0)),
        "s": pl.BlockSpec((None, dk, wide_v), lambda c: (at(c), 0, 0)),
        "tk": full((8, wide_k)),
        "tv": full((8, wide_v)),
        "par": full((8, LANES)),
        "gain": full((1, dv)),
    }


def fwd_gather_body(length, heads, dk, dv, *refs):
    ins, w_ref, outs, full_ref, rest = refs[:10], refs[10], refs[11:16], refs[16], refs[17:]
    step, steps = pl.program_id(0), pl.num_programs(0)
    gather = Gather(w_ref, full_ref, *rest[4:])

    @pl.when(step == 0)
    def _():
        greet_near(gather.me, gather.outer, gather.side)
        gather.begin()

    def between(part):
        gather.steps(*spread(gather.STEPS, 2 * step + part, 2 * (length // CH)))

    between(0)
    fwd_body(heads, dk, dv, *ins, *outs, *rest[:4], between)

    @pl.when(step == steps - 1)
    def _():
        gather.finish()


def bwd_scatter_body(length, heads, dk, dv, *refs):
    ins, pair, outs, own, rest = refs[:18], refs[18:20], refs[20:27], refs[27], refs[28:]
    step, steps = pl.program_id(0), pl.num_programs(0)
    scatter = Scatter(2, MIXER_CHUNKS, *pair, own, *rest[7:])

    @pl.when(step == 0)
    def _():
        greet_near(scatter.me, scatter.outer, scatter.side)
        scatter.begin()

    def between(part):
        scatter.steps(*spread(scatter.last, 2 * step + part, 2 * (length // CH)))

    between(0)
    bwd_body(heads, dk, dv, *ins, *outs, *rest[:7], between)

    @pl.when(step == steps - 1)
    def _():
        scatter.finish()


def mixer_forward(raw, ab, tq, tk, tv, par, gain, w=None, ident=None):
    length, wide_k, wide_v = raw.shape[0], tq.shape[1], tv.shape[1]
    dv = gain.shape[1]
    heads = wide_v // dv
    dk = wide_k // heads
    steps = length // CH
    sp = mixer_specs(heads, dk, dv, lambda c: c)
    any_ref = [pl.BlockSpec(memory_space=pl.ANY)]
    fused = w is not None
    return pl.pallas_call(
        functools.partial(*([fwd_gather_body, length] if fused else [fwd_body]), heads, dk, dv),
        grid=(steps,),
        in_specs=[sp[n] for n in ("q", "k", "val", "og", "ab", "tk", "tk", "tv", "par", "gain")] + any_ref * fused,
        out_specs=[sp[n] for n in ("v", "v", "v", "t", "s")] + any_ref * fused,
        out_shape=[
            jax.ShapeDtypeStruct((length, wide_v), BF),
            jax.ShapeDtypeStruct((length, wide_v), F32),
            jax.ShapeDtypeStruct((length, wide_v), BF),
            jax.ShapeDtypeStruct((length, heads * CH), BF),
            jax.ShapeDtypeStruct((steps, dk, wide_v), BF),
        ]
        + [jax.ShapeDtypeStruct((8 * w.shape[0], w.shape[1]), w.dtype) for _ in any_ref * fused],
        scratch_shapes=[
            pltpu.VMEM((CH + HALO, wide_k), F32),
            pltpu.VMEM((CH + HALO, wide_k), F32),
            pltpu.VMEM((CH + HALO, wide_v), F32),
            pltpu.VMEM((heads, dk, dv), F32),
        ]
        + gather_sems() * fused,
        compiler_params=pltpu.CompilerParams(
            dimension_semantics=("arbitrary",), vmem_limit_bytes=60 << 20, collective_id=ident,
            has_side_effects=fused,
        ),
        cost_estimate=pl.CostEstimate(flops=20_000_000_000, bytes_accessed=40_000_000, transcendentals=6_000_000),
        name="mixer_forward",
    )(raw, raw, raw, raw, ab, tq, tk, tv, par, gain, *([w] * fused))


def mixer_backward(raw, ab, tq, tk, tv, par, gain, grad, o, u, t, s, left=None, right=None, ident=None):
    length, wide_k, wide_v = raw.shape[0], tq.shape[1], tv.shape[1]
    dv = gain.shape[1]
    heads = wide_v // dv
    dk = wide_k // heads
    steps = length // CH
    at = lambda c: steps - 1 - c
    sp = mixer_specs(heads, dk, dv, at)
    before = lambda c: jnp.maximum(at(c) * (CH // HALO) - 1, 0)
    hq = pl.BlockSpec((HALO, wide_k), lambda c: (before(c), 0))
    hk = pl.BlockSpec((HALO, wide_k), lambda c: (before(c), 1))
    hv = pl.BlockSpec((HALO, wide_v), lambda c: (before(c), 2 * wide_k // wide_v))
    names = ("q", "k", "val", "og", "ab")
    rest = ("tk", "tk", "tv", "par", "gain", "v", "v", "v", "t", "s")
    fused = left is not None
    pair, own, extra = [], [], []
    if fused:
        whole = lambda x: pl.BlockSpec(x.shape, lambda c: (0, 0), pipeline_mode=pl.Buffered(1))
        mine = (left.shape[1] // 8, right.shape[1])
        pair = [whole(left), whole(right)]
        own = [pl.BlockSpec(mine, lambda c: (0, 0))]
        extra = scatter_scratch(*mine, MIXER_CHUNKS)
    return pl.pallas_call(
        functools.partial(*([bwd_scatter_body, length] if fused else [bwd_body]), heads, dk, dv),
        grid=(steps,),
        in_specs=[sp[n] for n in names] + [hq, hk, hv] + [sp[n] for n in rest] + pair,
        out_specs=[sp[n] for n in ("raw", "ab", "tk", "tk", "tv", "par", "gain")] + own,
        out_shape=[
            jax.ShapeDtypeStruct((length, 2 * (wide_k + wide_v)), BF),
            jax.ShapeDtypeStruct((length, LANES), BF),
            jax.ShapeDtypeStruct((8, wide_k), F32),
            jax.ShapeDtypeStruct((8, wide_k), F32),
            jax.ShapeDtypeStruct((8, wide_v), F32),
            jax.ShapeDtypeStruct((8, LANES), F32),
            jax.ShapeDtypeStruct((1, dv), F32),
        ]
        + [jax.ShapeDtypeStruct(spec.block_shape, F32) for spec in own],
        scratch_shapes=[
            pltpu.VMEM((CH + HALO, wide_k), F32),
            pltpu.VMEM((CH + HALO, wide_k), F32),
            pltpu.VMEM((CH + HALO, wide_v), F32),
            pltpu.VMEM((CH + HALO, wide_k), F32),
            pltpu.VMEM((CH + HALO, wide_k), F32),
            pltpu.VMEM((CH + HALO, wide_v), F32),
            pltpu.VMEM((heads, dk, dv), F32),
        ]
        + extra,
        compiler_params=pltpu.CompilerParams(
            dimension_semantics=("arbitrary",), vmem_limit_bytes=60 << 20, collective_id=ident,
            has_side_effects=fused,
        ),
        cost_estimate=pl.CostEstimate(flops=40_000_000_000, bytes_accessed=60_000_000, transcendentals=9_000_000),
        name="mixer_backward",
    )(
        raw, raw, raw, raw, ab, raw, raw, raw, tq, tk, tv, par, gain, grad, o, u, t, s,
        *([left, right] if fused else []),
    )


def on_dp(index):
    return {"dp": index}


def greet_all(me):
    barrier = pltpu.get_barrier_semaphore()
    for j in range(1, 8):
        pl.semaphore_signal(barrier, inc=1, device_id=on_dp((me + j) % 8))
    pl.semaphore_wait(barrier, 7)


def greet_near(me, outer, side):
    barrier = pltpu.get_barrier_semaphore()
    pl.semaphore_signal(barrier, inc=1, device_id=on_dp(me + 1 - 2 * side))

    @pl.when(outer < 3)
    def _():
        pl.semaphore_signal(barrier, inc=1, device_id=on_dp((me + 2) % 8))

    @pl.when(outer > 0)
    def _():
        pl.semaphore_signal(barrier, inc=1, device_id=on_dp((me + 6) % 8))

    pl.semaphore_wait(barrier, 1 + (outer + 2) // 3 + (5 - outer) // 3)


CHUNKS = 8
LAG = 2
LAST_CHUNKS = 8


def spread(total, slot, slots):
    return total * slot // slots, total * (slot + 1) // slots


GATHER_CHUNKS = 8
CROSS_FIRST = 1
GATHER_LAG = 2


def gather_sems():
    return [
        pltpu.SemaphoreType.DMA((6, GATHER_CHUNKS)),
        pltpu.SemaphoreType.DMA((6, GATHER_CHUNKS)),
        pltpu.SemaphoreType.DMA((4, GATHER_CHUNKS)),
        pltpu.SemaphoreType.DMA((8, GATHER_CHUNKS)),
        pltpu.SemaphoreType.DMA,
    ]


class Gather:
    STEPS = GATHER_CHUNKS + 4 * GATHER_LAG

    def __init__(self, w_ref, full_ref, right_s, left_s, swap_s, arrive, local):
        self.w, self.full, self.sems, self.arrive = w_ref, full_ref, (right_s, left_s, swap_s), arrive
        self.me = lax.axis_index("dp")
        self.outer, self.side = self.me // 2, self.me % 2
        self.block = w_ref.shape[0]
        self.part = self.block // GATHER_CHUNKS
        self.keep = pltpu.make_async_copy(w_ref, full_ref.at[pl.ds(0, self.block)], local)

    def spot(self, slot, c):
        return self.full.at[pl.ds(slot * self.block + c * self.part, self.part)]

    def source(self, slot, c):
        return self.w.at[pl.ds(c * self.part, self.part)] if slot == 0 else self.spot(slot, c)

    def copy(self, slot, to, c, sem, index, peer):
        return pltpu.make_async_remote_copy(
            self.source(slot, c), self.spot(to, c), sem.at[index, c], self.arrive.at[to, c], device_id=on_dp(peer)
        )

    def along(self, way, far, h, c):
        slot, to = ((4 - h) % 4, 3 - h) if way == 0 else (h, h + 1)
        peer = (self.me + (2, 6)[way]) % 8
        return self.copy(slot + 4 * far, to + 4 * far, c, self.sems[way], h + 3 * far, peer)

    def to_side(self, slot, c):
        return self.copy(slot, 4 + slot, c, self.sems[2], slot, self.me + 1 - 2 * self.side)

    def landed(self, slot, c):
        pltpu.make_async_copy(self.spot(slot, c), self.spot(slot, c), self.arrive.at[slot, c]).wait()

    def begin(self):
        self.keep.start()

    def go_on(self, way, far, h, c):
        if h < 3:
            @pl.when((self.outer < 3) if way == 0 else (self.outer > 0))
            def _():
                self.along(way, far, h, c).start()

    def step(self, i):
        @pl.when(i < GATHER_CHUNKS)
        def _():
            self.to_side(0, i).start()
            for way in range(2):
                self.go_on(way, 0, 0, i)

        far_at = i - GATHER_LAG

        @pl.when((far_at >= 0) & (far_at < CROSS_FIRST))
        def _():
            self.landed(4, far_at)
            for way in range(2):
                self.go_on(way, 1, 0, far_at)

        for far in range(2):
            last = CROSS_FIRST if far else GATHER_CHUNKS
            for h in range(1, 4):
                c = i - GATHER_LAG * (h + far)
                for way in range(2):
                    behind = self.outer if way == 0 else 3 - self.outer
                    slot = 4 - h if way == 0 else h

                    @pl.when((c >= 0) & (c < last) & (behind >= h))
                    def _():
                        self.landed(slot + 4 * far, c)
                        self.go_on(way, far, h, c)
                        if not far:
                            @pl.when(c >= CROSS_FIRST)
                            def _():
                                self.to_side(slot, c).start()

    def finish(self):
        def one(c, carry):
            self.to_side(0, c).wait_send()

            @pl.when(c >= CROSS_FIRST)
            def _():
                self.landed(4, c)
                for slot in range(1, 4):
                    self.to_side(slot, c).wait_send()
                    self.landed(4 + slot, c)

            for way in range(2):
                behind = self.outer if way == 0 else 3 - self.outer
                for h in range(3):
                    for far in range(2):
                        @pl.when((behind >= h) & (c < (CROSS_FIRST if far else GATHER_CHUNKS)))
                        def _():
                            @pl.when((self.outer < 3) if way == 0 else (self.outer > 0))
                            def _():
                                self.along(way, far, h, c).wait_send()

            return carry

        lax.fori_loop(0, GATHER_CHUNKS, one, 0)
        self.keep.wait()

    def steps(self, first, last):
        def one(i, carry):
            self.step(i)
            return carry

        lax.fori_loop(first, last, one, 0)


def gather_small_body(w_ref, small_ref, full_ref, all_ref, *sems):
    gather = Gather(w_ref, full_ref, *sems[:5])
    few_s, few_r, local = sems[5:]
    me, outer, side = gather.me, gather.outer, gather.side
    greet_all(me)
    gather.begin()
    keep = pltpu.make_async_copy(small_ref, all_ref.at[0], local)
    keep.start()

    def few(j):
        peer = (me + j) % 8
        slot = (outer - peer // 2 + 4) % 4 + 4 * ((side + peer % 2) % 2)
        return pltpu.make_async_remote_copy(
            small_ref, all_ref.at[slot], few_s.at[j - 1], few_r.at[j - 1], device_id=on_dp(peer)
        )

    for j in range(1, 8):
        few(j).start()
    gather.steps(0, gather.STEPS)
    gather.finish()
    for j in range(1, 8):
        few(j).wait()
    keep.wait()


def gather_body(w_ref, full_ref, *sems):
    gather = Gather(w_ref, full_ref, *sems)
    greet_near(gather.me, gather.outer, gather.side)
    gather.begin()
    gather.steps(0, gather.STEPS)
    gather.finish()


def ring_gather(w, ident, small=None):
    any_ref = pl.BlockSpec(memory_space=pl.ANY)
    full = jax.ShapeDtypeStruct((8 * w.shape[0], w.shape[1]), w.dtype)
    params = pltpu.CompilerParams(collective_id=ident, has_side_effects=True)
    cost = pl.CostEstimate(flops=0, bytes_accessed=150 * w.size, transcendentals=0)
    if small is None:
        return pl.pallas_call(
            gather_body, in_specs=[any_ref], out_specs=any_ref, out_shape=full, scratch_shapes=gather_sems(),
            compiler_params=params, cost_estimate=cost, name=f"ring_gather_{ident}",
        )(w)
    return pl.pallas_call(
        gather_small_body,
        in_specs=[any_ref] * 2,
        out_specs=[any_ref] * 2,
        out_shape=[full, jax.ShapeDtypeStruct((8,) + small.shape, small.dtype)],
        scratch_shapes=gather_sems()
        + [pltpu.SemaphoreType.DMA((7,)), pltpu.SemaphoreType.DMA((7,)), pltpu.SemaphoreType.DMA],
        compiler_params=params, cost_estimate=cost, name=f"ring_gather_{ident}",
    )(w, small)


def scatter_sems(chunks):
    return [pltpu.SemaphoreType.DMA((4, chunks)) for _ in range(6)]


class Scatter:
    def __init__(self, lag, chunks, left, right, out, mine, came, from_left, from_right, *sems):
        self.lag, self.chunks = lag, chunks
        self.last = 4 * chunks + 3 * lag
        self.left, self.right, self.mine, self.came = left, right, mine, came
        self.outs = out if isinstance(out, tuple) else (out,)
        self.acc = (from_left, from_right)
        self.swap_s, self.swap_r, self.send_l, self.recv_l, self.send_r, self.recv_r = sems
        self.me = lax.axis_index("dp")
        self.outer, self.side = self.me // 2, self.me % 2
        self.block, self.cols = self.outs[0].shape[0], right.shape[1]
        self.part = self.block // chunks

    def dot(self, slot):
        tile = self.cols if self.cols <= 1536 else 1024
        at = pl.multiple_of(slot * self.block, self.block)
        rows = self.left[:, pl.ds(at, self.block)]
        for j in range(0, self.cols, tile):
            self.mine[pl.ds(at, self.block), j : j + tile] = mm(rows, self.right[:, j : j + tile], TN).astype(BF)

    def item(self, t):
        dest = (3 * (t // self.chunks) + 1) % 4
        return dest, (dest - self.outer + 4) % 4, t % self.chunks

    def rows(self, slot, c):
        return pl.ds(pl.multiple_of(slot * self.block + c * self.part, self.part), self.part)

    def swap(self, slot, c):
        return pltpu.make_async_remote_copy(
            self.mine.at[self.rows(4 + slot, c)], self.came.at[self.rows(slot, c)],
            self.swap_s.at[slot, c], self.swap_r.at[slot, c], device_id=on_dp(self.me + 1 - 2 * self.side),
        )

    def onward(self, way, dest, c):
        ref, rows = self.acc[way], self.rows(dest - 1 + way, c)
        send, recv = ((self.send_l, self.recv_l), (self.send_r, self.recv_r))[way]
        peer = (self.me + (2, 6)[way]) % 8
        return pltpu.make_async_remote_copy(
            ref.at[rows], ref.at[rows], send.at[dest, c], recv.at[dest, c], device_id=on_dp(peer)
        )

    def arrived(self, way, dest, c):
        ref, rows = self.acc[way], self.rows(dest - 1 + way, c)
        recv = (self.recv_l, self.recv_r)[way]
        pltpu.make_async_copy(ref.at[rows], ref.at[rows], recv.at[dest, c]).wait()

    def pair(self, slot, c):
        return self.mine[self.rows(slot, c), :].astype(F32) + self.came[self.rows(slot, c), :].astype(F32)

    def begin(self):
        def send(j, carry):
            _, slot, _ = self.item(j * self.chunks)
            self.dot(4 + slot)

            def one(c, carry):
                self.swap(slot, c).start()
                return carry

            return lax.fori_loop(0, self.chunks, one, carry)

        lax.fori_loop(0, 4, send, 0)

    def step(self, t):
        outer = self.outer
        items = 4 * self.chunks

        @pl.when(t < items)
        def _():
            _, slot, c = self.item(t)

            @pl.when(c == 0)
            def _():
                self.dot(slot)

            self.swap(slot, c).wait_recv()

        for way in range(2):
            behind = outer if way == 0 else 3 - outer
            at = t - behind * self.lag
            dest, slot, c = self.item((at + 2 * items) % items)
            ahead = (outer < dest) if way == 0 else (outer > dest)

            @pl.when((at >= 0) & (at < items) & ahead)
            def _():
                total = self.pair(slot, c)
                ref, rows = self.acc[way], self.rows(dest - 1 + way, c)

                @pl.when(behind == 0)
                def _():
                    ref[rows, :] = total.astype(BF)

                @pl.when(behind > 0)
                def _():
                    self.arrived(way, dest, c)
                    ref[rows, :] = (total + ref[rows, :].astype(F32)).astype(BF)

                self.onward(way, dest, c).start()

        at = t - 3 * self.lag
        dest, _, c = self.item((at + 2 * items) % items)

        @pl.when((at >= 0) & (dest == outer))
        def _():
            rows = pl.ds(pl.multiple_of(c * self.part, self.part), self.part)
            total = self.pair(0, c)
            spans, start = [], 0
            for out in self.outs:
                spans.append((out, slice(start, start + out.shape[1])))
                start += out.shape[1]
            for out, cols in spans:
                out[rows, :] = total[:, cols]
            for way in range(2):
                @pl.when((outer if way == 0 else 3 - outer) > 0)
                def _():
                    self.arrived(way, outer, c)
                    for out, cols in spans:
                        out[rows, :] += self.acc[way][self.rows(outer - 1 + way, c), cols].astype(F32)

    def steps(self, first, last):
        def one(i, carry):
            self.step(i)
            return carry

        lax.fori_loop(first, last, one, 0)

    def finish(self):
        outer = self.outer

        def one(c, carry):
            for slot in range(4):
                self.swap(slot, c).wait_send()
            for way in range(2):
                for dest in range(4):
                    ahead = (outer < dest) if way == 0 else (outer > dest)

                    @pl.when(ahead)
                    def _():
                        self.onward(way, dest, c).wait_send()

            return carry

        lax.fori_loop(0, self.chunks, one, 0)


def scatter_scratch(block, cols, chunks):
    return [
        pltpu.VMEM((8 * block, cols), BF),
        pltpu.VMEM((4 * block, cols), BF),
        pltpu.VMEM((3 * block, cols), BF),
        pltpu.VMEM((3 * block, cols), BF),
    ] + scatter_sems(chunks)


def scatter_body(left_ref, right_ref, out_ref, *scratch):
    scatter = Scatter(LAG, CHUNKS, left_ref, right_ref, out_ref, *scratch)
    greet_near(scatter.me, scatter.outer, scatter.side)
    scatter.begin()
    scatter.steps(0, scatter.last)
    scatter.finish()


def scatter_last_body(
    t_size, left_ref, right_ref, ab_ref, few_ref, tap_ref, rest_ref, z_ref, mid_ref, gain_ref, fab_ref, full_ref,
    out_q, out_k, out_v, out_g, few_out, tap_out, vec_out, grad_ref, *scratch,
):
    w_buf, sum_out, sum_in, few_in, tap_in, vec, vec_t, vec_d, parts = scratch[:9]
    w_sem, s_sem, few_sem, tap_sem, t_sem, d_sem = scratch[9:15]
    scatter = Scatter(LAG, LAST_CHUNKS, left_ref, right_ref, (out_q, out_k, out_v, out_g), *scratch[15:])
    me, outer, side, block = scatter.me, scatter.outer, scatter.side, scatter.block
    mine = lax.axis_index("tensor")
    tokens = z_ref.shape[0]
    barrier = pltpu.get_barrier_semaphore()
    for j in range(1, t_size):
        pl.semaphore_signal(barrier, inc=1, device_id={"tensor": (mine + j) % t_size})
    for j in range(1, 8):
        pl.semaphore_signal(barrier, inc=1, device_id=on_dp((me + j) % 8))
    pl.semaphore_wait(barrier, 6 + t_size)

    def few(j):
        peer = (me + j) % 8
        slot = (peer // 2 - outer + 4) % 4 + 4 * ((side + peer % 2) % 2)
        return pltpu.make_async_remote_copy(
            few_ref.at[slot], few_in.at[j], few_sem.at[0, j], few_sem.at[1, j], device_id=on_dp(peer)
        )

    def tap(j):
        peer = (me + j) % 8
        return pltpu.make_async_remote_copy(
            tap_ref.at[peer], tap_in.at[j], tap_sem.at[0, j], tap_sem.at[1, j], device_id=on_dp(peer)
        )

    def across(j):
        return pltpu.make_async_remote_copy(
            vec, vec_t.at[mine], t_sem.at[0, j], t_sem.at[1, j], device_id={"tensor": (mine + j) % t_size}
        )

    def along(j):
        return pltpu.make_async_remote_copy(
            vec_d.at[me], vec_d.at[me], d_sem.at[0, j], d_sem.at[1, j], device_id=on_dp((me + j) % 8)
        )

    def load(n):
        return pltpu.make_async_copy(full_ref.at[pl.ds(n * block, block)], w_buf.at[n % 2], w_sem.at[n % 2])

    def share(j, n):
        return pltpu.make_async_remote_copy(
            sum_out.at[j, n], sum_in.at[j - 1, n], s_sem.at[0, j, n], s_sem.at[1, j, n],
            device_id={"tensor": (mine + j) % t_size},
        )

    load(0).start()
    scatter.begin()
    for j in range(1, 8):
        few(j).start()
        tap(j).start()

    def tile(n, carry):
        scatter.step(n)

        @pl.when(n < 7)
        def _():
            load(n + 1).start()

        load(n).wait()
        w = w_buf[n % 2]
        w_few = fab_ref[pl.ds(pl.multiple_of(n * block, block), block), :]
        for j in range(t_size):
            rows = pl.ds(pl.multiple_of(((mine + j) % t_size) * tokens, tokens), tokens)
            sum_out[j, n] = (mm(right_ref[rows, :], w, NT) + mm(ab_ref[rows, :], w_few, NT)).astype(BF)
            if j:
                share(j, n).start()
        return carry

    lax.fori_loop(0, 8, tile, 0)
    late = 3 * LAST_CHUNKS
    scatter.steps(8, late)

    def land(n, carry):
        for j in range(1, t_size):
            share(j, n).wait_recv()
        return carry

    lax.fori_loop(0, 8, land, 0)
    size = 32

    def norm(i):
        at = pl.ds(pl.multiple_of(i * size, size), size)
        squares, inner = 0.0, 0.0
        for n in range(8):
            cols = slice(n * block, (n + 1) * block)
            z = z_ref[at, cols]
            m = sum_out[0, n, at, :].astype(F32)
            for j in range(1, t_size):
                m = m + sum_in[j - 1, n, at, :].astype(F32)
            squares = squares + jnp.sum(z * z, axis=-1, keepdims=True)
            inner = inner + jnp.sum(m * gain_ref[:, cols] * z, axis=-1, keepdims=True)
        width = 8 * block
        r = lax.rsqrt(squares / width + 1e-05)
        pull = r * r * r * (inner / width)
        for n in range(8):
            cols = slice(n * block, (n + 1) * block)
            z = z_ref[at, cols]
            m = sum_out[0, n, at, :].astype(F32)
            for j in range(1, t_size):
                m = m + sum_in[j - 1, n, at, :].astype(F32)
            home = 2 * ((outer + n) % 4) + (side + n // 4) % 2
            to = pl.ds(pl.multiple_of(home * block, block), block)
            grad_ref[at, to] = mid_ref[at, cols] + r * (m * gain_ref[:, cols]) - z * pull
            parts[n : n + 1, :] += jnp.sum(m * (z * r), axis=0, keepdims=True)

    parts[...] = jnp.zeros_like(parts)
    rounds = tokens // size // 4

    def norms(i, carry):
        scatter.step(late + i)
        for k in range(rounds):
            norm(i * rounds + k)
        return carry

    lax.fori_loop(0, 4, norms, 0)
    per = block // LANES
    for n in range(8):
        home = 2 * ((outer + n) % 4) + (side + n // 4) % 2
        for k in range(per):
            vec[pl.ds(home * per + k, 1), :] = parts[n : n + 1, k * LANES : (k + 1) * LANES]
    vec[8 * per :, :] = rest_ref[...]
    for j in range(1, t_size):
        across(j).start()
    vec_t[mine] = vec[...]
    scatter.steps(late + 4, late + 6)
    for j in range(1, t_size):
        pltpu.make_async_copy(vec, vec_t.at[(mine + t_size - j) % t_size], t_sem.at[1, j]).wait()
    total = vec_t[0]
    for j in range(1, t_size):
        total = total + vec_t[j]
    vec_d[me] = total
    for j in range(1, 8):
        along(j).start()
    scatter.steps(late + 6, scatter.last)
    few_total, tap_total = few_ref[0], tap_ref[me]
    for j in range(1, 8):
        few(j).wait_recv()
        few_total = few_total + few_in[j]
        tap(j).wait_recv()
        tap_total = tap_total + tap_in[j]
    few_out[...] = few_total
    tap_out[...] = tap_total
    for j in range(1, 8):
        pltpu.make_async_copy(vec_d.at[me], vec_d.at[(me + 8 - j) % 8], d_sem.at[1, j]).wait()
    total = vec_d[0]
    for j in range(1, 8):
        total = total + vec_d[j]
    vec_out[...] = total
    for j in range(1, t_size):
        across(j).wait_send()
    for j in range(1, 8):
        few(j).wait_send()
        tap(j).wait_send()
        along(j).wait_send()

    def sent(n, carry):
        for j in range(1, t_size):
            share(j, n).wait_send()
        return carry

    lax.fori_loop(0, 8, sent, 0)
    scatter.finish()


def ring_scatter_last(left, right, ab, few, taps, rest, z, mid, gain, full_ab, full, widths, t_size, ident):
    width, cols, tokens = left.shape[1], right.shape[1], z.shape[0]
    block = width // 8
    vec = (width // LANES + rest.shape[0], LANES)
    vmem = pl.BlockSpec(memory_space=pltpu.VMEM)
    pair = pltpu.SemaphoreType.DMA((2, 8))
    return pl.pallas_call(
        functools.partial(scatter_last_body, t_size),
        in_specs=[vmem] * 10 + [pl.BlockSpec(memory_space=pl.ANY)],
        out_specs=[vmem] * 8,
        out_shape=[jax.ShapeDtypeStruct((block, w), F32) for w in widths]
        + [
            jax.ShapeDtypeStruct(few.shape[1:], F32),
            jax.ShapeDtypeStruct(taps.shape[1:], F32),
            jax.ShapeDtypeStruct(vec, F32),
            jax.ShapeDtypeStruct(z.shape, F32),
        ],
        scratch_shapes=[
            pltpu.VMEM((2, block, cols), BF),
            pltpu.VMEM((t_size, 8, tokens, block), BF),
            pltpu.VMEM((t_size - 1, 8, tokens, block), BF),
            pltpu.VMEM(few.shape, F32),
            pltpu.VMEM(taps.shape, F32),
            pltpu.VMEM(vec, F32),
            pltpu.VMEM((t_size,) + vec, F32),
            pltpu.VMEM((8,) + vec, F32),
            pltpu.VMEM((8, block), F32),
            pltpu.SemaphoreType.DMA((2,)),
            pltpu.SemaphoreType.DMA((2, t_size, 8)),
            pair,
            pair,
            pltpu.SemaphoreType.DMA((2, t_size)),
            pair,
        ]
        + scatter_scratch(block, cols, LAST_CHUNKS),
        compiler_params=pltpu.CompilerParams(
            collective_id=ident, has_side_effects=True, vmem_limit_bytes=63 << 20
        ),
        cost_estimate=pl.CostEstimate(flops=0, bytes_accessed=1200 * block * cols, transcendentals=0),
        name=f"ring_scatter_{ident}",
    )(left, right, ab, few, taps, rest, z, mid, gain, full_ab, full)


def ring_scatter(left, right, ident):
    block, cols = left.shape[1] // 8, right.shape[1]
    vmem = pl.BlockSpec(memory_space=pltpu.VMEM)
    return pl.pallas_call(
        scatter_body,
        in_specs=[vmem] * 2,
        out_specs=vmem,
        out_shape=jax.ShapeDtypeStruct((block, cols), F32),
        scratch_shapes=scatter_scratch(block, cols, CHUNKS),
        compiler_params=pltpu.CompilerParams(
            collective_id=ident, has_side_effects=True, vmem_limit_bytes=60 << 20
        ),
        cost_estimate=pl.CostEstimate(flops=0, bytes_accessed=1200 * block * cols, transcendentals=0),
        name=f"ring_scatter_{ident}",
    )(left, right)


FFN_ROWS = 256


def col_tiles(n, want):
    return [(at, min(want, n - at)) for at in range(0, n, want)]


def ffn_forward_body(slots, x_ref, gate_ref, up_ref, w_ref, act_ref, slope_ref, hid_ref, full_ref, *sems):
    step, steps = pl.program_id(0), pl.num_programs(0)
    gather = Gather(w_ref, full_ref, *sems)

    @pl.when(step == 0)
    def _():
        greet_near(gather.me, gather.outer, gather.side)
        gather.begin()

    x = x_ref[...]
    for part, (at, wide) in enumerate(col_tiles(gate_ref.shape[1], 512)):
        gather.steps(*spread(gather.STEPS, 3 * step + part, 3 * slots))
        gate = mm(x, gate_ref[:, at : at + wide])
        up = mm(x, up_ref[:, at : at + wide])
        sg = sigmoid(gate)
        act = gate * sg
        act_ref[:, at : at + wide] = act.astype(BF)
        slope_ref[:, at : at + wide] = (up * (sg * (1.0 + gate * (1.0 - sg)))).astype(BF)
        hid_ref[:, at : at + wide] = (act * up).astype(BF)

    @pl.when(step == steps - 1)
    def _():
        gather.finish()


def ffn_forward(x, full_gate, full_up, w, ident):
    length, ff = x.shape[0], full_gate.shape[1]
    any_ref = pl.BlockSpec(memory_space=pl.ANY)
    once = pl.BlockSpec(full_gate.shape, lambda c: (0, 0), pipeline_mode=pl.Buffered(1))
    tile = pl.BlockSpec((FFN_ROWS, ff), lambda c: (c, 0))
    return pl.pallas_call(
        functools.partial(ffn_forward_body, length // FFN_ROWS),
        grid=(length // FFN_ROWS,),
        in_specs=[pl.BlockSpec((FFN_ROWS, x.shape[1]), lambda c: (c, 0)), once, once, any_ref],
        out_specs=[tile] * 3 + [any_ref],
        out_shape=[jax.ShapeDtypeStruct((length, ff), BF)] * 3
        + [jax.ShapeDtypeStruct((8 * w.shape[0], w.shape[1]), w.dtype)],
        scratch_shapes=gather_sems(),
        compiler_params=pltpu.CompilerParams(
            dimension_semantics=("arbitrary",), vmem_limit_bytes=60 << 20, collective_id=ident, has_side_effects=True
        ),
        cost_estimate=pl.CostEstimate(flops=70_000_000_000, bytes_accessed=30_000_000, transcendentals=1_500_000),
        name="ffn_forward",
    )(x, full_gate, full_up, w)


def ffn_backward_body(
    left_ref, hid_ref, act_ref, slope_ref, down_hbm, gate_hbm, up_hbm,
    glow_ref, ulow_ref, back_ref, ffn_ref, out_ref, down_ref, gate_ref, up_ref, load_sem, *scratch,
):
    step, steps = pl.program_id(0), pl.num_programs(0)
    scatter = Scatter(2, CHUNKS, left_ref, hid_ref, out_ref, *scratch)
    loads = [
        pltpu.make_async_copy(src, dst, load_sem.at[i])
        for i, (src, dst) in enumerate(((down_hbm, down_ref), (gate_hbm, gate_ref), (up_hbm, up_ref)))
    ]

    @pl.when(step == 0)
    def _():
        greet_near(scatter.me, scatter.outer, scatter.side)
        for copy in loads:
            copy.start()
        scatter.begin()
        loads[0].wait()

    rows = pl.ds(pl.multiple_of(step * FFN_ROWS, FFN_ROWS), FFN_ROWS)
    x = left_ref[rows, :]
    for at, wide in col_tiles(down_ref.shape[1], 512):
        cols = slice(at, at + wide)
        grad = mm(x, down_ref[:, cols])
        glow_ref[:, cols] = (grad * slope_ref[:, cols].astype(F32)).astype(BF)
        ulow_ref[:, cols] = (grad * act_ref[:, cols].astype(F32)).astype(BF)

    @pl.when(step == 0)
    def _():
        loads[1].wait()
        loads[2].wait()

    hid = hid_ref[rows, :]
    glow, ulow = glow_ref[...], ulow_ref[...]
    for part, (at, wide) in enumerate(col_tiles(down_ref.shape[0], 512)):
        scatter.steps(*spread(scatter.last, 4 * step + part, 4 * (left_ref.shape[0] // FFN_ROWS)))
        cols = slice(at, at + wide)
        back_ref[:, cols] = (mm(glow, gate_ref[cols, :], NT) + mm(ulow, up_ref[cols, :], NT)).astype(BF)
        ffn_ref[:, cols] = mm(hid, down_ref[cols, :], NT).astype(BF)

    @pl.when(step == steps - 1)
    def _():
        scatter.finish()


def ffn_backward(left, hidden, act, slope, full_down, full_gate, full_up, ident):
    (length, width), ff = left.shape, hidden.shape[1]
    once = lambda x: pl.BlockSpec(x.shape, lambda c: (0, 0), pipeline_mode=pl.Buffered(1))
    tile = pl.BlockSpec((FFN_ROWS, ff), lambda c: (c, 0))
    wide = pl.BlockSpec((FFN_ROWS, width), lambda c: (c, 0))
    mine = (width // 8, ff)
    return pl.pallas_call(
        ffn_backward_body,
        grid=(length // FFN_ROWS,),
        in_specs=[once(left), once(hidden), tile, tile] + [pl.BlockSpec(memory_space=pl.ANY)] * 3,
        out_specs=[tile, tile, wide, wide, pl.BlockSpec(mine, lambda c: (0, 0))],
        out_shape=[jax.ShapeDtypeStruct((length, ff), BF)] * 2
        + [jax.ShapeDtypeStruct((length, width), BF)] * 2
        + [jax.ShapeDtypeStruct(mine, F32)],
        scratch_shapes=[pltpu.VMEM(full_down.shape, BF)] * 3
        + [pltpu.SemaphoreType.DMA((3,))]
        + scatter_scratch(*mine, CHUNKS),
        compiler_params=pltpu.CompilerParams(
            dimension_semantics=("arbitrary",), vmem_limit_bytes=62 << 20, collective_id=ident, has_side_effects=True
        ),
        cost_estimate=pl.CostEstimate(flops=90_000_000_000, bytes_accessed=50_000_000, transcendentals=0),
        name="ffn_backward",
    )(left, hidden, act, slope, full_down, full_gate, full_up)


def plain_dot(left_mat, right_mat):
    return jnp.dot(left_mat, right_mat, preferred_element_type=F32)


def dot_rows(left_mat, right_mat):
    return lax.dot_general(left_mat, right_mat, (((1,), (1,)), ((), ())), preferred_element_type=F32)


def dot_tokens(left_mat, right_mat):
    return lax.dot_general(left_mat, right_mat, (((0,), (0,)), ((), ())), preferred_element_type=F32)


def rms_apply(values, gain_vec):
    return values * lax.rsqrt(jnp.mean(values * values, axis=-1, keepdims=True) + 1e-05) * gain_vec


class RingRows:
    def __init__(self, dp_size):
        self.outer = dp_size // 2
        self.index = lax.axis_index("dp")

    def _roll(self, x, axis, blocks):
        size = x.shape[axis] // self.outer * blocks
        return jnp.concatenate(
            [lax.slice_in_dim(x, size, None, axis=axis), lax.slice_in_dim(x, 0, size, axis=axis)], axis
        )

    def reorder(self, x, axis):
        outer_at, pair_at = self.index // 2, self.index % 2
        size = x.shape[axis] // (2 * self.outer)
        cut = [lax.slice_in_dim(x, b * size, (b + 1) * size, axis=axis) for b in range(2 * self.outer)]
        even, odd = jnp.concatenate(cut[0::2], axis), jnp.concatenate(cut[1::2], axis)
        sides = [jnp.where(pair_at == 0, even, odd), jnp.where(pair_at == 0, odd, even)]
        bit = 1
        while bit < self.outer:
            sides = [jnp.where((outer_at // bit) % 2 == 1, self._roll(s, axis, bit), s) for s in sides]
            bit *= 2
        return jnp.concatenate(sides, axis)

    def restore(self, x, axis):
        outer_at, pair_at = self.index // 2, self.index % 2
        half = x.shape[axis] // 2
        sides = [lax.slice_in_dim(x, 0, half, axis=axis), lax.slice_in_dim(x, half, None, axis=axis)]
        bit = 1
        while bit < self.outer:
            sides = [
                jnp.where((outer_at // bit) % 2 == 1, self._roll(s, axis, self.outer - bit), s) for s in sides
            ]
            bit *= 2
        even = jnp.where(pair_at == 0, sides[0], sides[1])
        odd = jnp.where(pair_at == 0, sides[1], sides[0])
        size = half // self.outer
        cut = []
        for b in range(self.outer):
            cut += [lax.slice_in_dim(s, b * size, (b + 1) * size, axis=axis) for s in (even, odd)]
        return jnp.concatenate(cut, axis)

    def _swap(self, x):
        return lax.ppermute(x, "dp", [(i, i ^ 1) for i in range(2 * self.outer)])

    def gather_first(self, w, small):
        return ring_gather(w, 0, small)

    def gather(self, w, ident):
        return ring_gather(w, ident)

    def scatter(self, left, right, ident):
        return ring_scatter(left, right, ident)

    def ffn_forward(self, x, gate, up, w, ident):
        return ffn_forward(x, gate, up, w, ident)

    def ffn_backward(self, left, hidden, act, slope, down, gate, up, ident):
        return ffn_backward(left, hidden, act, slope, down, gate, up, ident)

    def forward(self, core_in, w, ident):
        return mixer_forward(*core_in, w, ident)

    def backward(self, core_in, saved, left, right, ident):
        return mixer_backward(*core_in, *saved, left, right, ident)

    def scatter_last(self, *args):
        return ring_scatter_last(*args)


class PlainRows:
    def reorder(self, x, axis):
        return x

    def restore(self, x, axis):
        return x

    def gather(self, w, ident):
        return lax.all_gather(w, "dp", axis=0, tiled=True)

    def scatter(self, left, right, ident):
        full = dot_tokens(left, right).astype(BF)
        return lax.psum_scatter(full, "dp", scatter_dimension=0, tiled=True).astype(F32)

    def gather_first(self, w, small):
        return lax.all_gather(w, "dp", axis=0, tiled=True), lax.all_gather(small, "dp", axis=0)

    def ffn_forward(self, x, gate, up, w, ident):
        gate_pre, up_pre = plain_dot(x, gate), plain_dot(x, up)
        sg = jax.nn.sigmoid(gate_pre)
        act = gate_pre * sg
        slope = up_pre * (sg * (1.0 + gate_pre * (1.0 - sg)))
        return act.astype(BF), slope.astype(BF), (act * up_pre).astype(BF), self.gather(w, ident)

    def ffn_backward(self, left, hidden, act, slope, down, gate, up, ident):
        grad = plain_dot(left, down)
        gate_low, up_low = (grad * slope.astype(F32)).astype(BF), (grad * act.astype(F32)).astype(BF)
        back = (dot_rows(gate_low, gate) + dot_rows(up_low, up)).astype(BF)
        return gate_low, up_low, back, dot_rows(hidden, down).astype(BF), self.scatter(left, hidden, ident)

    def forward(self, core_in, w, ident):
        return [*mixer_forward(*core_in), self.gather(w, ident)]

    def backward(self, core_in, saved, left, right, ident):
        return [*mixer_backward(*core_in, *saved), self.scatter(left, right, ident)]

    def scatter_last(self, left, right, ab, few, taps, rest, z, mid, gain, full_ab, full, widths, t_size, ident):
        summed = (dot_rows(right, full) + dot_rows(ab, full_ab)).astype(BF)
        grad, grad_gain = jax.vjp(rms_apply, z, gain[0])[1](tensor_scatter(summed).astype(F32))
        few, taps = (lax.psum_scatter(x, "dp", scatter_dimension=0, tiled=True)[0] for x in (few, taps))
        vec = lax.psum(jnp.concatenate([grad_gain.reshape(-1, LANES), rest]), ("dp", "tensor"))
        out, found, at = self.scatter(left, right, ident), [], 0
        for width in widths:
            found.append(out[:, at : at + width])
            at += width
        return *found, few, taps, vec, mid + grad


def tie(value, *others):
    return lax.optimization_barrier((value, others))[0]


def tensor_gather(x):
    return lax.all_gather(x, "tensor", axis=0, tiled=True)


def tensor_scatter(x):
    return lax.psum_scatter(x, "tensor", scatter_dimension=0, tiled=True)


def shards(
    dp_size, tensor_size, inputs, cotangent, lengths, norm1_gain, w_query, w_key, w_value, w_outgate, w_beta, w_alpha,
    conv_query, conv_key, conv_value, a_log, dt_bias, head_gain, w_out, norm2_gain, w_gate, w_up, w_down,
):
    rows = RingRows(dp_size) if dp_size == 8 else PlainRows()
    heads = w_beta.shape[1]
    wide_k, wide_v = w_query.shape[1], w_value.shape[1]
    dk, dv = wide_k // heads, wide_v // heads
    taps_n = conv_query.shape[2]
    block = w_query.shape[0]
    tensor_pos = lax.axis_index("tensor")
    head_start = tensor_pos * heads

    row_count = inputs.shape[1]
    positions = tensor_pos * row_count + jnp.arange(row_count, dtype=jnp.int32)
    valid_rows = (positions < lengths[0]).astype(F32)[:, None]

    def by_head(conv):
        return jnp.transpose(conv, (1, 2, 0)).reshape(-1)

    small = jnp.concatenate(
        [w_beta.T.reshape(-1), w_alpha.T.reshape(-1), by_head(conv_query), by_head(conv_key), by_head(conv_value)]
    )
    cuts = [0]
    for part in (w_beta, w_alpha, conv_query, conv_key, conv_value):
        cuts.append(cuts[-1] + part.size)
    small = jnp.pad(small, (0, -small.size % (32 * LANES))).reshape(-1, LANES)
    full_raw, small = rows.gather_first(
        jnp.concatenate([w_query, w_key, w_value, w_outgate], axis=1), small
    )
    small = small.reshape(dp_size, -1)
    few = small[:, : cuts[2]].reshape(dp_size, 2 * heads, block)
    full_ab = jnp.transpose(few, (1, 0, 2)).reshape(2 * heads, dp_size * block).T
    full_ab = jnp.pad(full_ab, ((0, 0), (0, LANES - 2 * heads)))
    taps_all = rows.restore(small[:, cuts[2] : cuts[5]], 0).astype(F32)

    def tap_table(at, size):
        table = taps_all[:, at - cuts[2] : at - cuts[2] + taps_n * heads * size // dp_size]
        table = jnp.transpose(table.reshape(dp_size, heads, taps_n, size // dp_size), (2, 1, 0, 3))
        return jnp.pad(table.reshape(taps_n, heads * size), ((0, 8 - taps_n), (0, 0)))

    tq, tk, tv = tap_table(cuts[2], dk), tap_table(cuts[3], dk), tap_table(cuts[4], dv)
    alog_local = lax.dynamic_slice_in_dim(a_log, head_start, heads)
    dtb_local = lax.dynamic_slice_in_dim(dt_bias, head_start, heads)
    par = jnp.pad(jnp.stack([alog_local, dtb_local]), ((0, 6), (heads, LANES - 2 * heads)))
    gain = head_gain[None]

    local_rows = rows.reorder(inputs[0], 1).astype(F32)
    gain_one = rows.reorder(norm1_gain[None], 1)[0]
    gain_two = rows.reorder(norm2_gain[None], 1)[0]
    normed_one = rms_apply(local_rows, gain_one)
    rows_one = tensor_gather(normed_one.astype(BF))
    grad_after = valid_rows * rows.reorder(cotangent[0], 1).astype(F32)
    incoming_ffn = tensor_gather(grad_after.astype(BF))

    ab_raw = plain_dot(rows_one, full_ab)
    core_in = (plain_dot(rows_one, full_raw), ab_raw, tq, tk, tv, par, gain)
    head_bf, delta_out, new_values, inverses, states, full_out = rows.forward(core_in, w_out, 1)
    mixed = dot_rows(head_bf, full_out).astype(BF)
    full_gate = rows.gather(tie(w_gate, mixed), 2)
    after_mix = local_rows + tie(tensor_scatter(mixed), full_gate).astype(F32)
    normed_two, norm_two_back = jax.vjp(rms_apply, after_mix, gain_two)
    normed_two = normed_two.astype(BF)
    full_up = rows.gather(tie(w_up, normed_two), 3)
    rows_two = tie(tensor_gather(normed_two), full_up)
    act, slope, hidden, full_down = rows.ffn_forward(rows_two, full_gate, full_up, w_down, 4)

    gate_low, up_low, back_two, ffn_out, out_down = rows.ffn_backward(
        incoming_ffn, hidden, act, slope, full_down, full_gate, full_up, 5
    )
    out_gate = rows.scatter(tie(rows_two, back_two), gate_low, 6)
    grad_normed_two = tie(tensor_scatter(back_two), out_gate).astype(F32)
    grad_mid, grad_norm2 = norm_two_back(grad_normed_two)
    grad_mid = grad_mid + grad_after
    grad_mix = grad_mid.astype(BF)
    out_up = rows.scatter(tie(rows_two, grad_mix), up_low, 7)
    incoming_mix = tie(tensor_gather(grad_mix), out_up)

    ffn_part = tensor_scatter(tie(ffn_out, incoming_mix)).astype(F32)
    outputs = rows.restore(((after_mix + ffn_part) * valid_rows).astype(BF), 1)[None]
    raw_low, ab_low, dtq, dtk, dtv, dpar, dgain, out_out = rows.backward(
        core_in, (plain_dot(incoming_mix, full_out), delta_out, new_values, inverses, states), incoming_mix, head_bf, 8
    )
    def in_lanes(x, lead):
        return jnp.pad(x, ((0, 0), (0, -x.shape[1] % (8 * LANES)))).reshape(lead + (-1, LANES))

    grad_ab = dot_tokens(ab_low, rows_one)[: 2 * heads].reshape(2 * heads, dp_size, block)
    few = [jnp.transpose(grad_ab, (1, 0, 2)).reshape(dp_size, -1)]

    def tap_grad(table, size):
        grad = table[:taps_n].reshape(taps_n, heads, dp_size, size // dp_size)
        return jnp.transpose(grad, (2, 1, 0, 3)).reshape(dp_size, -1)

    taps = [tap_grad(dtq, dk), tap_grad(dtk, dk), tap_grad(dtv, dv)]
    alog_full, dtb_full = (
        lax.dynamic_update_slice_in_dim(jnp.zeros_like(a_log), dpar[i, heads : 2 * heads], head_start, 0)
        for i in range(2)
    )
    rest = [rows.restore(grad_norm2[None], 1)[0], dgain[0], alog_full, dtb_full]
    few, taps, rest_in = (jnp.concatenate(x, axis=-1) for x in (few, taps, rest))
    out_query, out_key, out_value, out_outgate, few_sum, tap_sum, vec_sum, grad_inputs = rows.scatter_last(
        tie(rows_one, out_out), raw_low, ab_low, in_lanes(few, (dp_size,)), in_lanes(taps, (dp_size,)),
        in_lanes(rest_in[None], ()), local_rows, grad_mid, gain_one[None], full_ab, full_raw,
        (wide_k, wide_k, wide_v, wide_v), tensor_size, 9,
    )

    def pieces_of(total, like):
        flat, found, at = total.reshape(-1), [], 0
        for part in like:
            found.append(flat[at : at + part.size])
            at += part.size
        return found

    grad_ab = few_sum.reshape(-1)[: cuts[2]].reshape(2 * heads, block)
    out_beta, out_alpha = grad_ab[:heads].T, grad_ab[heads:].T
    out_cq, out_ck, out_cv = (
        jnp.transpose(x.reshape(heads, taps_n, -1), (2, 0, 1))
        for x in pieces_of(tap_sum, (conv_query, conv_key, conv_value))
    )
    norm1_sum, norm2_sum, hgain_sum, alog_sum, dtb_sum = pieces_of(vec_sum, [norm1_gain] + rest)
    return (
        outputs, grad_inputs[None], norm1_sum, out_query, out_key, out_value, out_outgate,
        out_beta, out_alpha, out_cq, out_ck, out_cv, alog_sum, dtb_sum, hgain_sum, out_out, norm2_sum,
        out_gate, out_up, out_down,
    )


def solution(mesh):
    mat, cube, whole = P("dp", "tensor"), P("dp", "tensor", None), P()
    in_specs = (
        (cube, cube, P("dp"), whole) + (mat,) * 6 + (cube,) * 3 + (whole,) * 3 + (mat, whole) + (mat,) * 3
    )
    out_specs = (
        (cube, cube, whole) + (mat,) * 6 + (cube,) * 3 + (whole,) * 3 + (mat, whole) + (mat,) * 3
    )
    return jax.shard_map(
        functools.partial(shards, mesh.shape["dp"], mesh.shape["tensor"]), mesh=mesh, in_specs=in_specs, out_specs=out_specs,
        check_vma=False,
    )
```

```python
import functools

import jax
import jax.numpy as jnp
from jax import lax
from jax.experimental import pallas as pl
from jax.experimental.pallas import tpu as pltpu
from jax.sharding import PartitionSpec as P

CH = 128
HALO = 8
MIXER_CHUNKS = 4
LANES = 128
F32 = jnp.float32
BF = jnp.bfloat16


def mm(a, b, dims=((1,), (0,))):
    return lax.dot_general(a, b, (dims, ((), ())), preferred_element_type=F32)


NT = ((1,), (1,))
TN = ((0,), (0,))


def split(x):
    hi = x.astype(BF)
    return hi, (x - hi.astype(F32)).astype(BF)


def mm3(a, b):
    return mm(a[0], b[0]) + (mm(a[0], b[1]) + mm(a[1], b[0]))


def exact_mm(a, b):
    return lax.dot_general(
        a, b, (((1,), (0,)), ((), ())), precision=lax.Precision.HIGHEST, preferred_element_type=F32
    )


def unit_lower_inverse(mats):
    n = mats[0].shape[0]
    row = lax.broadcasted_iota(jnp.int32, (n, n), 0)
    col = lax.broadcasted_iota(jnp.int32, (n, n), 1)

    def off_block(size):
        same = (row // (2 * size)) == (col // (2 * size))
        return same & ((row // size) % 2 == 1) & ((col // size) % 2 == 0)

    eye = jnp.where(row == col, 1.0, 0.0)
    inv = [eye - jnp.where(off_block(1), a, 0.0) for a in mats]
    size = 2
    while size < n:
        mask = off_block(size)
        halves = [split(x) for x in inv]
        low = [split(jnp.where(mask, a, 0.0)) for a in mats]
        mid = [split(mm3(b, x)) for b, x in zip(low, halves)]
        inv = [x - mm3(xs, y) for x, xs, y in zip(inv, halves, mid)]
        size *= 2
    return inv


def softplus(x):
    return jnp.maximum(x, 0.0) + jnp.log1p(jnp.exp(-jnp.abs(x)))


def sigmoid(x):
    return 0.5 * jnp.tanh(0.5 * x) + 0.5


def conv_of(buf, taps, rows):
    out = buf[HALO - 3 : HALO - 3 + rows, :] * taps[0:1, :]
    for i in range(1, 4):
        out = out + buf[HALO - 3 + i : HALO - 3 + i + rows, :] * taps[i : i + 1, :]
    return out


def decay_tables(ab, par, rows):
    beta = sigmoid(ab)
    decay = -jnp.exp(par[0:1, :]) * softplus(ab + par[1:2, :])
    row = lax.broadcasted_iota(jnp.int32, (rows, rows), 0)
    col = lax.broadcasted_iota(jnp.int32, (rows, rows), 1)
    run = exact_mm(jnp.where(row >= col, 1.0, 0.0), decay)
    return beta, decay, run, jnp.transpose(run), row, col


def fwd_body(
    heads, dk, dv, q_ref, k_ref, v_ref, og_ref, ab_ref, tq_ref, tk_ref, tv_ref, par_ref, gain_ref,
    head_ref, o_ref, u_ref, t_ref, s_ref, qb, kb, vb, state, between=lambda part: None,
):
    rows = CH

    @pl.when(pl.program_id(0) == 0)
    def _():
        for buf in (qb, kb, vb):
            buf[0:HALO, :] = jnp.zeros((HALO, buf.shape[1]), F32)
        state[...] = jnp.zeros_like(state)

    hs = range(heads)
    raw = []
    for buf, ref, taps in ((qb, q_ref, tq_ref), (kb, k_ref, tk_ref), (vb, v_ref, tv_ref)):
        buf[HALO : HALO + rows, :] = ref[...]
        raw.append(conv_of(buf, taps, rows))
        buf[0:HALO, :] = buf[rows : rows + HALO, :]
    zq, zk, zv = raw
    beta, _, run, run_t, row, col = decay_tables(ab_ref[...], par_ref, rows)
    low_inc = row >= col
    low_strict = row > col
    scale = dk ** (-0.5)

    def unit(z):
        y = z * sigmoid(z)
        return y * lax.rsqrt(jnp.sum(y * y, axis=-1, keepdims=True) + 1e-6)

    q = [unit(zq[:, h * dk : (h + 1) * dk]) * scale for h in hs]
    k = [unit(zk[:, h * dk : (h + 1) * dk]) for h in hs]
    qk_b = [(a.astype(BF), b.astype(BF)) for a, b in zip(q, k)]
    bt = [beta[:, h : h + 1] for h in hs]
    g_col = [run[:, heads + h : heads + h + 1] for h in hs]
    g_row = [run_t[heads + h : heads + h + 1, :] for h in hs]
    dec = [jnp.where(low_inc, jnp.exp(jnp.where(low_inc, g_col[h] - g_row[h], 0.0)), 0.0) for h in hs]
    kk = [mm(qk_b[h][1], qk_b[h][1], NT) for h in hs]
    inv = unit_lower_inverse([jnp.where(low_strict, bt[h] * dec[h] * kk[h], 0.0) for h in hs])
    inv_b = [x.astype(BF) for x in inv]
    between(1)
    p_b = [(mm(qk_b[h][0], qk_b[h][1], NT) * dec[h]).astype(BF) for h in hs]
    start = [jnp.exp(g) for g in g_col]
    end = [run[rows - 1 : rows, heads + h : heads + h + 1] for h in hs]
    s0 = [state[h] for h in hs]
    s0_b = [x.astype(BF) for x in s0]
    for h in hs:
        t_ref[:, h * rows : (h + 1) * rows] = inv_b[h]
        s_ref[:, h * dv : (h + 1) * dv] = s0_b[h]
    rhs = []
    for h in hs:
        z = zv[:, h * dv : (h + 1) * dv]
        val = z * sigmoid(z)
        rhs.append((bt[h] * val - (bt[h] * start[h]) * mm(qk_b[h][1], s0_b[h])).astype(BF))
    u_b = [mm(inv_b[h], rhs[h]).astype(BF) for h in hs]
    for h in hs:
        u_ref[:, h * dv : (h + 1) * dv] = u_b[h]
        tail = (k[h] * jnp.exp(end[h] - g_col[h])).astype(BF)
        state[h] = jnp.exp(end[h]) * s0[h] + mm(tail, u_b[h], TN)
    for h in hs:
        o = start[h] * mm(qk_b[h][0], s0_b[h]) + mm(p_b[h], u_b[h])
        o_ref[:, h * dv : (h + 1) * dv] = o
        og = og_ref[:, h * dv : (h + 1) * dv]
        r = lax.rsqrt(jnp.mean(o * o, axis=-1, keepdims=True) + 1e-5)
        head_ref[:, h * dv : (h + 1) * dv] = (o * r * gain_ref[...] * (og * sigmoid(og))).astype(BF)


def bwd_body(
    heads, dk, dv, q_ref, k_ref, v_ref, og_ref, ab_ref, qh_ref, kh_ref, vh_ref,
    tq_ref, tk_ref, tv_ref, par_ref, gain_ref, g_ref, o_ref, u_ref, t_ref, s_ref,
    draw_ref, dab_ref, dtq_ref, dtk_ref, dtv_ref, dpar_ref, dgain_ref,
    qb, kb, vb, qn, kn, vn, dstate, between=lambda part: None,
):
    rows = CH
    step = pl.program_id(0)
    first = step == 0
    is_top = step == pl.num_programs(0) - 1

    @pl.when(first)
    def _():
        for buf in (qn, kn, vn):
            buf[rows : rows + HALO, :] = jnp.zeros((HALO, buf.shape[1]), F32)
        for ref in (dtq_ref, dtk_ref, dtv_ref, dpar_ref, dgain_ref, dstate):
            ref[...] = jnp.zeros_like(ref)

    hs = range(heads)
    raw = []
    for buf, ref, halo, taps in (
        (qb, q_ref, qh_ref, tq_ref), (kb, k_ref, kh_ref, tk_ref), (vb, v_ref, vh_ref, tv_ref)
    ):
        buf[0:HALO, :] = jnp.where(is_top, 0.0, halo[...])
        buf[HALO : HALO + rows, :] = ref[...]
        raw.append(conv_of(buf, taps, rows))
    zq, zk, zv = raw
    ab = ab_ref[...]
    beta, decay, run, run_t, row, col = decay_tables(ab, par_ref, rows)
    low_inc = row >= col
    low_strict = row > col
    scale = dk ** (-0.5)

    def unit(z):
        sg = sigmoid(z)
        y = z * sg
        n = lax.rsqrt(jnp.sum(y * y, axis=-1, keepdims=True) + 1e-6)
        return y * n, n, sg * (1.0 + z * (1.0 - sg))

    qu = [unit(zq[:, h * dk : (h + 1) * dk]) for h in hs]
    ku = [unit(zk[:, h * dk : (h + 1) * dk]) for h in hs]
    q = [x[0] * scale for x in qu]
    k = [x[0] for x in ku]
    q_b = [x.astype(BF) for x in q]
    k_b = [x.astype(BF) for x in k]
    bt = [beta[:, h : h + 1] for h in hs]
    g_col = [run[:, heads + h : heads + h + 1] for h in hs]
    g_row = [run_t[heads + h : heads + h + 1, :] for h in hs]
    dec = [jnp.where(low_inc, jnp.exp(jnp.where(low_inc, g_col[h] - g_row[h], 0.0)), 0.0) for h in hs]
    start = [jnp.exp(g) for g in g_col]
    end = [run[rows - 1 : rows, heads + h : heads + h + 1] for h in hs]
    tail = [jnp.exp(end[h] - g_col[h]) for h in hs]
    dkk = [mm(k_b[h], k_b[h], NT) * dec[h] for h in hs]
    prob = [mm(q_b[h], k_b[h], NT) * dec[h] for h in hs]
    u_b = [u_ref[:, h * dv : (h + 1) * dv] for h in hs]
    s0_b = [s_ref[:, h * dv : (h + 1) * dv] for h in hs]
    ds1 = [dstate[h] for h in hs]
    ds1_b = [x.astype(BF) for x in ds1]

    gain = gain_ref[...]
    og_at = 2 * heads * dk + heads * dv
    do_b = []
    dgain = jnp.zeros_like(gain)
    for h in hs:
        sl = slice(h * dv, (h + 1) * dv)
        o = o_ref[:, sl]
        og = og_ref[:, sl]
        g = g_ref[:, sl]
        r = lax.rsqrt(jnp.mean(o * o, axis=-1, keepdims=True) + 1e-5)
        sg = sigmoid(og)
        gor = g * (o * r)
        dgain = dgain + jnp.sum(gor * (og * sg), axis=0, keepdims=True)
        draw_ref[:, og_at + h * dv : og_at + (h + 1) * dv] = (gor * gain * (sg * (1.0 + og * (1.0 - sg)))).astype(BF)
        m = g * gain * (og * sg)
        d_o = r * m - o * (r * r * r * jnp.mean(m * o, axis=-1, keepdims=True))
        do_b.append(d_o.astype(BF))
    dgain_ref[...] += dgain

    d_u = [
        mm(prob[h].astype(BF), do_b[h], TN) + mm((k[h] * tail[h]).astype(BF), ds1_b[h]) for h in hs
    ]
    d_r = [mm(t_ref[:, h * rows : (h + 1) * rows], d_u[h].astype(BF), TN) for h in hs]
    dr_b = [x.astype(BF) for x in d_r]
    for h in hs:
        left = jnp.concatenate(
            [(q[h] * start[h]).astype(BF), (k[h] * (-(bt[h] * start[h]))).astype(BF)], axis=0
        )
        right = jnp.concatenate([do_b[h], dr_b[h]], axis=0)
        dstate[h] = jnp.exp(end[h]) * ds1[h] + mm(left, right, TN)

    between(1)
    lane = lax.broadcasted_iota(jnp.int32, (rows, LANES), 1)
    sub = lax.broadcasted_iota(jnp.int32, (LANES, rows), 0)
    dab_cols = jnp.zeros((rows, LANES), F32)
    dg_cols = jnp.zeros((rows, LANES), F32)
    dg_rows = jnp.zeros((LANES, rows), F32)
    dend = jnp.zeros((1, LANES), F32)
    lane_one = lax.broadcasted_iota(jnp.int32, (1, LANES), 1)
    for h in hs:
        sl = slice(h * dv, (h + 1) * dv)
        ks = slice(h * dk, (h + 1) * dk)
        d_p = jnp.where(low_inc, mm(do_b[h], u_b[h], NT), 0.0)
        d_a = jnp.where(low_strict, -mm(dr_b[h], u_b[h], NT), 0.0)
        pp = d_p * prob[h]
        dqk_b = (d_p * dec[h]).astype(BF)
        ad = d_a * dkk[h]
        d_kk = d_a * (bt[h] * dec[h])
        d_kk = (d_kk + jnp.transpose(d_kk)).astype(BF)
        y = mm(do_b[h], s0_b[h], NT)
        x = mm(dr_b[h], s0_b[h], NT)
        z = mm(u_b[h], ds1_b[h], NT)
        dq = mm(dqk_b, k_b[h]) + start[h] * y
        bstart = bt[h] * start[h]
        kx = jnp.sum(k[h] * x, axis=-1, keepdims=True)
        kz = tail[h] * jnp.sum(k[h] * z, axis=-1, keepdims=True)
        dkey = mm(d_kk, k_b[h]) + mm(dqk_b, q_b[h], TN) - bstart * x + tail[h] * z
        zval = zv[:, sl]
        sgv = sigmoid(zval)
        val = zval * sgv
        ad_row = jnp.sum(ad, axis=-1, keepdims=True)
        d_beta = jnp.sum(d_r[h] * val, axis=-1, keepdims=True) - start[h] * kx + ad_row
        d_g = (
            jnp.sum(pp, axis=-1, keepdims=True)
            + bt[h] * ad_row
            + start[h] * jnp.sum(q[h] * y, axis=-1, keepdims=True)
            - bstart * kx
            - kz
        )
        d_g_row = -jnp.sum(pp + bt[h] * ad, axis=0, keepdims=True)
        d_end = jnp.sum(kz, axis=0, keepdims=True) + jnp.exp(end[h]) * jnp.sum(
            jnp.sum(s0_b[h].astype(F32) * ds1[h], axis=-1, keepdims=True), axis=0, keepdims=True
        )
        dab_cols = dab_cols + jnp.where(lane == h, d_beta, 0.0)
        dg_cols = dg_cols + jnp.where(lane == heads + h, d_g, 0.0)
        dg_rows = dg_rows + jnp.where(sub == heads + h, d_g_row, 0.0)
        dend = dend + jnp.where(lane_one == heads + h, d_end, 0.0)
        vn[0:rows, sl] = (bt[h] * d_r[h]) * (sgv * (1.0 + zval * (1.0 - sgv)))
        for buf, du, (un, n, slope) in ((qn, dq * scale, qu[h]), (kn, dkey, ku[h])):
            dy = n * (du - un * jnp.sum(un * du, axis=-1, keepdims=True))
            buf[0:rows, ks] = dy * slope

    d_run = dg_cols + jnp.transpose(dg_rows)
    d_decay = exact_mm(jnp.where(col >= row, 1.0, 0.0), d_run) + dend
    pick = (lane >= heads) & (lane < 2 * heads)
    d_decay = jnp.where(pick, d_decay, 0.0)
    d_alpha = d_decay * (-jnp.exp(par_ref[0:1, :])) * sigmoid(ab + par_ref[1:2, :])
    dpar_ref[0:1, :] += jnp.sum(d_decay * decay, axis=0, keepdims=True)
    dpar_ref[1:2, :] += jnp.sum(d_alpha, axis=0, keepdims=True)
    dab_ref[...] = (dab_cols * beta * (1.0 - beta) + d_alpha).astype(BF)

    wide = heads * dk
    for buf, cur, taps, out, at, dtap in (
        (qn, qb, tq_ref, draw_ref, 0, dtq_ref),
        (kn, kb, tk_ref, draw_ref, wide, dtk_ref),
        (vn, vb, tv_ref, draw_ref, 2 * wide, dtv_ref),
    ):
        here = cur[HALO : HALO + rows, :]
        total = None
        for i in range(4):
            moved = buf[3 - i : 3 - i + rows, :]
            term = moved * taps[i : i + 1, :]
            total = term if total is None else total + term
            dtap[i : i + 1, :] += jnp.sum(here * moved, axis=0, keepdims=True)
        out[:, at : at + total.shape[1]] = total.astype(BF)
        buf[rows : rows + HALO, :] = buf[0:HALO, :]


def mixer_specs(heads, dk, dv, at):
    wide_k, wide_v = heads * dk, heads * dv
    full = lambda shape: pl.BlockSpec(shape, lambda c: (0,) * len(shape))
    return {
        "q": pl.BlockSpec((CH, wide_k), lambda c: (at(c), 0)),
        "k": pl.BlockSpec((CH, wide_k), lambda c: (at(c), 1)),
        "val": pl.BlockSpec((CH, wide_v), lambda c: (at(c), 2 * wide_k // wide_v)),
        "og": pl.BlockSpec((CH, wide_v), lambda c: (at(c), 2 * wide_k // wide_v + 1)),
        "raw": pl.BlockSpec((CH, 2 * (wide_k + wide_v)), lambda c: (at(c), 0)),
        "v": pl.BlockSpec((CH, wide_v), lambda c: (at(c), 0)),
        "ab": pl.BlockSpec((CH, LANES), lambda c: (at(c), 0)),
        "t": pl.BlockSpec((CH, heads * CH), lambda c: (at(c), 0)),
        "s": pl.BlockSpec((None, dk, wide_v), lambda c: (at(c), 0, 0)),
        "tk": full((8, wide_k)),
        "tv": full((8, wide_v)),
        "par": full((8, LANES)),
        "gain": full((1, dv)),
    }


def fwd_gather_body(length, heads, dk, dv, *refs):
    ins, w_ref, outs, full_ref, rest = refs[:10], refs[10], refs[11:16], refs[16], refs[17:]
    step, steps = pl.program_id(0), pl.num_programs(0)
    gather = Gather(w_ref, full_ref, *rest[4:])

    @pl.when(step == 0)
    def _():
        greet_near(gather.me, gather.outer, gather.side)
        gather.begin()

    def between(part):
        gather.steps(*spread(gather.STEPS, 2 * step + part, 2 * (length // CH)))

    between(0)
    fwd_body(heads, dk, dv, *ins, *outs, *rest[:4], between)

    @pl.when(step == steps - 1)
    def _():
        gather.finish()


def bwd_scatter_body(length, heads, dk, dv, *refs):
    ins, pair, outs, own, rest = refs[:18], refs[18:20], refs[20:27], refs[27], refs[28:]
    step, steps = pl.program_id(0), pl.num_programs(0)
    scatter = Scatter(2, MIXER_CHUNKS, *pair, own, *rest[7:])

    @pl.when(step == 0)
    def _():
        greet_near(scatter.me, scatter.outer, scatter.side)
        scatter.begin()

    def between(part):
        scatter.steps(*spread(scatter.last, 2 * step + part, 2 * (length // CH)))

    between(0)
    bwd_body(heads, dk, dv, *ins, *outs, *rest[:7], between)

    @pl.when(step == steps - 1)
    def _():
        scatter.finish()


def mixer_forward(raw, ab, tq, tk, tv, par, gain, w=None, ident=None):
    length, wide_k, wide_v = raw.shape[0], tq.shape[1], tv.shape[1]
    dv = gain.shape[1]
    heads = wide_v // dv
    dk = wide_k // heads
    steps = length // CH
    sp = mixer_specs(heads, dk, dv, lambda c: c)
    any_ref = [pl.BlockSpec(memory_space=pl.ANY)]
    fused = w is not None
    return pl.pallas_call(
        functools.partial(*([fwd_gather_body, length] if fused else [fwd_body]), heads, dk, dv),
        grid=(steps,),
        in_specs=[sp[n] for n in ("q", "k", "val", "og", "ab", "tk", "tk", "tv", "par", "gain")] + any_ref * fused,
        out_specs=[sp[n] for n in ("v", "v", "v", "t", "s")] + any_ref * fused,
        out_shape=[
            jax.ShapeDtypeStruct((length, wide_v), BF),
            jax.ShapeDtypeStruct((length, wide_v), F32),
            jax.ShapeDtypeStruct((length, wide_v), BF),
            jax.ShapeDtypeStruct((length, heads * CH), BF),
            jax.ShapeDtypeStruct((steps, dk, wide_v), BF),
        ]
        + [jax.ShapeDtypeStruct((8 * w.shape[0], w.shape[1]), w.dtype) for _ in any_ref * fused],
        scratch_shapes=[
            pltpu.VMEM((CH + HALO, wide_k), F32),
            pltpu.VMEM((CH + HALO, wide_k), F32),
            pltpu.VMEM((CH + HALO, wide_v), F32),
            pltpu.VMEM((heads, dk, dv), F32),
        ]
        + gather_sems() * fused,
        compiler_params=pltpu.CompilerParams(
            dimension_semantics=("arbitrary",), vmem_limit_bytes=60 << 20, collective_id=ident,
            has_side_effects=fused,
        ),
        cost_estimate=pl.CostEstimate(flops=20_000_000_000, bytes_accessed=40_000_000, transcendentals=6_000_000),
        name="mixer_forward",
    )(raw, raw, raw, raw, ab, tq, tk, tv, par, gain, *([w] * fused))


def mixer_backward(raw, ab, tq, tk, tv, par, gain, grad, o, u, t, s, left=None, right=None, ident=None):
    length, wide_k, wide_v = raw.shape[0], tq.shape[1], tv.shape[1]
    dv = gain.shape[1]
    heads = wide_v // dv
    dk = wide_k // heads
    steps = length // CH
    at = lambda c: steps - 1 - c
    sp = mixer_specs(heads, dk, dv, at)
    before = lambda c: jnp.maximum(at(c) * (CH // HALO) - 1, 0)
    hq = pl.BlockSpec((HALO, wide_k), lambda c: (before(c), 0))
    hk = pl.BlockSpec((HALO, wide_k), lambda c: (before(c), 1))
    hv = pl.BlockSpec((HALO, wide_v), lambda c: (before(c), 2 * wide_k // wide_v))
    names = ("q", "k", "val", "og", "ab")
    rest = ("tk", "tk", "tv", "par", "gain", "v", "v", "v", "t", "s")
    fused = left is not None
    pair, own, extra = [], [], []
    if fused:
        whole = lambda x: pl.BlockSpec(x.shape, lambda c: (0, 0), pipeline_mode=pl.Buffered(1))
        mine = (left.shape[1] // 8, right.shape[1])
        pair = [whole(left), whole(right)]
        own = [pl.BlockSpec(mine, lambda c: (0, 0))]
        extra = scatter_scratch(*mine, MIXER_CHUNKS)
    return pl.pallas_call(
        functools.partial(*([bwd_scatter_body, length] if fused else [bwd_body]), heads, dk, dv),
        grid=(steps,),
        in_specs=[sp[n] for n in names] + [hq, hk, hv] + [sp[n] for n in rest] + pair,
        out_specs=[sp[n] for n in ("raw", "ab", "tk", "tk", "tv", "par", "gain")] + own,
        out_shape=[
            jax.ShapeDtypeStruct((length, 2 * (wide_k + wide_v)), BF),
            jax.ShapeDtypeStruct((length, LANES), BF),
            jax.ShapeDtypeStruct((8, wide_k), F32),
            jax.ShapeDtypeStruct((8, wide_k), F32),
            jax.ShapeDtypeStruct((8, wide_v), F32),
            jax.ShapeDtypeStruct((8, LANES), F32),
            jax.ShapeDtypeStruct((1, dv), F32),
        ]
        + [jax.ShapeDtypeStruct(spec.block_shape, F32) for spec in own],
        scratch_shapes=[
            pltpu.VMEM((CH + HALO, wide_k), F32),
            pltpu.VMEM((CH + HALO, wide_k), F32),
            pltpu.VMEM((CH + HALO, wide_v), F32),
            pltpu.VMEM((CH + HALO, wide_k), F32),
            pltpu.VMEM((CH + HALO, wide_k), F32),
            pltpu.VMEM((CH + HALO, wide_v), F32),
            pltpu.VMEM((heads, dk, dv), F32),
        ]
        + extra,
        compiler_params=pltpu.CompilerParams(
            dimension_semantics=("arbitrary",), vmem_limit_bytes=60 << 20, collective_id=ident,
            has_side_effects=fused,
        ),
        cost_estimate=pl.CostEstimate(flops=40_000_000_000, bytes_accessed=60_000_000, transcendentals=9_000_000),
        name="mixer_backward",
    )(
        raw, raw, raw, raw, ab, raw, raw, raw, tq, tk, tv, par, gain, grad, o, u, t, s,
        *([left, right] if fused else []),
    )


def on_dp(index):
    return {"dp": index}


def greet_all(me):
    barrier = pltpu.get_barrier_semaphore()
    for j in range(1, 8):
        pl.semaphore_signal(barrier, inc=1, device_id=on_dp((me + j) % 8))
    pl.semaphore_wait(barrier, 7)


def greet_near(me, outer, side):
    barrier = pltpu.get_barrier_semaphore()
    pl.semaphore_signal(barrier, inc=1, device_id=on_dp(me + 1 - 2 * side))

    @pl.when(outer < 3)
    def _():
        pl.semaphore_signal(barrier, inc=1, device_id=on_dp((me + 2) % 8))

    @pl.when(outer > 0)
    def _():
        pl.semaphore_signal(barrier, inc=1, device_id=on_dp((me + 6) % 8))

    pl.semaphore_wait(barrier, 1 + (outer + 2) // 3 + (5 - outer) // 3)


CHUNKS = 8
LAG = 2
LAST_CHUNKS = 8


def spread(total, slot, slots):
    return total * slot // slots, total * (slot + 1) // slots


GATHER_CHUNKS = 8
CROSS_FIRST = 1
GATHER_LAG = 3


def gather_sems():
    return [
        pltpu.SemaphoreType.DMA((6, GATHER_CHUNKS)),
        pltpu.SemaphoreType.DMA((6, GATHER_CHUNKS)),
        pltpu.SemaphoreType.DMA((4, GATHER_CHUNKS)),
        pltpu.SemaphoreType.DMA((8, GATHER_CHUNKS)),
        pltpu.SemaphoreType.DMA,
    ]


class Gather:
    STEPS = GATHER_CHUNKS + 4 * GATHER_LAG

    def __init__(self, w_ref, full_ref, right_s, left_s, swap_s, arrive, local):
        self.w, self.full, self.sems, self.arrive = w_ref, full_ref, (right_s, left_s, swap_s), arrive
        self.me = lax.axis_index("dp")
        self.outer, self.side = self.me // 2, self.me % 2
        self.block = w_ref.shape[0]
        self.part = self.block // GATHER_CHUNKS
        self.keep = pltpu.make_async_copy(w_ref, full_ref.at[pl.ds(0, self.block)], local)

    def spot(self, slot, c):
        return self.full.at[pl.ds(slot * self.block + c * self.part, self.part)]

    def source(self, slot, c):
        return self.w.at[pl.ds(c * self.part, self.part)] if slot == 0 else self.spot(slot, c)

    def copy(self, slot, to, c, sem, index, peer):
        return pltpu.make_async_remote_copy(
            self.source(slot, c), self.spot(to, c), sem.at[index, c], self.arrive.at[to, c], device_id=on_dp(peer)
        )

    def along(self, way, far, h, c):
        slot, to = ((4 - h) % 4, 3 - h) if way == 0 else (h, h + 1)
        peer = (self.me + (2, 6)[way]) % 8
        return self.copy(slot + 4 * far, to + 4 * far, c, self.sems[way], h + 3 * far, peer)

    def to_side(self, slot, c):
        return self.copy(slot, 4 + slot, c, self.sems[2], slot, self.me + 1 - 2 * self.side)

    def landed(self, slot, c):
        pltpu.make_async_copy(self.spot(slot, c), self.spot(slot, c), self.arrive.at[slot, c]).wait()

    def begin(self):
        self.keep.start()

    def go_on(self, way, far, h, c):
        if h < 3:
            @pl.when((self.outer < 3) if way == 0 else (self.outer > 0))
            def _():
                self.along(way, far, h, c).start()

    def step(self, i):
        @pl.when(i < GATHER_CHUNKS)
        def _():
            self.to_side(0, i).start()
            for way in range(2):
                self.go_on(way, 0, 0, i)

        far_at = i - GATHER_LAG

        @pl.when((far_at >= 0) & (far_at < CROSS_FIRST))
        def _():
            self.landed(4, far_at)
            for way in range(2):
                self.go_on(way, 1, 0, far_at)

        for far in range(2):
            last = CROSS_FIRST if far else GATHER_CHUNKS
            for h in range(1, 4):
                c = i - GATHER_LAG * (h + far)
                for way in range(2):
                    behind = self.outer if way == 0 else 3 - self.outer
                    slot = 4 - h if way == 0 else h

                    @pl.when((c >= 0) & (c < last) & (behind >= h))
                    def _():
                        self.landed(slot + 4 * far, c)
                        self.go_on(way, far, h, c)
                        if not far:
                            @pl.when(c >= CROSS_FIRST)
                            def _():
                                self.to_side(slot, c).start()

    def finish(self):
        def one(c, carry):
            self.to_side(0, c).wait_send()

            @pl.when(c >= CROSS_FIRST)
            def _():
                self.landed(4, c)
                for slot in range(1, 4):
                    self.to_side(slot, c).wait_send()
                    self.landed(4 + slot, c)

            for way in range(2):
                behind = self.outer if way == 0 else 3 - self.outer
                for h in range(3):
                    for far in range(2):
                        @pl.when((behind >= h) & (c < (CROSS_FIRST if far else GATHER_CHUNKS)))
                        def _():
                            @pl.when((self.outer < 3) if way == 0 else (self.outer > 0))
                            def _():
                                self.along(way, far, h, c).wait_send()

            return carry

        lax.fori_loop(0, GATHER_CHUNKS, one, 0)
        self.keep.wait()

    def steps(self, first, last):
        def one(i, carry):
            self.step(i)
            return carry

        lax.fori_loop(first, last, one, 0)


def gather_small_body(w_ref, small_ref, full_ref, all_ref, *sems):
    gather = Gather(w_ref, full_ref, *sems[:5])
    few_s, few_r, local = sems[5:]
    me, outer, side = gather.me, gather.outer, gather.side
    greet_all(me)
    gather.begin()
    keep = pltpu.make_async_copy(small_ref, all_ref.at[0], local)
    keep.start()

    def few(j):
        peer = (me + j) % 8
        slot = (outer - peer // 2 + 4) % 4 + 4 * ((side + peer % 2) % 2)
        return pltpu.make_async_remote_copy(
            small_ref, all_ref.at[slot], few_s.at[j - 1], few_r.at[j - 1], device_id=on_dp(peer)
        )

    for j in range(1, 8):
        few(j).start()
    gather.steps(0, gather.STEPS)
    gather.finish()
    for j in range(1, 8):
        few(j).wait()
    keep.wait()


def gather_body(w_ref, full_ref, *sems):
    gather = Gather(w_ref, full_ref, *sems)
    greet_near(gather.me, gather.outer, gather.side)
    gather.begin()
    gather.steps(0, gather.STEPS)
    gather.finish()


def ring_gather(w, ident, small=None):
    any_ref = pl.BlockSpec(memory_space=pl.ANY)
    full = jax.ShapeDtypeStruct((8 * w.shape[0], w.shape[1]), w.dtype)
    params = pltpu.CompilerParams(collective_id=ident, has_side_effects=True)
    cost = pl.CostEstimate(flops=0, bytes_accessed=150 * w.size, transcendentals=0)
    if small is None:
        return pl.pallas_call(
            gather_body, in_specs=[any_ref], out_specs=any_ref, out_shape=full, scratch_shapes=gather_sems(),
            compiler_params=params, cost_estimate=cost, name=f"ring_gather_{ident}",
        )(w)
    return pl.pallas_call(
        gather_small_body,
        in_specs=[any_ref] * 2,
        out_specs=[any_ref] * 2,
        out_shape=[full, jax.ShapeDtypeStruct((8,) + small.shape, small.dtype)],
        scratch_shapes=gather_sems()
        + [pltpu.SemaphoreType.DMA((7,)), pltpu.SemaphoreType.DMA((7,)), pltpu.SemaphoreType.DMA],
        compiler_params=params, cost_estimate=cost, name=f"ring_gather_{ident}",
    )(w, small)


def scatter_sems(chunks):
    return [pltpu.SemaphoreType.DMA((4, chunks)) for _ in range(6)]


class Scatter:
    def __init__(self, lag, chunks, left, right, out, mine, came, from_left, from_right, *sems):
        self.lag, self.chunks = lag, chunks
        self.last = 4 * chunks + 3 * lag
        self.left, self.right, self.mine, self.came = left, right, mine, came
        self.outs = out if isinstance(out, tuple) else (out,)
        self.acc = (from_left, from_right)
        self.swap_s, self.swap_r, self.send_l, self.recv_l, self.send_r, self.recv_r = sems
        self.me = lax.axis_index("dp")
        self.outer, self.side = self.me // 2, self.me % 2
        self.block, self.cols = self.outs[0].shape[0], right.shape[1]
        self.part = self.block // chunks

    def dot(self, slot):
        tile = self.cols if self.cols <= 1536 else 1024
        at = pl.multiple_of(slot * self.block, self.block)
        rows = self.left[:, pl.ds(at, self.block)]
        for j in range(0, self.cols, tile):
            self.mine[pl.ds(at, self.block), j : j + tile] = mm(rows, self.right[:, j : j + tile], TN).astype(BF)

    def item(self, t):
        dest = (3 * (t // self.chunks) + 1) % 4
        return dest, (dest - self.outer + 4) % 4, t % self.chunks

    def rows(self, slot, c):
        return pl.ds(pl.multiple_of(slot * self.block + c * self.part, self.part), self.part)

    def swap(self, slot, c):
        return pltpu.make_async_remote_copy(
            self.mine.at[self.rows(4 + slot, c)], self.came.at[self.rows(slot, c)],
            self.swap_s.at[slot, c], self.swap_r.at[slot, c], device_id=on_dp(self.me + 1 - 2 * self.side),
        )

    def onward(self, way, dest, c):
        ref, rows = self.acc[way], self.rows(dest - 1 + way, c)
        send, recv = ((self.send_l, self.recv_l), (self.send_r, self.recv_r))[way]
        peer = (self.me + (2, 6)[way]) % 8
        return pltpu.make_async_remote_copy(
            ref.at[rows], ref.at[rows], send.at[dest, c], recv.at[dest, c], device_id=on_dp(peer)
        )

    def arrived(self, way, dest, c):
        ref, rows = self.acc[way], self.rows(dest - 1 + way, c)
        recv = (self.recv_l, self.recv_r)[way]
        pltpu.make_async_copy(ref.at[rows], ref.at[rows], recv.at[dest, c]).wait()

    def pair(self, slot, c):
        return self.mine[self.rows(slot, c), :].astype(F32) + self.came[self.rows(slot, c), :].astype(F32)

    def begin(self):
        def send(j, carry):
            _, slot, _ = self.item(j * self.chunks)
            self.dot(4 + slot)

            def one(c, carry):
                self.swap(slot, c).start()
                return carry

            return lax.fori_loop(0, self.chunks, one, carry)

        lax.fori_loop(0, 4, send, 0)

    def step(self, t):
        outer = self.outer
        items = 4 * self.chunks

        @pl.when(t < items)
        def _():
            _, slot, c = self.item(t)

            @pl.when(c == 0)
            def _():
                self.dot(slot)

            self.swap(slot, c).wait_recv()

        for way in range(2):
            behind = outer if way == 0 else 3 - outer
            at = t - behind * self.lag
            dest, slot, c = self.item((at + 2 * items) % items)
            ahead = (outer < dest) if way == 0 else (outer > dest)

            @pl.when((at >= 0) & (at < items) & ahead)
            def _():
                total = self.pair(slot, c)
                ref, rows = self.acc[way], self.rows(dest - 1 + way, c)

                @pl.when(behind == 0)
                def _():
                    ref[rows, :] = total.astype(BF)

                @pl.when(behind > 0)
                def _():
                    self.arrived(way, dest, c)
                    ref[rows, :] = (total + ref[rows, :].astype(F32)).astype(BF)

                self.onward(way, dest, c).start()

        at = t - 3 * self.lag
        dest, _, c = self.item((at + 2 * items) % items)

        @pl.when((at >= 0) & (dest == outer))
        def _():
            rows = pl.ds(pl.multiple_of(c * self.part, self.part), self.part)
            total = self.pair(0, c)
            spans, start = [], 0
            for out in self.outs:
                spans.append((out, slice(start, start + out.shape[1])))
                start += out.shape[1]
            for out, cols in spans:
                out[rows, :] = total[:, cols]
            for way in range(2):
                @pl.when((outer if way == 0 else 3 - outer) > 0)
                def _():
                    self.arrived(way, outer, c)
                    for out, cols in spans:
                        out[rows, :] += self.acc[way][self.rows(outer - 1 + way, c), cols].astype(F32)

    def steps(self, first, last):
        def one(i, carry):
            self.step(i)
            return carry

        lax.fori_loop(first, last, one, 0)

    def finish(self):
        outer = self.outer

        def one(c, carry):
            for slot in range(4):
                self.swap(slot, c).wait_send()
            for way in range(2):
                for dest in range(4):
                    ahead = (outer < dest) if way == 0 else (outer > dest)

                    @pl.when(ahead)
                    def _():
                        self.onward(way, dest, c).wait_send()

            return carry

        lax.fori_loop(0, self.chunks, one, 0)


def scatter_scratch(block, cols, chunks):
    return [
        pltpu.VMEM((8 * block, cols), BF),
        pltpu.VMEM((4 * block, cols), BF),
        pltpu.VMEM((3 * block, cols), BF),
        pltpu.VMEM((3 * block, cols), BF),
    ] + scatter_sems(chunks)


def scatter_body(left_ref, right_ref, out_ref, *scratch):
    scatter = Scatter(LAG, CHUNKS, left_ref, right_ref, out_ref, *scratch)
    greet_near(scatter.me, scatter.outer, scatter.side)
    scatter.begin()
    scatter.steps(0, scatter.last)
    scatter.finish()


def scatter_last_body(
    t_size, left_ref, right_ref, ab_ref, few_ref, tap_ref, rest_ref, z_ref, mid_ref, gain_ref, fab_ref, full_ref,
    out_q, out_k, out_v, out_g, few_out, tap_out, vec_out, grad_ref, *scratch,
):
    w_buf, sum_out, sum_in, few_in, tap_in, vec, vec_t, vec_d, parts = scratch[:9]
    w_sem, s_sem, few_sem, tap_sem, t_sem, d_sem = scratch[9:15]
    scatter = Scatter(LAG, LAST_CHUNKS, left_ref, right_ref, (out_q, out_k, out_v, out_g), *scratch[15:])
    me, outer, side, block = scatter.me, scatter.outer, scatter.side, scatter.block
    mine = lax.axis_index("tensor")
    tokens = z_ref.shape[0]
    barrier = pltpu.get_barrier_semaphore()
    for j in range(1, t_size):
        pl.semaphore_signal(barrier, inc=1, device_id={"tensor": (mine + j) % t_size})
    for j in range(1, 8):
        pl.semaphore_signal(barrier, inc=1, device_id=on_dp((me + j) % 8))
    pl.semaphore_wait(barrier, 6 + t_size)

    def few(j):
        peer = (me + j) % 8
        slot = (peer // 2 - outer + 4) % 4 + 4 * ((side + peer % 2) % 2)
        return pltpu.make_async_remote_copy(
            few_ref.at[slot], few_in.at[j], few_sem.at[0, j], few_sem.at[1, j], device_id=on_dp(peer)
        )

    def tap(j):
        peer = (me + j) % 8
        return pltpu.make_async_remote_copy(
            tap_ref.at[peer], tap_in.at[j], tap_sem.at[0, j], tap_sem.at[1, j], device_id=on_dp(peer)
        )

    def across(j):
        return pltpu.make_async_remote_copy(
            vec, vec_t.at[mine], t_sem.at[0, j], t_sem.at[1, j], device_id={"tensor": (mine + j) % t_size}
        )

    def along(j):
        return pltpu.make_async_remote_copy(
            vec_d.at[me], vec_d.at[me], d_sem.at[0, j], d_sem.at[1, j], device_id=on_dp((me + j) % 8)
        )

    def load(n):
        return pltpu.make_async_copy(full_ref.at[pl.ds(n * block, block)], w_buf.at[n % 2], w_sem.at[n % 2])

    def share(j, n):
        return pltpu.make_async_remote_copy(
            sum_out.at[j, n], sum_in.at[j - 1, n], s_sem.at[0, j, n], s_sem.at[1, j, n],
            device_id={"tensor": (mine + j) % t_size},
        )

    load(0).start()
    scatter.begin()
    for j in range(1, 8):
        few(j).start()
        tap(j).start()

    def tile(n, carry):
        scatter.step(n)

        @pl.when(n < 7)
        def _():
            load(n + 1).start()

        load(n).wait()
        w = w_buf[n % 2]
        w_few = fab_ref[pl.ds(pl.multiple_of(n * block, block), block), :]
        for j in range(t_size):
            rows = pl.ds(pl.multiple_of(((mine + j) % t_size) * tokens, tokens), tokens)
            sum_out[j, n] = (mm(right_ref[rows, :], w, NT) + mm(ab_ref[rows, :], w_few, NT)).astype(BF)
            if j:
                share(j, n).start()
        return carry

    lax.fori_loop(0, 8, tile, 0)
    late = 3 * LAST_CHUNKS
    scatter.steps(8, late)

    def land(n, carry):
        for j in range(1, t_size):
            share(j, n).wait_recv()
        return carry

    lax.fori_loop(0, 8, land, 0)
    size = 32

    def norm(i):
        at = pl.ds(pl.multiple_of(i * size, size), size)
        squares, inner = 0.0, 0.0
        for n in range(8):
            cols = slice(n * block, (n + 1) * block)
            z = z_ref[at, cols]
            m = sum_out[0, n, at, :].astype(F32)
            for j in range(1, t_size):
                m = m + sum_in[j - 1, n, at, :].astype(F32)
            squares = squares + jnp.sum(z * z, axis=-1, keepdims=True)
            inner = inner + jnp.sum(m * gain_ref[:, cols] * z, axis=-1, keepdims=True)
        width = 8 * block
        r = lax.rsqrt(squares / width + 1e-05)
        pull = r * r * r * (inner / width)
        for n in range(8):
            cols = slice(n * block, (n + 1) * block)
            z = z_ref[at, cols]
            m = sum_out[0, n, at, :].astype(F32)
            for j in range(1, t_size):
                m = m + sum_in[j - 1, n, at, :].astype(F32)
            home = 2 * ((outer + n) % 4) + (side + n // 4) % 2
            to = pl.ds(pl.multiple_of(home * block, block), block)
            grad_ref[at, to] = mid_ref[at, cols] + r * (m * gain_ref[:, cols]) - z * pull
            parts[n : n + 1, :] += jnp.sum(m * (z * r), axis=0, keepdims=True)

    parts[...] = jnp.zeros_like(parts)
    rounds = tokens // size // 4

    def norms(i, carry):
        scatter.step(late + i)
        for k in range(rounds):
            norm(i * rounds + k)
        return carry

    lax.fori_loop(0, 4, norms, 0)
    per = block // LANES
    for n in range(8):
        home = 2 * ((outer + n) % 4) + (side + n // 4) % 2
        for k in range(per):
            vec[pl.ds(home * per + k, 1), :] = parts[n : n + 1, k * LANES : (k + 1) * LANES]
    vec[8 * per :, :] = rest_ref[...]
    for j in range(1, t_size):
        across(j).start()
    vec_t[mine] = vec[...]
    scatter.steps(late + 4, late + 6)
    for j in range(1, t_size):
        pltpu.make_async_copy(vec, vec_t.at[(mine + t_size - j) % t_size], t_sem.at[1, j]).wait()
    total = vec_t[0]
    for j in range(1, t_size):
        total = total + vec_t[j]
    vec_d[me] = total
    for j in range(1, 8):
        along(j).start()
    scatter.steps(late + 6, scatter.last)
    few_total, tap_total = few_ref[0], tap_ref[me]
    for j in range(1, 8):
        few(j).wait_recv()
        few_total = few_total + few_in[j]
        tap(j).wait_recv()
        tap_total = tap_total + tap_in[j]
    few_out[...] = few_total
    tap_out[...] = tap_total
    for j in range(1, 8):
        pltpu.make_async_copy(vec_d.at[me], vec_d.at[(me + 8 - j) % 8], d_sem.at[1, j]).wait()
    total = vec_d[0]
    for j in range(1, 8):
        total = total + vec_d[j]
    vec_out[...] = total
    for j in range(1, t_size):
        across(j).wait_send()
    for j in range(1, 8):
        few(j).wait_send()
        tap(j).wait_send()
        along(j).wait_send()

    def sent(n, carry):
        for j in range(1, t_size):
            share(j, n).wait_send()
        return carry

    lax.fori_loop(0, 8, sent, 0)
    scatter.finish()


def ring_scatter_last(left, right, ab, few, taps, rest, z, mid, gain, full_ab, full, widths, t_size, ident):
    width, cols, tokens = left.shape[1], right.shape[1], z.shape[0]
    block = width // 8
    vec = (width // LANES + rest.shape[0], LANES)
    vmem = pl.BlockSpec(memory_space=pltpu.VMEM)
    pair = pltpu.SemaphoreType.DMA((2, 8))
    return pl.pallas_call(
        functools.partial(scatter_last_body, t_size),
        in_specs=[vmem] * 10 + [pl.BlockSpec(memory_space=pl.ANY)],
        out_specs=[vmem] * 8,
        out_shape=[jax.ShapeDtypeStruct((block, w), F32) for w in widths]
        + [
            jax.ShapeDtypeStruct(few.shape[1:], F32),
            jax.ShapeDtypeStruct(taps.shape[1:], F32),
            jax.ShapeDtypeStruct(vec, F32),
            jax.ShapeDtypeStruct(z.shape, F32),
        ],
        scratch_shapes=[
            pltpu.VMEM((2, block, cols), BF),
            pltpu.VMEM((t_size, 8, tokens, block), BF),
            pltpu.VMEM((t_size - 1, 8, tokens, block), BF),
            pltpu.VMEM(few.shape, F32),
            pltpu.VMEM(taps.shape, F32),
            pltpu.VMEM(vec, F32),
            pltpu.VMEM((t_size,) + vec, F32),
            pltpu.VMEM((8,) + vec, F32),
            pltpu.VMEM((8, block), F32),
            pltpu.SemaphoreType.DMA((2,)),
            pltpu.SemaphoreType.DMA((2, t_size, 8)),
            pair,
            pair,
            pltpu.SemaphoreType.DMA((2, t_size)),
            pair,
        ]
        + scatter_scratch(block, cols, LAST_CHUNKS),
        compiler_params=pltpu.CompilerParams(
            collective_id=ident, has_side_effects=True, vmem_limit_bytes=63 << 20
        ),
        cost_estimate=pl.CostEstimate(flops=0, bytes_accessed=1200 * block * cols, transcendentals=0),
        name=f"ring_scatter_{ident}",
    )(left, right, ab, few, taps, rest, z, mid, gain, full_ab, full)


def ring_scatter(left, right, ident):
    block, cols = left.shape[1] // 8, right.shape[1]
    vmem = pl.BlockSpec(memory_space=pltpu.VMEM)
    return pl.pallas_call(
        scatter_body,
        in_specs=[vmem] * 2,
        out_specs=vmem,
        out_shape=jax.ShapeDtypeStruct((block, cols), F32),
        scratch_shapes=scatter_scratch(block, cols, CHUNKS),
        compiler_params=pltpu.CompilerParams(
            collective_id=ident, has_side_effects=True, vmem_limit_bytes=60 << 20
        ),
        cost_estimate=pl.CostEstimate(flops=0, bytes_accessed=1200 * block * cols, transcendentals=0),
        name=f"ring_scatter_{ident}",
    )(left, right)


FFN_ROWS = 256


def col_tiles(n, want):
    return [(at, min(want, n - at)) for at in range(0, n, want)]


def ffn_forward_body(slots, x_ref, gate_ref, up_ref, w_ref, act_ref, slope_ref, hid_ref, full_ref, *sems):
    step, steps = pl.program_id(0), pl.num_programs(0)
    gather = Gather(w_ref, full_ref, *sems)

    @pl.when(step == 0)
    def _():
        greet_near(gather.me, gather.outer, gather.side)
        gather.begin()

    x = x_ref[...]
    for part, (at, wide) in enumerate(col_tiles(gate_ref.shape[1], 512)):
        gather.steps(*spread(gather.STEPS, 3 * step + part, 3 * slots))
        gate = mm(x, gate_ref[:, at : at + wide])
        up = mm(x, up_ref[:, at : at + wide])
        sg = sigmoid(gate)
        act = gate * sg
        act_ref[:, at : at + wide] = act.astype(BF)
        slope_ref[:, at : at + wide] = (up * (sg * (1.0 + gate * (1.0 - sg)))).astype(BF)
        hid_ref[:, at : at + wide] = (act * up).astype(BF)

    @pl.when(step == steps - 1)
    def _():
        gather.finish()


def ffn_forward(x, full_gate, full_up, w, ident):
    length, ff = x.shape[0], full_gate.shape[1]
    any_ref = pl.BlockSpec(memory_space=pl.ANY)
    once = pl.BlockSpec(full_gate.shape, lambda c: (0, 0), pipeline_mode=pl.Buffered(1))
    tile = pl.BlockSpec((FFN_ROWS, ff), lambda c: (c, 0))
    return pl.pallas_call(
        functools.partial(ffn_forward_body, length // FFN_ROWS),
        grid=(length // FFN_ROWS,),
        in_specs=[pl.BlockSpec((FFN_ROWS, x.shape[1]), lambda c: (c, 0)), once, once, any_ref],
        out_specs=[tile] * 3 + [any_ref],
        out_shape=[jax.ShapeDtypeStruct((length, ff), BF)] * 3
        + [jax.ShapeDtypeStruct((8 * w.shape[0], w.shape[1]), w.dtype)],
        scratch_shapes=gather_sems(),
        compiler_params=pltpu.CompilerParams(
            dimension_semantics=("arbitrary",), vmem_limit_bytes=60 << 20, collective_id=ident, has_side_effects=True
        ),
        cost_estimate=pl.CostEstimate(flops=70_000_000_000, bytes_accessed=30_000_000, transcendentals=1_500_000),
        name="ffn_forward",
    )(x, full_gate, full_up, w)


def ffn_backward_body(
    left_ref, hid_ref, act_ref, slope_ref, down_hbm, gate_hbm, up_hbm,
    glow_ref, ulow_ref, back_ref, ffn_ref, out_ref, down_ref, gate_ref, up_ref, load_sem, *scratch,
):
    step, steps = pl.program_id(0), pl.num_programs(0)
    scatter = Scatter(3, CHUNKS, left_ref, hid_ref, out_ref, *scratch)
    loads = [
        pltpu.make_async_copy(src, dst, load_sem.at[i])
        for i, (src, dst) in enumerate(((down_hbm, down_ref), (gate_hbm, gate_ref), (up_hbm, up_ref)))
    ]

    @pl.when(step == 0)
    def _():
        greet_near(scatter.me, scatter.outer, scatter.side)
        for copy in loads:
            copy.start()
        scatter.begin()
        loads[0].wait()

    rows = pl.ds(pl.multiple_of(step * FFN_ROWS, FFN_ROWS), FFN_ROWS)
    x = left_ref[rows, :]
    for at, wide in col_tiles(down_ref.shape[1], 512):
        cols = slice(at, at + wide)
        grad = mm(x, down_ref[:, cols])
        glow_ref[:, cols] = (grad * slope_ref[:, cols].astype(F32)).astype(BF)
        ulow_ref[:, cols] = (grad * act_ref[:, cols].astype(F32)).astype(BF)

    @pl.when(step == 0)
    def _():
        loads[1].wait()
        loads[2].wait()

    hid = hid_ref[rows, :]
    glow, ulow = glow_ref[...], ulow_ref[...]
    for part, (at, wide) in enumerate(col_tiles(down_ref.shape[0], 512)):
        scatter.steps(*spread(scatter.last, 4 * step + part, 4 * (left_ref.shape[0] // FFN_ROWS)))
        cols = slice(at, at + wide)
        back_ref[:, cols] = (mm(glow, gate_ref[cols, :], NT) + mm(ulow, up_ref[cols, :], NT)).astype(BF)
        ffn_ref[:, cols] = mm(hid, down_ref[cols, :], NT).astype(BF)

    @pl.when(step == steps - 1)
    def _():
        scatter.finish()


def ffn_backward(left, hidden, act, slope, full_down, full_gate, full_up, ident):
    (length, width), ff = left.shape, hidden.shape[1]
    once = lambda x: pl.BlockSpec(x.shape, lambda c: (0, 0), pipeline_mode=pl.Buffered(1))
    tile = pl.BlockSpec((FFN_ROWS, ff), lambda c: (c, 0))
    wide = pl.BlockSpec((FFN_ROWS, width), lambda c: (c, 0))
    mine = (width // 8, ff)
    return pl.pallas_call(
        ffn_backward_body,
        grid=(length // FFN_ROWS,),
        in_specs=[once(left), once(hidden), tile, tile] + [pl.BlockSpec(memory_space=pl.ANY)] * 3,
        out_specs=[tile, tile, wide, wide, pl.BlockSpec(mine, lambda c: (0, 0))],
        out_shape=[jax.ShapeDtypeStruct((length, ff), BF)] * 2
        + [jax.ShapeDtypeStruct((length, width), BF)] * 2
        + [jax.ShapeDtypeStruct(mine, F32)],
        scratch_shapes=[pltpu.VMEM(full_down.shape, BF)] * 3
        + [pltpu.SemaphoreType.DMA((3,))]
        + scatter_scratch(*mine, CHUNKS),
        compiler_params=pltpu.CompilerParams(
            dimension_semantics=("arbitrary",), vmem_limit_bytes=62 << 20, collective_id=ident, has_side_effects=True
        ),
        cost_estimate=pl.CostEstimate(flops=90_000_000_000, bytes_accessed=50_000_000, transcendentals=0),
        name="ffn_backward",
    )(left, hidden, act, slope, full_down, full_gate, full_up)


def plain_dot(left_mat, right_mat):
    return jnp.dot(left_mat, right_mat, preferred_element_type=F32)


def dot_rows(left_mat, right_mat):
    return lax.dot_general(left_mat, right_mat, (((1,), (1,)), ((), ())), preferred_element_type=F32)


def dot_tokens(left_mat, right_mat):
    return lax.dot_general(left_mat, right_mat, (((0,), (0,)), ((), ())), preferred_element_type=F32)


def rms_apply(values, gain_vec):
    return values * lax.rsqrt(jnp.mean(values * values, axis=-1, keepdims=True) + 1e-05) * gain_vec


class RingRows:
    def __init__(self, dp_size):
        self.outer = dp_size // 2
        self.index = lax.axis_index("dp")

    def _roll(self, x, axis, blocks):
        size = x.shape[axis] // self.outer * blocks
        return jnp.concatenate(
            [lax.slice_in_dim(x, size, None, axis=axis), lax.slice_in_dim(x, 0, size, axis=axis)], axis
        )

    def reorder(self, x, axis):
        outer_at, pair_at = self.index // 2, self.index % 2
        size = x.shape[axis] // (2 * self.outer)
        cut = [lax.slice_in_dim(x, b * size, (b + 1) * size, axis=axis) for b in range(2 * self.outer)]
        even, odd = jnp.concatenate(cut[0::2], axis), jnp.concatenate(cut[1::2], axis)
        sides = [jnp.where(pair_at == 0, even, odd), jnp.where(pair_at == 0, odd, even)]
        bit = 1
        while bit < self.outer:
            sides = [jnp.where((outer_at // bit) % 2 == 1, self._roll(s, axis, bit), s) for s in sides]
            bit *= 2
        return jnp.concatenate(sides, axis)

    def restore(self, x, axis):
        outer_at, pair_at = self.index // 2, self.index % 2
        half = x.shape[axis] // 2
        sides = [lax.slice_in_dim(x, 0, half, axis=axis), lax.slice_in_dim(x, half, None, axis=axis)]
        bit = 1
        while bit < self.outer:
            sides = [
                jnp.where((outer_at // bit) % 2 == 1, self._roll(s, axis, self.outer - bit), s) for s in sides
            ]
            bit *= 2
        even = jnp.where(pair_at == 0, sides[0], sides[1])
        odd = jnp.where(pair_at == 0, sides[1], sides[0])
        size = half // self.outer
        cut = []
        for b in range(self.outer):
            cut += [lax.slice_in_dim(s, b * size, (b + 1) * size, axis=axis) for s in (even, odd)]
        return jnp.concatenate(cut, axis)

    def _swap(self, x):
        return lax.ppermute(x, "dp", [(i, i ^ 1) for i in range(2 * self.outer)])

    def gather_first(self, w, small):
        return ring_gather(w, 0, small)

    def gather(self, w, ident):
        return ring_gather(w, ident)

    def scatter(self, left, right, ident):
        return ring_scatter(left, right, ident)

    def ffn_forward(self, x, gate, up, w, ident):
        return ffn_forward(x, gate, up, w, ident)

    def ffn_backward(self, left, hidden, act, slope, down, gate, up, ident):
        return ffn_backward(left, hidden, act, slope, down, gate, up, ident)

    def forward(self, core_in, w, ident):
        return mixer_forward(*core_in, w, ident)

    def backward(self, core_in, saved, left, right, ident):
        return mixer_backward(*core_in, *saved, left, right, ident)

    def scatter_last(self, *args):
        return ring_scatter_last(*args)


class PlainRows:
    def reorder(self, x, axis):
        return x

    def restore(self, x, axis):
        return x

    def gather(self, w, ident):
        return lax.all_gather(w, "dp", axis=0, tiled=True)

    def scatter(self, left, right, ident):
        full = dot_tokens(left, right).astype(BF)
        return lax.psum_scatter(full, "dp", scatter_dimension=0, tiled=True).astype(F32)

    def gather_first(self, w, small):
        return lax.all_gather(w, "dp", axis=0, tiled=True), lax.all_gather(small, "dp", axis=0)

    def ffn_forward(self, x, gate, up, w, ident):
        gate_pre, up_pre = plain_dot(x, gate), plain_dot(x, up)
        sg = jax.nn.sigmoid(gate_pre)
        act = gate_pre * sg
        slope = up_pre * (sg * (1.0 + gate_pre * (1.0 - sg)))
        return act.astype(BF), slope.astype(BF), (act * up_pre).astype(BF), self.gather(w, ident)

    def ffn_backward(self, left, hidden, act, slope, down, gate, up, ident):
        grad = plain_dot(left, down)
        gate_low, up_low = (grad * slope.astype(F32)).astype(BF), (grad * act.astype(F32)).astype(BF)
        back = (dot_rows(gate_low, gate) + dot_rows(up_low, up)).astype(BF)
        return gate_low, up_low, back, dot_rows(hidden, down).astype(BF), self.scatter(left, hidden, ident)

    def forward(self, core_in, w, ident):
        return [*mixer_forward(*core_in), self.gather(w, ident)]

    def backward(self, core_in, saved, left, right, ident):
        return [*mixer_backward(*core_in, *saved), self.scatter(left, right, ident)]

    def scatter_last(self, left, right, ab, few, taps, rest, z, mid, gain, full_ab, full, widths, t_size, ident):
        summed = (dot_rows(right, full) + dot_rows(ab, full_ab)).astype(BF)
        grad, grad_gain = jax.vjp(rms_apply, z, gain[0])[1](tensor_scatter(summed).astype(F32))
        few, taps = (lax.psum_scatter(x, "dp", scatter_dimension=0, tiled=True)[0] for x in (few, taps))
        vec = lax.psum(jnp.concatenate([grad_gain.reshape(-1, LANES), rest]), ("dp", "tensor"))
        out, found, at = self.scatter(left, right, ident), [], 0
        for width in widths:
            found.append(out[:, at : at + width])
            at += width
        return *found, few, taps, vec, mid + grad


def tie(value, *others):
    return lax.optimization_barrier((value, others))[0]


def tensor_gather(x):
    return lax.all_gather(x, "tensor", axis=0, tiled=True)


def tensor_scatter(x):
    return lax.psum_scatter(x, "tensor", scatter_dimension=0, tiled=True)


def shards(
    dp_size, tensor_size, inputs, cotangent, lengths, norm1_gain, w_query, w_key, w_value, w_outgate, w_beta, w_alpha,
    conv_query, conv_key, conv_value, a_log, dt_bias, head_gain, w_out, norm2_gain, w_gate, w_up, w_down,
):
    rows = RingRows(dp_size) if dp_size == 8 else PlainRows()
    heads = w_beta.shape[1]
    wide_k, wide_v = w_query.shape[1], w_value.shape[1]
    dk, dv = wide_k // heads, wide_v // heads
    taps_n = conv_query.shape[2]
    block = w_query.shape[0]
    tensor_pos = lax.axis_index("tensor")
    head_start = tensor_pos * heads

    row_count = inputs.shape[1]
    positions = tensor_pos * row_count + jnp.arange(row_count, dtype=jnp.int32)
    valid_rows = (positions < lengths[0]).astype(F32)[:, None]

    def by_head(conv):
        return jnp.transpose(conv, (1, 2, 0)).reshape(-1)

    small = jnp.concatenate(
        [w_beta.T.reshape(-1), w_alpha.T.reshape(-1), by_head(conv_query), by_head(conv_key), by_head(conv_value)]
    )
    cuts = [0]
    for part in (w_beta, w_alpha, conv_query, conv_key, conv_value):
        cuts.append(cuts[-1] + part.size)
    small = jnp.pad(small, (0, -small.size % (32 * LANES))).reshape(-1, LANES)
    full_raw, small = rows.gather_first(
        jnp.concatenate([w_query, w_key, w_value, w_outgate], axis=1), small
    )
    small = small.reshape(dp_size, -1)
    few = small[:, : cuts[2]].reshape(dp_size, 2 * heads, block)
    full_ab = jnp.transpose(few, (1, 0, 2)).reshape(2 * heads, dp_size * block).T
    full_ab = jnp.pad(full_ab, ((0, 0), (0, LANES - 2 * heads)))
    taps_all = rows.restore(small[:, cuts[2] : cuts[5]], 0).astype(F32)

    def tap_table(at, size):
        table = taps_all[:, at - cuts[2] : at - cuts[2] + taps_n * heads * size // dp_size]
        table = jnp.transpose(table.reshape(dp_size, heads, taps_n, size // dp_size), (2, 1, 0, 3))
        return jnp.pad(table.reshape(taps_n, heads * size), ((0, 8 - taps_n), (0, 0)))

    tq, tk, tv = tap_table(cuts[2], dk), tap_table(cuts[3], dk), tap_table(cuts[4], dv)
    alog_local = lax.dynamic_slice_in_dim(a_log, head_start, heads)
    dtb_local = lax.dynamic_slice_in_dim(dt_bias, head_start, heads)
    par = jnp.pad(jnp.stack([alog_local, dtb_local]), ((0, 6), (heads, LANES - 2 * heads)))
    gain = head_gain[None]

    local_rows = rows.reorder(inputs[0], 1).astype(F32)
    gain_one = rows.reorder(norm1_gain[None], 1)[0]
    gain_two = rows.reorder(norm2_gain[None], 1)[0]
    normed_one = rms_apply(local_rows, gain_one)
    rows_one = tensor_gather(normed_one.astype(BF))
    grad_after = valid_rows * rows.reorder(cotangent[0], 1).astype(F32)
    incoming_ffn = tensor_gather(grad_after.astype(BF))

    ab_raw = plain_dot(rows_one, full_ab)
    core_in = (plain_dot(rows_one, full_raw), ab_raw, tq, tk, tv, par, gain)
    head_bf, delta_out, new_values, inverses, states, full_out = rows.forward(core_in, w_out, 1)
    mixed = dot_rows(head_bf, full_out).astype(BF)
    full_gate = rows.gather(tie(w_gate, mixed), 2)
    after_mix = local_rows + tie(tensor_scatter(mixed), full_gate).astype(F32)
    normed_two, norm_two_back = jax.vjp(rms_apply, after_mix, gain_two)
    normed_two = normed_two.astype(BF)
    full_up = rows.gather(tie(w_up, normed_two), 3)
    rows_two = tie(tensor_gather(normed_two), full_up)
    act, slope, hidden, full_down = rows.ffn_forward(rows_two, full_gate, full_up, w_down, 4)

    gate_low, up_low, back_two, ffn_out, out_down = rows.ffn_backward(
        incoming_ffn, hidden, act, slope, full_down, full_gate, full_up, 5
    )
    out_gate = rows.scatter(tie(rows_two, back_two), gate_low, 6)
    grad_normed_two = tie(tensor_scatter(back_two), out_gate).astype(F32)
    grad_mid, grad_norm2 = norm_two_back(grad_normed_two)
    grad_mid = grad_mid + grad_after
    grad_mix = grad_mid.astype(BF)
    out_up = rows.scatter(tie(rows_two, grad_mix), up_low, 7)
    incoming_mix = tie(tensor_gather(grad_mix), out_up)

    ffn_part = tensor_scatter(tie(ffn_out, incoming_mix)).astype(F32)
    outputs = rows.restore(((after_mix + ffn_part) * valid_rows).astype(BF), 1)[None]
    raw_low, ab_low, dtq, dtk, dtv, dpar, dgain, out_out = rows.backward(
        core_in, (plain_dot(incoming_mix, full_out), delta_out, new_values, inverses, states), incoming_mix, head_bf, 8
    )
    def in_lanes(x, lead):
        return jnp.pad(x, ((0, 0), (0, -x.shape[1] % (8 * LANES)))).reshape(lead + (-1, LANES))

    grad_ab = dot_tokens(ab_low, rows_one)[: 2 * heads].reshape(2 * heads, dp_size, block)
    few = [jnp.transpose(grad_ab, (1, 0, 2)).reshape(dp_size, -1)]

    def tap_grad(table, size):
        grad = table[:taps_n].reshape(taps_n, heads, dp_size, size // dp_size)
        return jnp.transpose(grad, (2, 1, 0, 3)).reshape(dp_size, -1)

    taps = [tap_grad(dtq, dk), tap_grad(dtk, dk), tap_grad(dtv, dv)]
    alog_full, dtb_full = (
        lax.dynamic_update_slice_in_dim(jnp.zeros_like(a_log), dpar[i, heads : 2 * heads], head_start, 0)
        for i in range(2)
    )
    rest = [rows.restore(grad_norm2[None], 1)[0], dgain[0], alog_full, dtb_full]
    few, taps, rest_in = (jnp.concatenate(x, axis=-1) for x in (few, taps, rest))
    out_query, out_key, out_value, out_outgate, few_sum, tap_sum, vec_sum, grad_inputs = rows.scatter_last(
        tie(rows_one, out_out), raw_low, ab_low, in_lanes(few, (dp_size,)), in_lanes(taps, (dp_size,)),
        in_lanes(rest_in[None], ()), local_rows, grad_mid, gain_one[None], full_ab, full_raw,
        (wide_k, wide_k, wide_v, wide_v), tensor_size, 9,
    )

    def pieces_of(total, like):
        flat, found, at = total.reshape(-1), [], 0
        for part in like:
            found.append(flat[at : at + part.size])
            at += part.size
        return found

    grad_ab = few_sum.reshape(-1)[: cuts[2]].reshape(2 * heads, block)
    out_beta, out_alpha = grad_ab[:heads].T, grad_ab[heads:].T
    out_cq, out_ck, out_cv = (
        jnp.transpose(x.reshape(heads, taps_n, -1), (2, 0, 1))
        for x in pieces_of(tap_sum, (conv_query, conv_key, conv_value))
    )
    norm1_sum, norm2_sum, hgain_sum, alog_sum, dtb_sum = pieces_of(vec_sum, [norm1_gain] + rest)
    return (
        outputs, grad_inputs[None], norm1_sum, out_query, out_key, out_value, out_outgate,
        out_beta, out_alpha, out_cq, out_ck, out_cv, alog_sum, dtb_sum, hgain_sum, out_out, norm2_sum,
        out_gate, out_up, out_down,
    )


def solution(mesh):
    mat, cube, whole = P("dp", "tensor"), P("dp", "tensor", None), P()
    in_specs = (
        (cube, cube, P("dp"), whole) + (mat,) * 6 + (cube,) * 3 + (whole,) * 3 + (mat, whole) + (mat,) * 3
    )
    out_specs = (
        (cube, cube, whole) + (mat,) * 6 + (cube,) * 3 + (whole,) * 3 + (mat, whole) + (mat,) * 3
    )
    return jax.shard_map(
        functools.partial(shards, mesh.shape["dp"], mesh.shape["tensor"]), mesh=mesh, in_specs=in_specs, out_specs=out_specs,
        check_vma=False,
    )
```
